32 devices in a mesh: region: 4 (over z), depth: 2 (over y), member: 4 (over x, core).
Axes of the slice: x: 2, y: 2, z: 4, core: 2. Of those that a mesh axis runs over, the one named last changes fastest.
Arguments:
- ensemble: bfloat16 [14, 384, 4096], P('depth', 'member', 'region'), may hold values from -6 to 6
- obs_weights: float32 [14], P('depth'), may hold values from -1.5 to 1.5
- obs_tiles: int32 [2048], P('region'), may hold values from 0 to 1023
- obs_values: float32 [2048], P('region'), may hold values from -8 to 8
- obs_error: float32 [2048], P('region'), may hold values from 0.2 to 2
- obs_noise: float32 [384, 2048], P('member', 'region'), may hold values from -6 to 6
Outputs:
- analysis: bfloat16 [14, 384, 4096], P('depth', 'member', 'region')
- inflation: float32 [], replicated
The draws below stay inside these ranges and needn't reach their ends.
Inputs may be any that keep to these rules, and one draw needn't show every extreme that they name: `obs_tiles`: the tile of the observation, counted within the 1024 tiles of the region whose block holds the observation.
All inputs are finite; a program needn't handle non-finite values.
Results may differ from the reference program's by a relative error of at most 0.011.
Values may be sent and summed in bfloat16 or wider, within the bound.
A program may use at most 64 MiB of HBM per device.

```python
import math
import jax
import jax.numpy as jnp
from jax import lax

VARS = 14
MEMBERS = 384
TILE_DEV = 1024
OBS_DEV = 512
NTILES = 4096
NOBS = 2048
RADIUS = 1024
N_REGION = 4


def touch_ends(values, own_key, smallest, largest):
    shape = values.shape
    spot = [jax.random.randint(jax.random.fold_in(own_key, axis), (), 0, shape[axis]) for axis in range(len(shape))]
    values = values.at[tuple(spot)].set(smallest)
    longest = shape.index(max(shape))
    spot[longest] = (spot[longest] + 1) % shape[longest]
    return values.at[tuple(spot)].set(largest)


def block_levels(key, dims, cuts, least, top_value):
    level = 1.0
    for dim, blocks in cuts:
        draws = jax.random.uniform(jax.random.fold_in(jax.random.fold_in(key, 6), dim), (blocks,), jnp.float32, least / len(cuts), top_value / len(cuts))
        level = level * jnp.repeat(jnp.exp(draws), dims[dim] // blocks).reshape((-1,) + (1,) * (len(dims) - 1 - dim))
    return level


def gaussian(key, dims, scale, limit, split=(), kind=jnp.bfloat16):
    factor_of = block_levels(key, dims, split, -0.22, 0.18) if split else 1.0
    drawn = jax.random.normal(key, dims, jnp.float32) * scale * factor_of
    return jnp.minimum(jnp.maximum(drawn, -limit), limit).astype(kind)


def setup_inputs(seed: int = 0) -> dict:
    splits = jax.random.split(jax.random.key(seed), 7)
    return {
        "ensemble": gaussian(splits[0], (VARS, MEMBERS, NTILES), 1.0, 6.0, ((0, 2), (1, 4), (2, 4))),
        "obs_weights": gaussian(splits[1], (VARS,), VARS ** -0.5, 1.5, ((0, 2),), jnp.float32),
        "obs_tiles": touch_ends(jax.random.randint(splits[2], (NOBS,), 0, TILE_DEV), jax.random.fold_in(splits[2], 1), 0, TILE_DEV - 1).astype(jnp.int32),
        "obs_values": gaussian(splits[3], (NOBS,), 2.0, 8.0, ((0, 4),), jnp.float32),
        "obs_error": jnp.clip(jnp.exp(math.log(2.0) - 2.3025851 * jax.random.uniform(splits[4], (NOBS,), jnp.float32) ** block_levels(splits[4], (NOBS,), ((0, 4),), -0.2, 0.2)), 0.2, 2.0),
        "obs_noise": gaussian(splits[5], (MEMBERS, NOBS), 1.0, 6.0, ((0, 4), (1, 4)), jnp.float32),
    }


def reference(ensemble, obs_weights, obs_tiles, obs_values, obs_error, obs_noise):
    state_f = ensemble.astype(jnp.float32)
    state_mean = lax.optimization_barrier(jnp.sum(state_f, axis=1)) / MEMBERS
    anomalies = (state_f - state_mean[:, None, :]).astype(jnp.bfloat16)
    obs_region = jnp.arange(NOBS, dtype=jnp.int32) // OBS_DEV
    obs_global = obs_region * TILE_DEV + obs_tiles.astype(jnp.int32)
    picked = jnp.take(ensemble, obs_global, axis=2).astype(jnp.float32)
    predicted = jnp.einsum('lmk,l->mk', picked, obs_weights.astype(jnp.float32), precision=lax.Precision.HIGHEST)
    obs_mean = lax.optimization_barrier(jnp.sum(predicted, axis=0)) / MEMBERS
    obs_dev = predicted - obs_mean[None, :]
    obs_spread = lax.optimization_barrier(jnp.sum(obs_dev * obs_dev, axis=0)) / (MEMBERS - 1)
    innovation = obs_values - obs_mean
    inflation = jnp.sum(innovation * innovation) / jnp.sum(obs_spread + obs_error)
    infl_root = jnp.sqrt(inflation)
    factor = inflation / (inflation * obs_spread + obs_error)
    obs_anom = obs_dev.astype(jnp.bfloat16)
    perturbed = (innovation[None, :] + jnp.sqrt(obs_error)[None, :] * obs_noise - infl_root * obs_dev).astype(jnp.bfloat16)
    padded_anom = jnp.pad(obs_anom, ((0, 0), (OBS_DEV, OBS_DEV)))
    padded_pert = jnp.pad(perturbed, ((0, 0), (OBS_DEV, OBS_DEV)))
    padded_factor = jnp.pad(factor, (OBS_DEV, OBS_DEV))
    padded_pos = jnp.pad(obs_global.astype(jnp.float32), (OBS_DEV, OBS_DEV))

    def one_region(region_id):
        first_obs = region_id * OBS_DEV
        anom_window = lax.dynamic_slice_in_dim(padded_anom, first_obs, 3 * OBS_DEV, 1).astype(jnp.float32)
        pert_window = lax.dynamic_slice_in_dim(padded_pert, first_obs, 3 * OBS_DEV, 1).astype(jnp.float32)
        factor_window = lax.dynamic_slice_in_dim(padded_factor, first_obs, 3 * OBS_DEV, 0)
        pos_window = lax.dynamic_slice_in_dim(padded_pos, first_obs, 3 * OBS_DEV, 0)
        first_tile = region_id * TILE_DEV
        region_anom = lax.dynamic_slice_in_dim(anomalies, first_tile, TILE_DEV, 2).astype(jnp.float32)
        region_mean = lax.dynamic_slice_in_dim(state_mean, first_tile, TILE_DEV, 1)
        covariance = jnp.einsum('lmt,mj->ltj', region_anom, anom_window) / (MEMBERS - 1)
        tile_pos = (first_tile + jnp.arange(TILE_DEV, dtype=jnp.int32)).astype(jnp.float32)
        closeness = jnp.maximum(0.0, 1.0 - jnp.abs(tile_pos[:, None] - pos_window[None, :]) / RADIUS)
        kalman_gain = (covariance * (closeness * closeness * factor_window[None, :])[None]).astype(jnp.bfloat16)
        increment = jnp.einsum('ltj,mj->lmt', kalman_gain.astype(jnp.float32), pert_window)
        return (region_mean[:, None, :] + infl_root * region_anom + increment).astype(jnp.bfloat16)
    region_out = lax.map(one_region, jnp.arange(N_REGION, dtype=jnp.int32))
    analysis = jnp.transpose(region_out, (1, 2, 0, 3)).reshape(VARS, MEMBERS, NTILES)
    return (analysis, inflation)
```

```python
import functools

import jax
import jax.numpy as jnp
from jax import lax
from jax.experimental import pallas as pl
from jax.experimental.pallas import tpu as pltpu
from jax.sharding import PartitionSpec as P

RADIUS = 1024
LEAD = 2
READY = 3
F32 = jnp.float32
BF16 = jnp.bfloat16
MESH = pl.DeviceIdType.MESH


def kernel(
    sizes,
    weights_hbm,
    ensemble,
    tiles_hbm,
    values_hbm,
    errors_hbm,
    noise,
    out,
    infl_out,
    weights,
    tiles,
    values,
    errors,
    own,
    gathered,
    noise_v,
    part,
    part_in,
    squares,
    tot_in,
    tot_out,
    pos,
    stats,
    obs,
    pert,
    obs_t,
    taper,
    anom,
    means,
    gain,
    result,
    small_sem,
    local_sem,
    send_e,
    recv_e,
    send_p,
    recv_p,
    send_q,
    recv_q,
    send_o,
    recv_o,
    send_g,
    recv_g,
    send_z,
    recv_z,
    send_st,
    recv_st,
    send_pos,
    recv_pos,
    send_ps,
    recv_ps,
    send_pz,
    recv_pz,
    send_pf,
    recv_pf,
    send_f,
    recv_f,
    send_out,
    recv_out,
    own_out,
):
    nr, nd, nm, nl, mm, tt, kk = sizes
    ng = nm // 2
    half = tt // 2
    members = nm * mm
    r = lax.axis_index("region")
    d = lax.axis_index("depth")
    me = lax.axis_index("member")
    q = me // 2
    c = me % 2
    sib = 2 * q + (1 - c)
    has_side = (r > 0, r < nr - 1)

    def dev(region=None, depth=None, member=None):
        return {
            "region": r if region is None else region,
            "depth": d if depth is None else depth,
            "member": me if member is None else member,
        }

    def rdma(src, dst, ssem, rsem, device):
        return pltpu.make_async_remote_copy(
            src_ref=src,
            dst_ref=dst,
            send_sem=ssem,
            recv_sem=rsem,
            device_id=device,
            device_id_type=MESH,
        )

    barrier = pltpu.get_barrier_semaphore()
    for i in range(1, nd):
        pl.semaphore_signal(barrier, inc=1, device_id=dev(depth=(d + i) % nd), device_id_type=MESH)
    for j in range(1, nm):
        pl.semaphore_signal(
            barrier, inc=1, device_id=dev(member=(me + j) % nm), device_id_type=MESH
        )

    local_own = pltpu.make_async_copy(ensemble, own, local_sem.at[0])
    local_own.start()
    smalls = [
        pltpu.make_async_copy(a, b, small_sem.at[i])
        for i, (a, b) in enumerate(
            ((weights_hbm, weights), (tiles_hbm, tiles), (values_hbm, values), (errors_hbm, errors))
        )
    ]
    for copy in smalls:
        copy.start()
    local_half = pltpu.make_async_copy(
        ensemble.at[:, :, pl.ds(pl.multiple_of(c * half, 128), half)],
        gathered.at[:, me],
        local_sem.at[1],
    )
    local_half.start()
    local_noise = pltpu.make_async_copy(noise, noise_v, local_sem.at[2])
    local_noise.start()

    pl.semaphore_wait(barrier, nd - 1 + nm - 1 + (r > 0).astype(jnp.int32))
    for side in (0, 1):

        @pl.when(has_side[side])
        def _():
            pl.semaphore_signal(
                barrier, inc=1, device_id=dev(region=r + (2 * side - 1)), device_id_type=MESH
            )

    def bulk(l, j):
        to = (me + j) % nm
        return rdma(
            ensemble.at[l, :, pl.ds(pl.multiple_of((to % 2) * half, 128), half)],
            gathered.at[l, me],
            send_e.at[l, j],
            recv_e.at[l, me],
            dev(member=to),
        )

    def send_bulk(l, carry):
        for j in range(1, nm):
            bulk(l, j).start()
        return carry

    lead = min(LEAD, nl)
    lax.fori_loop(0, lead, send_bulk, 0)
    for copy in smalls:
        copy.wait()
    local_own.wait()
    total = own[0].astype(F32) * weights[0]
    for l in range(1, nl):
        total = total + own[l].astype(F32) * weights[l]
    hi = total.astype(BF16)
    rest = total - hi.astype(F32)
    mid = rest.astype(BF16)
    low = (rest - mid.astype(F32)).astype(BF16)
    tile_ids = lax.broadcasted_iota(jnp.int32, (tt, kk), 0)
    onehot = jnp.where(tile_ids == tiles[...], 1.0, 0.0).astype(BF16)
    terms = jnp.dot(
        jnp.concatenate([hi, mid, low], axis=0), onehot, preferred_element_type=F32
    )
    picked = terms[0:mm] + terms[mm : 2 * mm] + terms[2 * mm : 3 * mm]
    part_mean = jnp.sum(picked, axis=0, keepdims=True) / mm
    top = part_mean.astype(BF16).astype(F32)
    second_row = (part_mean - top).astype(BF16).astype(F32)
    third_row = part_mean - top - second_row
    prow = lax.broadcasted_iota(jnp.int32, (16, kk), 0)
    split = jnp.where(prow == 0, top, jnp.where(prow == 1, second_row, third_row))
    part[0:mm] = (picked - part_mean).astype(BF16)
    part[mm : mm + 16] = jnp.where(prow < 3, split, 0.0).astype(BF16)

    def whole(block):
        values_of = block.astype(F32)
        return values_of[0:mm] + jnp.sum(values_of[mm : mm + 16], axis=0, keepdims=True)

    def part_copy(i):
        to = (d + i) % nd
        return rdma(part, part_in.at[d], send_p.at[i], recv_p.at[d], dev(depth=to))

    def part_from(i):
        frm = (d + i) % nd
        return rdma(part, part_in.at[frm], send_p.at[i], recv_p.at[frm], dev(depth=frm))

    for i in range(1, nd):
        part_copy(i).start()

    pos[1] = jnp.broadcast_to(tiles[...].astype(F32), (8, kk))

    def pos_copy(side):
        return rdma(
            pos.at[1],
            pos.at[2 - 2 * side],
            send_pos.at[side],
            recv_pos.at[1 - side],
            dev(region=r + (2 * side - 1)),
        )

    def pos_from(side):
        return rdma(
            pos.at[1],
            pos.at[2 * side],
            send_pos.at[side],
            recv_pos.at[side],
            dev(region=r + (2 * side - 1)),
        )

    lane = (lax.broadcasted_iota(jnp.int32, (kk, half), 1) + c * half).astype(F32)

    def make_taper(w):
        position = pos[w].T[:, 0:1] + float((w - 1) * tt)
        close = jnp.maximum(0.0, 1.0 - jnp.abs(lane - position) * (1.0 / RADIUS))
        taper[w * kk : (w + 1) * kk] = close * close

    make_taper(1)

    @pl.when(has_side[1])
    def _():
        pl.semaphore_wait(barrier, 1)

    for side in (0, 1):

        @pl.when(has_side[side])
        def _():
            pos_copy(side).start()

        @pl.when(jnp.logical_not(has_side[side]))
        def _():
            window = 0 if side == 0 else 2 * kk
            obs[:, :, window : window + kk] = jnp.zeros((nm, mm, kk), BF16)
            pert[:, :, window : window + kk] = jnp.zeros((2, mm, kk), BF16)
            stats[2 * side] = jnp.zeros((8, kk), F32)
            pos[2 * side] = jnp.zeros((8, kk), F32)

    predicted = whole(part[...])
    for i in range(1, nd):
        part_from(i).wait_recv()
        predicted = predicted + whole(part_in[(d + i) % nd])
    own_sum = jnp.sum(predicted, axis=0, keepdims=True)
    spread_in = predicted - own_sum / mm
    own_square = jnp.sum(spread_in * spread_in, axis=0, keepdims=True)
    qrow = lax.broadcasted_iota(jnp.int32, (2, kk), 0)
    squares[me] = jnp.where(qrow == 0, own_sum, own_square)
    obs[me, :, kk : 2 * kk] = spread_in.astype(BF16)

    def square_copy(j, slot):
        return rdma(
            squares.at[slot],
            squares.at[slot],
            send_q.at[j],
            recv_q.at[slot],
            dev(member=(me + j) % nm),
        )

    def obs_copy(j, slot):
        block = obs.at[slot, :, pl.ds(kk, kk)]
        return rdma(block, block, send_o.at[j], recv_o.at[slot], dev(member=(me + j) % nm))

    def side_obs(side, slot, pair):
        window = 2 * kk if side == 0 else 0
        return rdma(
            obs.at[slot, :, pl.ds(kk, kk)],
            obs.at[slot, :, pl.ds(window, kk)],
            send_z.at[side, pair],
            recv_z.at[1 - side, pair],
            dev(region=r + (2 * side - 1)),
        )

    def obs_forward(w, slot, pair):
        block = obs.at[slot, :, pl.ds(w * kk, kk)]
        return rdma(block, block, send_f.at[w, pair], recv_f.at[w, pair], dev(member=sib))

    def cross(g):
        return 2 * ((q + g) % ng) + c

    def cross_sib(g):
        return 2 * ((q + g) % ng) + (1 - c)

    for j in range(1, nm):
        square_copy(j, me).start()
    for g in range(1, ng):
        obs_copy(2 * g, me).start()
    obs_forward(1, me, 0).start()
    lax.fori_loop(lead, nl, send_bulk, 0)
    for side in (0, 1):

        @pl.when(has_side[side])
        def _():
            side_obs(side, me, 0).start()
            pos_from(side).wait_recv()

        make_taper(2 * side)

    for j in range(1, nm):
        square_copy(j, (me + j) % nm).wait_recv()
    moments = [squares[j] for j in range(nm)]
    obs_mean = sum(m[0:1] for m in moments) / members
    deviation = predicted - obs_mean
    square_sum = sum(
        m[1:2] + mm * (m[0:1] / mm - obs_mean) * (m[0:1] / mm - obs_mean) for m in moments
    )
    spread = square_sum / (members - 1)
    error = errors[...]
    innovation = values[...] - obs_mean
    first = jnp.sum(innovation * innovation, axis=1, keepdims=True)
    second = jnp.sum(spread + error, axis=1, keepdims=True)
    rp = tot_in.shape[1]
    trow = lax.broadcasted_iota(jnp.int32, (rp, 128), 0)
    tlane = lax.broadcasted_iota(jnp.int32, (rp, 128), 1)
    own_total = jnp.where(tlane == 0, first, second)
    krow = lax.broadcasted_iota(jnp.int32, (8, kk), 0)
    shifts_of = jnp.zeros((8, kk), F32)
    for g in range(nm):
        shifts_of = jnp.where(krow == g, moments[g][0:1] / mm - obs_mean, shifts_of)
    stats[1] = shifts_of

    def stat_copy(side):
        return rdma(
            stats.at[1],
            stats.at[2 - 2 * side],
            send_st.at[side],
            recv_st.at[1 - side],
            dev(region=r + (2 * side - 1)),
        )

    def total_copy(way):
        return rdma(
            tot_out.at[way],
            tot_in.at[way],
            send_g.at[way],
            recv_g.at[way],
            dev(region=r + (1 - 2 * way)),
        )

    def total_from(way):
        return rdma(
            tot_out.at[way],
            tot_in.at[way],
            send_g.at[way],
            recv_g.at[way],
            dev(region=r - (1 - 2 * way)),
        )

    def relay(way):
        @pl.when(has_side[way])
        def _():
            total_from(way).wait_recv()

        behind = trow < r if way == 0 else trow > r
        tot_out[way] = jnp.where(
            behind, tot_in[way], jnp.where(trow == r, own_total, 0.0)
        )

        @pl.when(has_side[1 - way])
        def _():
            total_copy(way).start()

    low_end = r == 0
    high_end = r == nr - 1

    @pl.when(low_end)
    def _():
        relay(0)

    @pl.when(high_end)
    def _():
        relay(1)

    for side in (0, 1):

        @pl.when(has_side[side])
        def _():
            stat_copy(side).start()

    for g in range(1, ng):
        obs_copy(2 * g, cross(g)).wait_recv()
        for side in (0, 1):

            @pl.when(has_side[side])
            def _():
                side_obs(side, cross(g), g).start()

        obs_forward(1, cross(g), g).start()

    def transpose_all(w):
        shifts = stats[w].T
        for g in range(nm):
            block = obs[g, :, w * kk : (w + 1) * kk].astype(F32).T + shifts[:, g : g + 1]
            obs_t[w * kk : (w + 1) * kk, g * mm : (g + 1) * mm] = block.astype(BF16)

    def gain_rows(l, windows):
        right = anom[l].reshape(members, half)
        for w in windows:
            rows_of = slice(w * kk, (w + 1) * kk)
            cov = jnp.dot(obs_t[rows_of], right, preferred_element_type=F32)
            gain[l, rows_of] = (cov * taper[rows_of]).astype(BF16)

    def own_window(l, windows):
        for j in range(1, nm):
            slot = (me + j) % nm
            rdma(
                gathered.at[l, slot],
                gathered.at[l, slot],
                send_e.at[l, j],
                recv_e.at[l, slot],
                dev(member=slot),
            ).wait_recv()
        raw = gathered[l].astype(F32)
        mean = jnp.sum(jnp.sum(raw, axis=0), axis=0, keepdims=True) / members
        means[l] = jnp.broadcast_to(mean, (8, half))
        anom[l] = (raw - mean[None]).astype(BF16)
        gain_rows(l, windows)

    for g in range(ng):
        obs_forward(1, cross_sib(g), g).wait_recv()
    transpose_all(1)
    mid_low = jnp.logical_and(r > 0, 2 * r < nr)
    mid_high = jnp.logical_and(r < nr - 1, 2 * r >= nr)

    @pl.when(mid_low)
    def _():
        relay(0)

    @pl.when(mid_high)
    def _():
        relay(1)

    local_half.wait()
    own_window(0, (1,))

    @pl.when(2 * r < nr)
    def _():
        relay(1)

    @pl.when(2 * r >= nr)
    def _():
        relay(0)

    everyone = jnp.where(trow < r, tot_in[0], jnp.where(trow > r, tot_in[1], own_total))
    grand = everyone[0:1]
    for i in range(1, nr):
        grand = grand + everyone[i : i + 1]
    inflation = grand[0:1, 0:1] / grand[0:1, 1:2]
    root = jnp.sqrt(inflation)
    infl_out[...] = inflation
    factor = inflation / (inflation * spread + error)
    local_noise.wait()
    pert[c, :, kk : 2 * kk] = (
        (innovation + jnp.sqrt(error) * noise_v[...] - root * deviation)
        * (factor / (members - 1))
    ).astype(BF16)

    def sib_pert(slot):
        block = pert.at[slot, :, pl.ds(kk, kk)]
        return rdma(block, block, send_ps.at[0], recv_ps.at[0], dev(member=sib))

    def side_pert(side):
        window = 2 * kk if side == 0 else 0
        return rdma(
            pert.at[c, :, pl.ds(kk, kk)],
            pert.at[c, :, pl.ds(window, kk)],
            send_pz.at[side],
            recv_pz.at[1 - side],
            dev(region=r + (2 * side - 1)),
        )

    def pert_forward(side, slot):
        block = pert.at[slot, :, pl.ds(2 * kk * side, kk)]
        return rdma(block, block, send_pf.at[side], recv_pf.at[side], dev(member=sib))

    sib_pert(c).start()
    for side in (0, 1):

        @pl.when(has_side[side])
        def _():
            side_pert(side).start()

    for g in range(ng):
        for side in (0, 1):

            @pl.when(has_side[side])
            def _():
                side_obs(1 - side, cross(g), g).wait_recv()
                obs_forward(2 * side, cross(g), g).start()

    own_window(1, (1,))
    for side in (0, 1):

        @pl.when(has_side[side])
        def _():
            rdma(
                stats.at[1],
                stats.at[2 * side],
                send_st.at[side],
                recv_st.at[side],
                dev(region=r + (2 * side - 1)),
            ).wait_recv()
            for g in range(ng):
                obs_forward(2 * side, cross_sib(g), g).wait_recv()

        transpose_all(2 * side)

    def out_half(l, which):
        return out.at[l, :, pl.ds(pl.multiple_of(which * half, 128), half)]

    def out_local(l):
        return pltpu.make_async_copy(result.at[l, c], out_half(l, c), own_out.at[l])

    def out_remote(l):
        return rdma(
            result.at[l, 1 - c], out_half(l, c), send_out.at[l], recv_out.at[l], dev(member=sib)
        )

    def out_from(l):
        return rdma(
            result.at[l, 1 - c], out_half(l, 1 - c), send_out.at[l], recv_out.at[l], dev(member=sib)
        )

    def finish_variable(l):
        increment = jnp.dot(
            pert[...].reshape(2 * mm, 3 * kk), gain[l], preferred_element_type=F32
        )
        base = means[l][0:1][None] + root[None] * anom[l, pl.ds(2 * q, 2)].astype(F32)
        result[l] = (base + increment.reshape(2, mm, half)).astype(BF16)
        out_local(l).start()
        out_remote(l).start()

    def side_gain(l, carry):
        gain_rows(l, (0, 2))
        return carry

    lax.fori_loop(0, 2, side_gain, 0)
    for side in (0, 1):

        @pl.when(has_side[side])
        def _():
            side_pert(1 - side).wait_recv()
            pert_forward(side, c).start()

    ready = min(READY, nl)

    def ahead(l, carry):
        own_window(l, (0, 1, 2))
        return carry

    lax.fori_loop(2, ready, ahead, 0)
    sib_pert(1 - c).wait_recv()
    for side in (0, 1):

        @pl.when(has_side[side])
        def _():
            pert_forward(side, 1 - c).wait_recv()

    def late_variable(l, carry):
        finish_variable(l)
        return carry

    lax.fori_loop(0, ready, late_variable, 0)

    def one_variable(l, carry):
        own_window(l, (0, 1, 2))
        finish_variable(l)
        return carry

    lax.fori_loop(ready, nl, one_variable, 0)

    def finish(l, carry):
        for j in range(1, nm):
            bulk(l, j).wait_send()
        out_local(l).wait()
        out_remote(l).wait_send()
        out_from(l).wait_recv()
        return carry

    lax.fori_loop(0, nl, finish, 0)
    for i in range(1, nd):
        part_copy(i).wait_send()
    for j in range(1, nm):
        square_copy(j, me).wait_send()
    for g in range(1, ng):
        obs_copy(2 * g, me).wait_send()
    for g in range(ng):
        obs_forward(1, cross(g), g).wait_send()
    sib_pert(c).wait_send()
    for way in (0, 1):

        @pl.when(has_side[1 - way])
        def _():
            total_copy(way).wait_send()

    for side in (0, 1):

        @pl.when(has_side[side])
        def _():
            for g in range(ng):
                side_obs(side, cross(g), g).wait_send()
                obs_forward(2 * side, cross(g), g).wait_send()
            side_pert(side).wait_send()
            pert_forward(side, c).wait_send()
            stat_copy(side).wait_send()
            pos_copy(side).wait_send()


def hand_on(block, out):
    pass


def solution(mesh):
    nr, nd, nm = (mesh.shape[a] for a in ("region", "depth", "member"))

    def shards(ensemble, obs_weights, obs_tiles, obs_values, obs_error, obs_noise):
        nl, mm, tt = ensemble.shape
        kk = obs_tiles.shape[0]
        ng = nm // 2
        half = tt // 2
        rp = -(-nr // 8) * 8
        dma = pltpu.SemaphoreType.DMA
        vmem = pl.BlockSpec(memory_space=pltpu.VMEM)
        anywhere = pl.BlockSpec(memory_space=pl.ANY)
        analysis, inflation = pl.pallas_call(
            functools.partial(kernel, (nr, nd, nm, nl, mm, tt, kk)),
            out_shape=(
                pltpu.VMEM((nl, mm, tt), BF16),
                jax.ShapeDtypeStruct((1, 1), F32),
            ),
            in_specs=[anywhere] * 6,
            out_specs=(vmem, vmem),
            scratch_shapes=[
                pltpu.SMEM((nl,), F32),
                pltpu.VMEM((1, kk), jnp.int32),
                pltpu.VMEM((1, kk), F32),
                pltpu.VMEM((1, kk), F32),
                pltpu.VMEM((nl, mm, tt), BF16),
                pltpu.VMEM((nl, nm, mm, half), BF16),
                pltpu.VMEM((mm, kk), F32),
                pltpu.VMEM((mm + 16, kk), BF16),
                pltpu.VMEM((nd, mm + 16, kk), BF16),
                pltpu.VMEM((nm, 2, kk), F32),
                pltpu.VMEM((2, rp, 128), F32),
                pltpu.VMEM((2, rp, 128), F32),
                pltpu.VMEM((3, 8, kk), F32),
                pltpu.VMEM((3, 8, kk), F32),
                pltpu.VMEM((nm, mm, 3 * kk), BF16),
                pltpu.VMEM((2, mm, 3 * kk), BF16),
                pltpu.VMEM((3 * kk, nm * mm), BF16),
                pltpu.VMEM((3 * kk, half), F32),
                pltpu.VMEM((nl, nm, mm, half), BF16),
                pltpu.VMEM((nl, 8, half), F32),
                pltpu.VMEM((nl, 3 * kk, half), BF16),
                pltpu.VMEM((nl, 2, mm, half), BF16),
                dma((4,)),
                dma((3,)),
                dma((nl, nm)),
                dma((nl, nm)),
                dma((nd,)),
                dma((nd,)),
                dma((nm,)),
                dma((nm,)),
                dma((nm,)),
                dma((nm,)),
                dma((2,)),
                dma((2,)),
                dma((2, ng)),
                dma((2, ng)),
                dma((2,)),
                dma((2,)),
                dma((2,)),
                dma((2,)),
                dma((1,)),
                dma((1,)),
                dma((2,)),
                dma((2,)),
                dma((2,)),
                dma((2,)),
                dma((3, ng)),
                dma((3, ng)),
                dma((nl,)),
                dma((nl,)),
                dma((nl,)),
            ],
            compiler_params=pltpu.CompilerParams(
                collective_id=0, has_side_effects=True, vmem_limit_bytes=56 * 1024 * 1024
            ),
        )(
            obs_weights,
            ensemble,
            obs_tiles.reshape(1, kk),
            obs_values.reshape(1, kk),
            obs_error.reshape(1, kk),
            obs_noise,
        )
        analysis = pl.pallas_call(
            hand_on,
            out_shape=jax.ShapeDtypeStruct((nl, mm, tt), BF16),
            in_specs=[anywhere],
            out_specs=anywhere,
            input_output_aliases={0: 0},
        )(analysis)
        return analysis, inflation.reshape(())

    return jax.shard_map(
        shards,
        mesh=mesh,
        in_specs=(
            P("depth", "member", "region"),
            P("depth"),
            P("region"),
            P("region"),
            P("region"),
            P("member", "region"),
        ),
        out_specs=(P("depth", "member", "region"), P()),
        check_vma=False,
    )
```

```python
import functools

import jax
import jax.numpy as jnp
from jax import lax
from jax.experimental import pallas as pl
from jax.experimental.pallas import tpu as pltpu
from jax.sharding import PartitionSpec as P

RADIUS = 1024
LEAD = 3
READY = 5
PIECES = 2
F32 = jnp.float32
BF16 = jnp.bfloat16
MESH = pl.DeviceIdType.MESH


def kernel(
    sizes,
    weights_hbm,
    ensemble,
    tiles_hbm,
    values_hbm,
    errors_hbm,
    noise,
    out,
    infl_out,
    weights,
    tiles,
    values,
    errors,
    own,
    gathered,
    noise_v,
    part,
    part_in,
    squares,
    tot_in,
    tot_out,
    pos,
    stats,
    obs,
    pert,
    obs_t,
    taper,
    anom,
    means,
    gain,
    result,
    scale,
    answer,
    small_sem,
    local_sem,
    send_e,
    recv_e,
    send_p,
    recv_p,
    send_q,
    recv_q,
    send_o,
    recv_o,
    send_g,
    recv_g,
    send_y,
    recv_y,
    send_z,
    recv_z,
    send_st,
    recv_st,
    send_pos,
    recv_pos,
    send_ps,
    recv_ps,
    send_pz,
    recv_pz,
    send_pf,
    recv_pf,
    send_f,
    recv_f,
    send_out,
    recv_out,
    own_out,
):
    nr, nd, nm, nl, mm, tt, kk = sizes
    ng = nm // 2
    half = tt // 2
    members = nm * mm
    r = lax.axis_index("region")
    d = lax.axis_index("depth")
    me = lax.axis_index("member")
    q = me // 2
    c = me % 2
    sib = 2 * q + (1 - c)
    has_side = (r > 0, r < nr - 1)

    def dev(region=None, depth=None, member=None):
        return {
            "region": r if region is None else region,
            "depth": d if depth is None else depth,
            "member": me if member is None else member,
        }

    def rdma(src, dst, ssem, rsem, device):
        return pltpu.make_async_remote_copy(
            src_ref=src,
            dst_ref=dst,
            send_sem=ssem,
            recv_sem=rsem,
            device_id=device,
            device_id_type=MESH,
        )

    barrier = pltpu.get_barrier_semaphore()
    for j in range(1, nm):
        pl.semaphore_signal(
            barrier, inc=1, device_id=dev(member=(me + j) % nm), device_id_type=MESH
        )
    for i in range(1, nd):

        @pl.when(d + i < nd)
        def _():
            pl.semaphore_signal(barrier, inc=1, device_id=dev(depth=d + i), device_id_type=MESH)

    @pl.when(has_side[1])
    def _():
        pl.semaphore_signal(barrier, inc=1, device_id=dev(region=r + 1), device_id_type=MESH)

    local_own = pltpu.make_async_copy(ensemble, own, local_sem.at[0])
    local_own.start()
    smalls = [
        pltpu.make_async_copy(a, b, small_sem.at[i])
        for i, (a, b) in enumerate(
            ((weights_hbm, weights), (tiles_hbm, tiles), (values_hbm, values), (errors_hbm, errors))
        )
    ]
    for copy in smalls:
        copy.start()
    local_half = pltpu.make_async_copy(
        ensemble.at[:, :, pl.ds(pl.multiple_of(c * half, 128), half)],
        gathered.at[:, me],
        local_sem.at[1],
    )
    local_half.start()
    local_noise = pltpu.make_async_copy(noise, noise_v, local_sem.at[2])
    local_noise.start()

    pl.semaphore_wait(barrier, nm - 1 + d + (r > 0).astype(jnp.int32))

    piece = half // PIECES
    units = nl * PIECES

    def bulk(u, j):
        to = (me + j) % nm
        l, at = u // PIECES, (u % PIECES) * piece
        return rdma(
            ensemble.at[l, :, pl.ds(pl.multiple_of((to % 2) * half + at, 128), piece)],
            gathered.at[l, me, :, pl.ds(pl.multiple_of(at, 128), piece)],
            send_e.at[u, j],
            recv_e.at[u, me],
            dev(member=to),
        )

    def bulk_from(u, j):
        slot = (me + j) % nm
        l, at = u // PIECES, (u % PIECES) * piece
        block = gathered.at[l, slot, :, pl.ds(pl.multiple_of(at, 128), piece)]
        return rdma(block, block, send_e.at[u, j], recv_e.at[u, slot], dev(member=slot))

    def send_bulk(u, carry):
        for j in range(1, nm):
            bulk(u, j).start()
        return carry

    lead = min(LEAD, units)
    lax.fori_loop(0, lead, send_bulk, 0)
    for i in range(1, nd):

        @pl.when(d >= i)
        def _():
            pl.semaphore_signal(
                answer.at[0], inc=1, device_id=dev(depth=d - i), device_id_type=MESH
            )

    @pl.when(has_side[0])
    def _():
        pl.semaphore_signal(answer.at[1], inc=1, device_id=dev(region=r - 1), device_id_type=MESH)

    for copy in smalls:
        copy.wait()
    local_own.wait()
    total = own[0].astype(F32) * weights[0]
    for l in range(1, nl):
        total = total + own[l].astype(F32) * weights[l]
    hi = total.astype(BF16)
    rest = total - hi.astype(F32)
    mid = rest.astype(BF16)
    low = (rest - mid.astype(F32)).astype(BF16)
    tile_ids = lax.broadcasted_iota(jnp.int32, (tt, kk), 0)
    onehot = jnp.where(tile_ids == tiles[...], 1.0, 0.0).astype(BF16)
    terms = jnp.dot(
        jnp.concatenate([hi, mid, low], axis=0), onehot, preferred_element_type=F32
    )
    picked = terms[0:mm] + terms[mm : 2 * mm] + terms[2 * mm : 3 * mm]
    part_mean = jnp.sum(picked, axis=0, keepdims=True) / mm
    top = part_mean.astype(BF16).astype(F32)
    second_row = (part_mean - top).astype(BF16).astype(F32)
    third_row = part_mean - top - second_row
    prow = lax.broadcasted_iota(jnp.int32, (16, kk), 0)
    split = jnp.where(prow == 0, top, jnp.where(prow == 1, second_row, third_row))
    part[0:mm] = (picked - part_mean).astype(BF16)
    part[mm : mm + 16] = jnp.where(prow < 3, split, 0.0).astype(BF16)

    def whole(block):
        values_of = block.astype(F32)
        return values_of[0:mm] + jnp.sum(values_of[mm : mm + 16], axis=0, keepdims=True)

    def part_copy(i):
        to = (d + i) % nd
        return rdma(part, part_in.at[d], send_p.at[i], recv_p.at[d], dev(depth=to))

    def part_from(i):
        frm = (d + i) % nd
        return rdma(part, part_in.at[frm], send_p.at[i], recv_p.at[frm], dev(depth=frm))

    @pl.when(d < nd - 1)
    def _():
        pl.semaphore_wait(answer.at[0], nd - 1 - d)

    for i in range(1, nd):
        part_copy(i).start()

    pos[1] = jnp.broadcast_to(tiles[...].astype(F32), (8, kk))

    def pos_copy(side):
        return rdma(
            pos.at[1],
            pos.at[2 - 2 * side],
            send_pos.at[side],
            recv_pos.at[1 - side],
            dev(region=r + (2 * side - 1)),
        )

    def pos_from(side):
        return rdma(
            pos.at[1],
            pos.at[2 * side],
            send_pos.at[side],
            recv_pos.at[side],
            dev(region=r + (2 * side - 1)),
        )

    lane = (lax.broadcasted_iota(jnp.int32, (kk, half), 1) + c * half).astype(F32)

    def make_taper(w):
        position = pos[w].T[:, 0:1] + float((w - 1) * tt)
        close = jnp.maximum(0.0, 1.0 - jnp.abs(lane - position) * (1.0 / RADIUS))
        taper[w * kk : (w + 1) * kk] = close * close

    make_taper(1)

    @pl.when(has_side[1])
    def _():
        pl.semaphore_wait(answer.at[1], 1)

    for side in (0, 1):

        @pl.when(has_side[side])
        def _():
            pos_copy(side).start()

        @pl.when(jnp.logical_not(has_side[side]))
        def _():
            window = 0 if side == 0 else 2 * kk
            obs[:, :, window : window + kk] = jnp.zeros((nm, mm, kk), BF16)
            pert[:, :, window : window + kk] = jnp.zeros((2, mm, kk), BF16)
            stats[2 * side] = jnp.zeros((8, kk), F32)
            pos[2 * side] = jnp.zeros((8, kk), F32)

    predicted = whole(part[...])
    for i in range(1, nd):
        part_from(i).wait_recv()
        predicted = predicted + whole(part_in[(d + i) % nd])
    own_sum = jnp.sum(predicted, axis=0, keepdims=True)
    spread_in = predicted - own_sum / mm
    own_square = jnp.sum(spread_in * spread_in, axis=0, keepdims=True)
    qrow = lax.broadcasted_iota(jnp.int32, (2, kk), 0)
    squares[me] = jnp.where(qrow == 0, own_sum, own_square)
    obs[me, :, kk : 2 * kk] = spread_in.astype(BF16)

    def square_copy(j, slot):
        return rdma(
            squares.at[slot],
            squares.at[slot],
            send_q.at[j],
            recv_q.at[slot],
            dev(member=(me + j) % nm),
        )

    hk = kk // nd

    def obs_at(slot, w, h, width):
        return obs.at[slot, :, pl.ds(pl.multiple_of(w * kk + h * hk, 128), width)]

    def obs_copy(j, slot):
        block = obs_at(slot, 1, d, hk)
        return rdma(block, block, send_o.at[j], recv_o.at[slot], dev(member=(me + j) % nm))

    def obs_swap(g, i, h):
        block = obs_at(cross(g), 1, h, hk)
        return rdma(block, block, send_y.at[g, i], recv_y.at[g, h], dev(depth=(d + i) % nd))

    def side_obs(side, slot, pair, h, width):
        return rdma(
            obs_at(slot, 1, h, width),
            obs_at(slot, 2 if side == 0 else 0, h, width),
            send_z.at[side, pair, h],
            recv_z.at[1 - side, pair, h],
            dev(region=r + (2 * side - 1)),
        )

    def side_from(side, slot, pair, h, width):
        block = obs_at(slot, 2 * side, h, width)
        return rdma(
            block,
            block,
            send_z.at[side, pair, h],
            recv_z.at[side, pair, h],
            dev(region=r + (2 * side - 1)),
        )

    def obs_forward(w, slot, pair, h, width):
        block = obs_at(slot, w, h, width)
        return rdma(
            block, block, send_f.at[w, pair, h], recv_f.at[w, pair, h], dev(member=sib)
        )

    def cross(g):
        return 2 * ((q + g) % ng) + c

    def cross_sib(g):
        return 2 * ((q + g) % ng) + (1 - c)

    for j in range(1, nm):
        square_copy(j, me).start()
    for g in range(1, ng):
        obs_copy(2 * g, me).start()
    obs_forward(1, me, 0, 0, kk).start()
    lax.fori_loop(lead, units, send_bulk, 0)
    for side in (0, 1):

        @pl.when(has_side[side])
        def _():
            side_obs(side, me, 0, 0, kk).start()
            pos_from(side).wait_recv()

        make_taper(2 * side)

    for j in range(1, nm):
        square_copy(j, (me + j) % nm).wait_recv()
    moments = [squares[j] for j in range(nm)]
    obs_mean = sum(m[0:1] for m in moments) / members
    deviation = predicted - obs_mean
    square_sum = sum(
        m[1:2] + mm * (m[0:1] / mm - obs_mean) * (m[0:1] / mm - obs_mean) for m in moments
    )
    spread = square_sum / (members - 1)
    error = errors[...]
    innovation = values[...] - obs_mean
    first = jnp.sum(innovation * innovation, axis=1, keepdims=True)
    second = jnp.sum(spread + error, axis=1, keepdims=True)
    rp = tot_in.shape[1]
    trow = lax.broadcasted_iota(jnp.int32, (rp, 128), 0)
    tlane = lax.broadcasted_iota(jnp.int32, (rp, 128), 1)
    own_total = jnp.where(tlane == 0, first, second)
    krow = lax.broadcasted_iota(jnp.int32, (8, kk), 0)
    shifts_of = jnp.zeros((8, kk), F32)
    for g in range(nm):
        shifts_of = jnp.where(krow == g, moments[g][0:1] / mm - obs_mean, shifts_of)
    stats[1] = shifts_of

    def stat_copy(side):
        return rdma(
            stats.at[1],
            stats.at[2 - 2 * side],
            send_st.at[side],
            recv_st.at[1 - side],
            dev(region=r + (2 * side - 1)),
        )

    def total_copy(way):
        return rdma(
            tot_out.at[way],
            tot_in.at[way],
            send_g.at[way],
            recv_g.at[way],
            dev(region=r + (1 - 2 * way)),
        )

    def total_from(way):
        return rdma(
            tot_out.at[way],
            tot_in.at[way],
            send_g.at[way],
            recv_g.at[way],
            dev(region=r - (1 - 2 * way)),
        )

    def relay(way):
        @pl.when(has_side[way])
        def _():
            total_from(way).wait_recv()

        behind = trow < r if way == 0 else trow > r
        tot_out[way] = jnp.where(
            behind, tot_in[way], jnp.where(trow == r, own_total, 0.0)
        )

        @pl.when(has_side[1 - way])
        def _():
            total_copy(way).start()

    low_end = r == 0
    high_end = r == nr - 1

    @pl.when(low_end)
    def _():
        relay(0)

    @pl.when(high_end)
    def _():
        relay(1)

    for side in (0, 1):

        @pl.when(has_side[side])
        def _():
            stat_copy(side).start()

    def hand_part(g, h):
        for side in (0, 1):

            @pl.when(has_side[side])
            def _():
                side_obs(side, cross(g), g, h, hk).start()

        obs_forward(1, cross(g), g, h, hk).start()

    for g in range(1, ng):
        obs_copy(2 * g, cross(g)).wait_recv()
        for i in range(1, nd):
            obs_swap(g, i, d).start()
        hand_part(g, d)

    def transpose_part(w, h, width):
        at = pl.multiple_of(h * hk, 128)
        rows_of = pl.ds(pl.multiple_of(w * kk + at, 128), width)
        shifts = stats[w, :, pl.ds(at, width)].T
        for g in range(nm):
            block = obs[g, :, rows_of].astype(F32).T + shifts[:, g : g + 1]
            obs_t[rows_of, g * mm : (g + 1) * mm] = block.astype(BF16)

    everything = (0, half)

    def gain_rows(l, windows, columns=everything):
        cols = slice(*columns)
        right = anom[l, :, :, cols].reshape(members, columns[1] - columns[0])
        for w in windows:
            rows_of = slice(w * kk, (w + 1) * kk)
            cov = jnp.dot(obs_t[rows_of], right, preferred_element_type=F32)
            gain[l, rows_of, cols] = (cov * taper[rows_of, cols]).astype(BF16)

    def center(l, columns=everything):
        cols = slice(*columns)
        for u in range(columns[0] // piece, columns[1] // piece):
            for j in range(1, nm):
                bulk_from(l * PIECES + u, j).wait_recv()
        raw = gathered[l, :, :, cols].astype(F32)
        mean = jnp.sum(jnp.sum(raw, axis=0), axis=0, keepdims=True) / members
        means[l, :, cols] = jnp.broadcast_to(mean, (8, columns[1] - columns[0]))
        anom[l, :, :, cols] = (raw - mean[None]).astype(BF16)

    def own_window(l, windows, columns=everything):
        center(l, columns)
        gain_rows(l, windows, columns)

    def sib_pert(slot):
        block = pert.at[slot, :, pl.ds(kk, kk)]
        return rdma(block, block, send_ps.at[0], recv_ps.at[0], dev(member=sib))

    def side_pert(side):
        window = 2 * kk if side == 0 else 0
        return rdma(
            pert.at[c, :, pl.ds(kk, kk)],
            pert.at[c, :, pl.ds(window, kk)],
            send_pz.at[side],
            recv_pz.at[1 - side],
            dev(region=r + (2 * side - 1)),
        )

    def pert_forward(side, slot):
        block = pert.at[slot, :, pl.ds(2 * kk * side, kk)]
        return rdma(block, block, send_pf.at[side], recv_pf.at[side], dev(member=sib))

    def make_pert():
        everyone = jnp.where(trow < r, tot_in[0], jnp.where(trow > r, tot_in[1], own_total))
        grand = everyone[0:1]
        for i in range(1, nr):
            grand = grand + everyone[i : i + 1]
        inflation = grand[0:1, 0:1] / grand[0:1, 1:2]
        root = jnp.sqrt(inflation)
        infl_out[...] = inflation
        scale[...] = jnp.broadcast_to(root, (1, 128))
        factor = inflation / (inflation * spread + error)
        local_noise.wait()
        pert[c, :, kk : 2 * kk] = (
            (innovation + jnp.sqrt(error) * noise_v[...] - root * deviation)
            * (factor / (members - 1))
        ).astype(BF16)

        sib_pert(c).start()
        for side in (0, 1):

            @pl.when(has_side[side])
            def _():
                side_pert(side).start()

    mid_low = jnp.logical_and(r > 0, 2 * r < nr)
    mid_high = jnp.logical_and(r < nr - 1, 2 * r >= nr)

    @pl.when(mid_low)
    def _():
        relay(0)

    @pl.when(mid_high)
    def _():
        relay(1)

    obs_forward(1, sib, 0, 0, kk).wait_recv()
    for g in range(1, ng):
        obs_forward(1, cross_sib(g), g, d, hk).wait_recv()
    transpose_part(1, d, hk)
    local_half.wait()
    center(0)
    for i in range(1, nd):
        h = (d + i) % nd
        for g in range(1, ng):
            obs_swap(g, i, h).wait_recv()
            hand_part(g, h)
    center(1)
    for i in range(1, nd):
        h = (d + i) % nd
        for g in range(1, ng):
            obs_forward(1, cross_sib(g), g, h, hk).wait_recv()
        transpose_part(1, h, hk)
    gain_rows(0, (1,))

    for side in (0, 1):

        @pl.when(has_side[side])
        def _():
            side_from(side, me, 0, 0, kk).wait_recv()
            obs_forward(2 * side, me, 0, 0, kk).start()
            for g in range(1, ng):
                for h in range(nd):
                    side_from(side, cross(g), g, h, hk).wait_recv()
                obs_forward(2 * side, cross(g), g, 0, kk).start()

    gain_rows(1, (1,))

    @pl.when(mid_low)
    def _():
        relay(1)
        make_pert()

    @pl.when(mid_high)
    def _():
        relay(0)
        make_pert()

    for side in (0, 1):

        @pl.when(has_side[side])
        def _():
            rdma(
                stats.at[1],
                stats.at[2 * side],
                send_st.at[side],
                recv_st.at[side],
                dev(region=r + (2 * side - 1)),
            ).wait_recv()
            for g in range(ng):
                obs_forward(2 * side, cross_sib(g), g, 0, kk).wait_recv()

        transpose_part(2 * side, 0, kk)

    def out_block(l, which, p):
        at = which * half + p * piece
        return out.at[l, :, pl.ds(pl.multiple_of(at, 128), piece)]

    def out_piece(l, which, p):
        return result.at[l, which, :, p * piece : (p + 1) * piece]

    def out_local(l, p):
        return pltpu.make_async_copy(out_piece(l, c, p), out_block(l, c, p), own_out.at[l, p])

    def out_remote(l, p):
        return rdma(
            out_piece(l, 1 - c, p),
            out_block(l, c, p),
            send_out.at[l, p],
            recv_out.at[l, p],
            dev(member=sib),
        )

    def out_from(l, p):
        return rdma(
            out_piece(l, 1 - c, p),
            out_block(l, 1 - c, p),
            send_out.at[l, p],
            recv_out.at[l, p],
            dev(member=sib),
        )

    def finish_variable(l, columns=everything):
        cols = slice(*columns)
        width = columns[1] - columns[0]
        increment = jnp.dot(
            pert[...].reshape(2 * mm, 3 * kk), gain[l, :, cols], preferred_element_type=F32
        )
        base = means[l, 0:1, cols][None] + root[None] * anom[l, pl.ds(2 * q, 2), :, cols].astype(F32)
        result[l, :, :, cols] = (base + increment.reshape(2, mm, width)).astype(BF16)
        for p in range(columns[0] // piece, columns[1] // piece):
            out_remote(l, p).start()
            out_local(l, p).start()

    def side_gain(l, carry):
        gain_rows(l, (0, 2))
        return carry

    lax.fori_loop(0, 2, side_gain, 0)
    own_window(2, (0, 1, 2))

    @pl.when(low_end)
    def _():
        relay(1)
        make_pert()

    @pl.when(high_end)
    def _():
        relay(0)
        make_pert()

    own_window(3, (0, 1, 2))
    for side in (0, 1):

        @pl.when(has_side[side])
        def _():
            side_pert(1 - side).wait_recv()
            pert_forward(side, c).start()

    root = scale[0:1, 0:1]
    ready = min(READY, nl - 1)

    def ahead(l, carry):
        own_window(l, (0, 1, 2))
        return carry

    lax.fori_loop(4, ready, ahead, 0)
    sib_pert(1 - c).wait_recv()
    for side in (0, 1):

        @pl.when(has_side[side])
        def _():
            pert_forward(side, 1 - c).wait_recv()

    def late_variable(l, carry):
        finish_variable(l)
        return carry

    lax.fori_loop(0, ready, late_variable, 0)

    def one_variable(l, carry):
        own_window(l, (0, 1, 2))
        finish_variable(l)
        return carry

    lax.fori_loop(ready, nl - 1, one_variable, 0)
    for p in range(PIECES):
        columns = (p * piece, (p + 1) * piece)
        own_window(nl - 1, (0, 1, 2), columns)
        finish_variable(nl - 1, columns)

    def finish(l, carry):
        for p in range(PIECES):
            for j in range(1, nm):
                bulk(l * PIECES + p, j).wait_send()
            out_local(l, p).wait()
            out_remote(l, p).wait_send()
            out_from(l, p).wait_recv()
        return carry

    lax.fori_loop(0, nl, finish, 0)
    for i in range(1, nd):
        part_copy(i).wait_send()
    for j in range(1, nm):
        square_copy(j, me).wait_send()
    for g in range(1, ng):
        obs_copy(2 * g, me).wait_send()
    obs_forward(1, me, 0, 0, kk).wait_send()
    for g in range(1, ng):
        for i in range(1, nd):
            obs_swap(g, i, d).wait_send()
        for h in range(nd):
            obs_forward(1, cross(g), g, h, hk).wait_send()
    sib_pert(c).wait_send()
    for way in (0, 1):

        @pl.when(has_side[1 - way])
        def _():
            total_copy(way).wait_send()

    for side in (0, 1):

        @pl.when(has_side[side])
        def _():
            side_obs(side, me, 0, 0, kk).wait_send()
            obs_forward(2 * side, me, 0, 0, kk).wait_send()
            for g in range(1, ng):
                for h in range(nd):
                    side_obs(side, cross(g), g, h, hk).wait_send()
                obs_forward(2 * side, cross(g), g, 0, kk).wait_send()
            side_pert(side).wait_send()
            pert_forward(side, c).wait_send()
            stat_copy(side).wait_send()
            pos_copy(side).wait_send()


def hand_on(block, out):
    pass


def solution(mesh):
    nr, nd, nm = (mesh.shape[a] for a in ("region", "depth", "member"))

    def shards(ensemble, obs_weights, obs_tiles, obs_values, obs_error, obs_noise):
        nl, mm, tt = ensemble.shape
        kk = obs_tiles.shape[0]
        ng = nm // 2
        half = tt // 2
        rp = -(-nr // 8) * 8
        dma = pltpu.SemaphoreType.DMA
        vmem = pl.BlockSpec(memory_space=pltpu.VMEM)
        anywhere = pl.BlockSpec(memory_space=pl.ANY)
        analysis, inflation = pl.pallas_call(
            functools.partial(kernel, (nr, nd, nm, nl, mm, tt, kk)),
            out_shape=(
                pltpu.VMEM((nl, mm, tt), BF16),
                jax.ShapeDtypeStruct((1, 1), F32),
            ),
            in_specs=[anywhere] * 6,
            out_specs=(vmem, vmem),
            scratch_shapes=[
                pltpu.SMEM((nl,), F32),
                pltpu.VMEM((1, kk), jnp.int32),
                pltpu.VMEM((1, kk), F32),
                pltpu.VMEM((1, kk), F32),
                pltpu.VMEM((nl, mm, tt), BF16),
                pltpu.VMEM((nl, nm, mm, half), BF16),
                pltpu.VMEM((mm, kk), F32),
                pltpu.VMEM((mm + 16, kk), BF16),
                pltpu.VMEM((nd, mm + 16, kk), BF16),
                pltpu.VMEM((nm, 2, kk), F32),
                pltpu.VMEM((2, rp, 128), F32),
                pltpu.VMEM((2, rp, 128), F32),
                pltpu.VMEM((3, 8, kk), F32),
                pltpu.VMEM((3, 8, kk), F32),
                pltpu.VMEM((nm, mm, 3 * kk), BF16),
                pltpu.VMEM((2, mm, 3 * kk), BF16),
                pltpu.VMEM((3 * kk, nm * mm), BF16),
                pltpu.VMEM((3 * kk, half), F32),
                pltpu.VMEM((nl, nm, mm, half), BF16),
                pltpu.VMEM((nl, 8, half), F32),
                pltpu.VMEM((nl, 3 * kk, half), BF16),
                pltpu.VMEM((nl, 2, mm, half), BF16),
                pltpu.VMEM((1, 128), F32),
                pltpu.SemaphoreType.REGULAR((2,)),
                dma((4,)),
                dma((3,)),
                dma((nl * PIECES, nm)),
                dma((nl * PIECES, nm)),
                dma((nd,)),
                dma((nd,)),
                dma((nm,)),
                dma((nm,)),
                dma((nm,)),
                dma((nm,)),
                dma((2,)),
                dma((2,)),
                dma((ng, nd)),
                dma((ng, nd)),
                dma((2, ng, nd)),
                dma((2, ng, nd)),
                dma((2,)),
                dma((2,)),
                dma((2,)),
                dma((2,)),
                dma((1,)),
                dma((1,)),
                dma((2,)),
                dma((2,)),
                dma((2,)),
                dma((2,)),
                dma((3, ng, nd)),
                dma((3, ng, nd)),
                dma((nl, PIECES)),
                dma((nl, PIECES)),
                dma((nl, PIECES)),
            ],
            compiler_params=pltpu.CompilerParams(
                collective_id=0, has_side_effects=True, vmem_limit_bytes=56 * 1024 * 1024
            ),
        )(
            obs_weights,
            ensemble,
            obs_tiles.reshape(1, kk),
            obs_values.reshape(1, kk),
            obs_error.reshape(1, kk),
            obs_noise,
        )
        analysis = pl.pallas_call(
            hand_on,
            out_shape=jax.ShapeDtypeStruct((nl, mm, tt), BF16),
            in_specs=[anywhere],
            out_specs=anywhere,
            input_output_aliases={0: 0},
        )(analysis)
        return analysis, inflation.reshape(())

    return jax.shard_map(
        shards,
        mesh=mesh,
        in_specs=(
            P("depth", "member", "region"),
            P("depth"),
            P("region"),
            P("region"),
            P("region"),
            P("member", "region"),
        ),
        out_specs=(P("depth", "member", "region"), P()),
        check_vma=False,
    )
```

```python
import functools

import jax
import jax.numpy as jnp
from jax import lax
from jax.experimental import pallas as pl
from jax.experimental.pallas import tpu as pltpu
from jax.sharding import PartitionSpec as P

RADIUS = 1024
LEAD = 4
READY = 5
PIECES = 2
F32 = jnp.float32
BF16 = jnp.bfloat16
MESH = pl.DeviceIdType.MESH


def kernel(
    sizes,
    weights_hbm,
    ensemble,
    tiles_hbm,
    values_hbm,
    errors_hbm,
    noise,
    out,
    infl_out,
    weights,
    tiles,
    values,
    errors,
    own,
    gathered,
    noise_v,
    part,
    part_in,
    squares,
    tot_in,
    tot_out,
    pos,
    stats,
    obs,
    pert,
    obs_t,
    taper,
    anom,
    means,
    gain,
    result,
    scale,
    infl_v,
    answer,
    small_sem,
    local_sem,
    send_e,
    recv_e,
    send_p,
    recv_p,
    send_q,
    recv_q,
    send_o,
    recv_o,
    send_g,
    recv_g,
    send_y,
    recv_y,
    send_z,
    recv_z,
    send_st,
    recv_st,
    send_pos,
    recv_pos,
    send_ps,
    recv_ps,
    send_pz,
    recv_pz,
    send_pf,
    recv_pf,
    send_f,
    recv_f,
    send_out,
    recv_out,
    own_out,
):
    nr, nd, nm, nl, mm, tt, kk = sizes
    ng = nm // 2
    half = tt // 2
    members = nm * mm
    r = lax.axis_index("region")
    d = lax.axis_index("depth")
    me = lax.axis_index("member")
    q = me // 2
    c = me % 2
    sib = 2 * q + (1 - c)
    has_side = (r > 0, r < nr - 1)

    def dev(region=None, depth=None, member=None):
        return {
            "region": r if region is None else region,
            "depth": d if depth is None else depth,
            "member": me if member is None else member,
        }

    def rdma(src, dst, ssem, rsem, device):
        return pltpu.make_async_remote_copy(
            src_ref=src,
            dst_ref=dst,
            send_sem=ssem,
            recv_sem=rsem,
            device_id=device,
            device_id_type=MESH,
        )

    barrier = pltpu.get_barrier_semaphore()
    for j in range(1, nm):
        pl.semaphore_signal(
            barrier, inc=1, device_id=dev(member=(me + j) % nm), device_id_type=MESH
        )
    for i in range(1, nd):

        @pl.when(d + i < nd)
        def _():
            pl.semaphore_signal(barrier, inc=1, device_id=dev(depth=d + i), device_id_type=MESH)

    @pl.when(has_side[1])
    def _():
        pl.semaphore_signal(barrier, inc=1, device_id=dev(region=r + 1), device_id_type=MESH)

    local_own = pltpu.make_async_copy(ensemble, own, local_sem.at[0])
    local_own.start()
    smalls = [
        pltpu.make_async_copy(a, b, small_sem.at[i])
        for i, (a, b) in enumerate(
            ((weights_hbm, weights), (tiles_hbm, tiles), (values_hbm, values), (errors_hbm, errors))
        )
    ]
    for copy in smalls:
        copy.start()
    local_half = pltpu.make_async_copy(
        ensemble.at[:, :, pl.ds(pl.multiple_of(c * half, 128), half)],
        gathered.at[:, me],
        local_sem.at[1],
    )
    local_half.start()
    local_noise = pltpu.make_async_copy(noise, noise_v, local_sem.at[2])
    local_noise.start()

    pl.semaphore_wait(barrier, nm - 1 + d + (r > 0).astype(jnp.int32))

    piece = half // PIECES
    small = half // 4
    last = nl - 1
    units = (
        [(0, 0, half)]
        + [(1, p * small, small) for p in range(4)]
        + [(l, 0, half) for l in range(2, last)]
        + [(last, p * piece, piece) for p in range(PIECES)]
    )

    def arrival(l, lo):
        return recv_e.at[l + lo // piece] if isinstance(l, int) and l == last else recv_e.at[l]

    def send_bulk(chosen):
        for l, lo, width in chosen:
            for j in range(1, nm):
                to = (me + j) % nm
                rdma(
                    ensemble.at[
                        l, :, pl.ds(pl.multiple_of((to % 2) * half + lo, 128), width)
                    ],
                    gathered.at[l, me, :, pl.ds(lo, width)],
                    send_e.at[0],
                    arrival(l, lo),
                    dev(member=to),
                ).start()

    def wait_bulk(l, lo, width):
        block = gathered.at[l, pl.ds(0, nm - 1), :, pl.ds(lo, width)]
        rdma(block, block, send_e.at[0], arrival(l, lo), dev(member=sib)).wait_recv()

    send_bulk(units[:LEAD])
    for i in range(1, nd):

        @pl.when(d >= i)
        def _():
            pl.semaphore_signal(
                answer.at[0], inc=1, device_id=dev(depth=d - i), device_id_type=MESH
            )

    @pl.when(has_side[0])
    def _():
        pl.semaphore_signal(answer.at[1], inc=1, device_id=dev(region=r - 1), device_id_type=MESH)

    for copy in smalls:
        copy.wait()
    local_own.wait()
    total = own[0].astype(F32) * weights[0]
    for l in range(1, nl):
        total = total + own[l].astype(F32) * weights[l]
    hi = total.astype(BF16)
    rest = total - hi.astype(F32)
    mid = rest.astype(BF16)
    low = (rest - mid.astype(F32)).astype(BF16)
    tile_ids = lax.broadcasted_iota(jnp.int32, (tt, kk), 0)
    onehot = jnp.where(tile_ids == tiles[...], 1.0, 0.0).astype(BF16)
    terms = jnp.dot(
        jnp.concatenate([hi, mid, low], axis=0), onehot, preferred_element_type=F32
    )
    picked = terms[0:mm] + terms[mm : 2 * mm] + terms[2 * mm : 3 * mm]
    part_mean = jnp.sum(picked, axis=0, keepdims=True) / mm
    top = part_mean.astype(BF16).astype(F32)
    second_row = (part_mean - top).astype(BF16).astype(F32)
    third_row = part_mean - top - second_row
    prow = lax.broadcasted_iota(jnp.int32, (16, kk), 0)
    split = jnp.where(prow == 0, top, jnp.where(prow == 1, second_row, third_row))
    part[0:mm] = (picked - part_mean).astype(BF16)
    part[mm : mm + 16] = jnp.where(prow < 3, split, 0.0).astype(BF16)

    def whole(block):
        values_of = block.astype(F32)
        return values_of[0:mm] + jnp.sum(values_of[mm : mm + 16], axis=0, keepdims=True)

    def part_copy(i):
        to = (d + i) % nd
        return rdma(part, part_in.at[d], send_p.at[i], recv_p.at[d], dev(depth=to))

    def part_from(i):
        frm = (d + i) % nd
        return rdma(part, part_in.at[frm], send_p.at[i], recv_p.at[frm], dev(depth=frm))

    @pl.when(d < nd - 1)
    def _():
        pl.semaphore_wait(answer.at[0], nd - 1 - d)

    for i in range(1, nd):
        part_copy(i).start()

    pos[1] = jnp.broadcast_to(tiles[...].astype(F32), (8, kk))

    def pos_copy(side):
        return rdma(
            pos.at[1],
            pos.at[2 - 2 * side],
            send_pos.at[side],
            recv_pos.at[1 - side],
            dev(region=r + (2 * side - 1)),
        )

    def pos_from(side):
        return rdma(
            pos.at[1],
            pos.at[2 * side],
            send_pos.at[side],
            recv_pos.at[side],
            dev(region=r + (2 * side - 1)),
        )

    lane = (lax.broadcasted_iota(jnp.int32, (kk, half), 1) + c * half).astype(F32)

    def make_taper(w):
        position = pos[w].T[:, 0:1] + float((w - 1) * tt)
        close = jnp.maximum(0.0, 1.0 - jnp.abs(lane - position) * (1.0 / RADIUS))
        taper[w * kk : (w + 1) * kk] = close * close

    make_taper(1)

    @pl.when(has_side[1])
    def _():
        pl.semaphore_wait(answer.at[1], 1)

    for side in (0, 1):

        @pl.when(has_side[side])
        def _():
            pos_copy(side).start()

        @pl.when(jnp.logical_not(has_side[side]))
        def _():
            window = 0 if side == 0 else 2 * kk
            obs[:, :, window : window + kk] = jnp.zeros((nm, mm, kk), BF16)
            pert[:, :, window : window + kk] = jnp.zeros((2, mm, kk), BF16)
            stats[2 * side] = jnp.zeros((8, kk), F32)
            pos[2 * side] = jnp.zeros((8, kk), F32)

    predicted = whole(part[...])
    for i in range(1, nd):
        part_from(i).wait_recv()
        predicted = predicted + whole(part_in[(d + i) % nd])
    own_sum = jnp.sum(predicted, axis=0, keepdims=True)
    spread_in = predicted - own_sum / mm
    own_square = jnp.sum(spread_in * spread_in, axis=0, keepdims=True)
    qrow = lax.broadcasted_iota(jnp.int32, (2, kk), 0)
    squares[me] = jnp.where(qrow == 0, own_sum, own_square)
    obs[me, :, kk : 2 * kk] = spread_in.astype(BF16)

    def square_copy(j, slot):
        return rdma(
            squares.at[slot],
            squares.at[slot],
            send_q.at[j],
            recv_q.at[slot],
            dev(member=(me + j) % nm),
        )

    hk = kk // nd

    def obs_at(slot, w, h, width):
        return obs.at[slot, :, pl.ds(pl.multiple_of(w * kk + h * hk, 128), width)]

    def obs_copy(j, slot):
        block = obs_at(slot, 1, d, hk)
        return rdma(block, block, send_o.at[j], recv_o.at[slot], dev(member=(me + j) % nm))

    def obs_swap(g, i, h):
        block = obs_at(cross(g), 1, h, hk)
        return rdma(block, block, send_y.at[g, i], recv_y.at[g, h], dev(depth=(d + i) % nd))

    def side_obs(side, slot, pair, h, width):
        return rdma(
            obs_at(slot, 1, h, width),
            obs_at(slot, 2 if side == 0 else 0, h, width),
            send_z.at[side, pair, h],
            recv_z.at[1 - side, pair, h],
            dev(region=r + (2 * side - 1)),
        )

    def side_from(side, slot, pair, h, width):
        block = obs_at(slot, 2 * side, h, width)
        return rdma(
            block,
            block,
            send_z.at[side, pair, h],
            recv_z.at[side, pair, h],
            dev(region=r + (2 * side - 1)),
        )

    def obs_forward(w, slot, pair, h, width):
        block = obs_at(slot, w, h, width)
        return rdma(
            block, block, send_f.at[w, pair, h], recv_f.at[w, pair, h], dev(member=sib)
        )

    def cross(g):
        return 2 * ((q + g) % ng) + c

    def cross_sib(g):
        return 2 * ((q + g) % ng) + (1 - c)

    for j in range(1, nm):
        square_copy(j, me).start()
    for g in range(1, ng):
        obs_copy(2 * g, me).start()
    obs_forward(1, me, 0, 0, kk).start()
    send_bulk(units[LEAD:])
    for side in (0, 1):

        @pl.when(has_side[side])
        def _():
            side_obs(side, me, 0, 0, kk).start()
            pos_from(side).wait_recv()

        make_taper(2 * side)

    for j in range(1, nm):
        square_copy(j, (me + j) % nm).wait_recv()
    moments = [squares[j] for j in range(nm)]
    obs_mean = sum(m[0:1] for m in moments) / members
    deviation = predicted - obs_mean
    square_sum = sum(
        m[1:2] + mm * (m[0:1] / mm - obs_mean) * (m[0:1] / mm - obs_mean) for m in moments
    )
    spread = square_sum / (members - 1)
    error = errors[...]
    innovation = values[...] - obs_mean
    first = jnp.sum(innovation * innovation, axis=1, keepdims=True)
    second = jnp.sum(spread + error, axis=1, keepdims=True)
    rp = tot_in.shape[1]
    trow = lax.broadcasted_iota(jnp.int32, (rp, 128), 0)
    tlane = lax.broadcasted_iota(jnp.int32, (rp, 128), 1)
    own_total = jnp.where(tlane == 0, first, second)
    krow = lax.broadcasted_iota(jnp.int32, (8, kk), 0)
    shifts_of = jnp.zeros((8, kk), F32)
    for g in range(nm):
        shifts_of = jnp.where(krow == g, moments[g][0:1] / mm - obs_mean, shifts_of)
    stats[1] = shifts_of

    def stat_copy(side):
        return rdma(
            stats.at[1],
            stats.at[2 - 2 * side],
            send_st.at[side],
            recv_st.at[1 - side],
            dev(region=r + (2 * side - 1)),
        )

    def total_copy(way):
        return rdma(
            tot_out.at[way],
            tot_in.at[way],
            send_g.at[way],
            recv_g.at[way],
            dev(region=r + (1 - 2 * way)),
        )

    def total_from(way):
        return rdma(
            tot_out.at[way],
            tot_in.at[way],
            send_g.at[way],
            recv_g.at[way],
            dev(region=r - (1 - 2 * way)),
        )

    def relay(way):
        @pl.when(has_side[way])
        def _():
            total_from(way).wait_recv()

        behind = trow < r if way == 0 else trow > r
        tot_out[way] = jnp.where(
            behind, tot_in[way], jnp.where(trow == r, own_total, 0.0)
        )

        @pl.when(has_side[1 - way])
        def _():
            total_copy(way).start()

    low_end = r == 0
    high_end = r == nr - 1

    @pl.when(low_end)
    def _():
        relay(0)

    @pl.when(high_end)
    def _():
        relay(1)

    for side in (0, 1):

        @pl.when(has_side[side])
        def _():
            stat_copy(side).start()

    def hand_part(g, h):
        for side in (0, 1):

            @pl.when(has_side[side])
            def _():
                side_obs(side, cross(g), g, h, hk).start()

        obs_forward(1, cross(g), g, h, hk).start()

    for g in range(1, ng):
        obs_copy(2 * g, cross(g)).wait_recv()
        for i in range(1, nd):
            obs_swap(g, i, d).start()
        hand_part(g, d)

    def transpose_part(w, h, width):
        at = pl.multiple_of(h * hk, 128)
        rows_of = pl.ds(pl.multiple_of(w * kk + at, 128), width)
        shifts = stats[w, :, pl.ds(at, width)].T
        for g in range(nm):
            block = obs[g, :, rows_of].astype(F32).T + shifts[:, g : g + 1]
            obs_t[rows_of, g * mm : (g + 1) * mm] = block.astype(BF16)

    everything = (0, half)

    def gain_rows(l, windows, columns=everything):
        cols = slice(*columns)
        right = anom[l, :, :, cols].reshape(members, columns[1] - columns[0])
        for w in windows:
            rows_of = slice(w * kk, (w + 1) * kk)
            cov = jnp.dot(obs_t[rows_of], right, preferred_element_type=F32)
            gain[l, rows_of, cols] = (cov * taper[rows_of, cols]).astype(BF16)

    def gain_part(l, h):
        at = pl.ds(pl.multiple_of(kk + h * hk, 128), hk)
        cov = jnp.dot(
            obs_t[at], anom[l].reshape(members, half), preferred_element_type=F32
        )
        gain[l, at] = (cov * taper[at]).astype(BF16)

    def center(l, columns=everything):
        cols = slice(*columns)
        wait_bulk(l, columns[0], columns[1] - columns[0])
        raw = gathered[l, :, :, cols].astype(F32)
        mean = jnp.sum(jnp.sum(raw, axis=0), axis=0, keepdims=True) / members
        means[l, :, cols] = jnp.broadcast_to(mean, (8, columns[1] - columns[0]))
        anom[l, :, :, cols] = (raw - mean[None]).astype(BF16)

    def own_window(l, windows, columns=everything):
        center(l, columns)
        gain_rows(l, windows, columns)

    def sib_pert(slot):
        block = pert.at[slot, :, pl.ds(kk, kk)]
        return rdma(block, block, send_ps.at[0], recv_ps.at[0], dev(member=sib))

    def side_pert(side):
        window = 2 * kk if side == 0 else 0
        return rdma(
            pert.at[c, :, pl.ds(kk, kk)],
            pert.at[c, :, pl.ds(window, kk)],
            send_pz.at[side],
            recv_pz.at[1 - side],
            dev(region=r + (2 * side - 1)),
        )

    def pert_forward(side, slot):
        block = pert.at[slot, :, pl.ds(2 * kk * side, kk)]
        return rdma(block, block, send_pf.at[side], recv_pf.at[side], dev(member=sib))

    def make_pert():
        everyone = jnp.where(trow < r, tot_in[0], jnp.where(trow > r, tot_in[1], own_total))
        grand = everyone[0:1]
        for i in range(1, nr):
            grand = grand + everyone[i : i + 1]
        inflation = grand[0:1, 0:1] / grand[0:1, 1:2]
        root = jnp.sqrt(inflation)
        infl_v[...] = inflation
        pltpu.make_async_copy(infl_v, infl_out, small_sem.at[4]).start()
        scale[...] = jnp.broadcast_to(root, (1, 128))
        factor = inflation / (inflation * spread + error)
        local_noise.wait()
        pert[c, :, kk : 2 * kk] = (
            (innovation + jnp.sqrt(error) * noise_v[...] - root * deviation)
            * (factor / (members - 1))
        ).astype(BF16)

        sib_pert(c).start()
        for side in (0, 1):

            @pl.when(has_side[side])
            def _():
                side_pert(side).start()

    mid_low = jnp.logical_and(r > 0, 2 * r < nr)
    mid_high = jnp.logical_and(r < nr - 1, 2 * r >= nr)

    @pl.when(mid_low)
    def _():
        relay(0)

    @pl.when(mid_high)
    def _():
        relay(1)

    obs_forward(1, sib, 0, 0, kk).wait_recv()
    for g in range(1, ng):
        obs_forward(1, cross_sib(g), g, d, hk).wait_recv()
    transpose_part(1, d, hk)
    local_half.wait()
    center(0)
    gain_part(0, d)
    for i in range(1, nd):
        h = (d + i) % nd
        for g in range(1, ng):
            obs_swap(g, i, h).wait_recv()
            hand_part(g, h)
    center(1)
    gain_part(1, d)
    for i in range(1, nd):
        h = (d + i) % nd
        for g in range(1, ng):
            obs_forward(1, cross_sib(g), g, h, hk).wait_recv()
        transpose_part(1, h, hk)
        gain_part(0, h)
        gain_part(1, h)
    own_window(2, (1,))

    for side in (0, 1):

        @pl.when(has_side[side])
        def _():
            side_from(side, me, 0, 0, kk).wait_recv()
            obs_forward(2 * side, me, 0, 0, kk).start()
            for g in range(1, ng):
                for h in range(nd):
                    side_from(side, cross(g), g, h, hk).wait_recv()
                obs_forward(2 * side, cross(g), g, 0, kk).start()


    @pl.when(mid_low)
    def _():
        relay(1)
        make_pert()

    @pl.when(mid_high)
    def _():
        relay(0)
        make_pert()

    for side in (0, 1):

        @pl.when(has_side[side])
        def _():
            rdma(
                stats.at[1],
                stats.at[2 * side],
                send_st.at[side],
                recv_st.at[side],
                dev(region=r + (2 * side - 1)),
            ).wait_recv()
            for g in range(ng):
                obs_forward(2 * side, cross_sib(g), g, 0, kk).wait_recv()

        transpose_part(2 * side, 0, kk)

    def out_block(l, which, columns):
        lo, width = columns[0], columns[1] - columns[0]
        return out.at[l, :, pl.ds(pl.multiple_of(which * half + lo, 128), width)]

    def out_copies(l, columns):
        cols = slice(*columns)
        there = rdma(
            result.at[l, 1 - c, :, cols],
            out_block(l, c, columns),
            send_out.at[0],
            recv_out.at[0],
            dev(member=sib),
        )
        here = pltpu.make_async_copy(
            result.at[l, c, :, cols], out_block(l, c, columns), own_out.at[0]
        )
        return there, here

    def finish_variable(l, columns=everything):
        cols = slice(*columns)
        width = columns[1] - columns[0]
        increment = jnp.dot(
            pert[...].reshape(2 * mm, 3 * kk), gain[l, :, cols], preferred_element_type=F32
        )
        base = means[l, 0:1, cols][None] + root[None] * anom[l, pl.ds(2 * q, 2), :, cols].astype(F32)
        result[l, :, :, cols] = (base + increment.reshape(2, mm, width)).astype(BF16)
        for copy in out_copies(l, columns):
            copy.start()

    def side_gain(l, carry):
        gain_rows(l, (0, 2))
        return carry

    lax.fori_loop(0, 3, side_gain, 0)

    @pl.when(low_end)
    def _():
        relay(1)
        make_pert()

    @pl.when(high_end)
    def _():
        relay(0)
        make_pert()

    own_window(3, (0, 1, 2))
    for side in (0, 1):

        @pl.when(has_side[side])
        def _():
            side_pert(1 - side).wait_recv()
            pert_forward(side, c).start()

    root = scale[0:1, 0:1]
    ready = min(READY, last)

    def ahead(l, carry):
        own_window(l, (0, 1, 2))
        return carry

    lax.fori_loop(4, ready, ahead, 0)
    sib_pert(1 - c).wait_recv()
    for side in (0, 1):

        @pl.when(has_side[side])
        def _():
            pert_forward(side, 1 - c).wait_recv()

    def late_variable(l, carry):
        finish_variable(l)
        return carry

    lax.fori_loop(0, ready, late_variable, 0)

    def one_variable(l, carry):
        own_window(l, (0, 1, 2))
        finish_variable(l)
        return carry

    lax.fori_loop(ready, last, one_variable, 0)
    for p in range(PIECES):
        columns = (p * piece, (p + 1) * piece)
        own_window(last, (0, 1, 2), columns)
        finish_variable(last, columns)

    sent = gathered.at[:, pl.ds(0, nm - 1)]
    rdma(sent, sent, send_e.at[0], recv_e.at[0], dev(member=sib)).wait_send()
    mine = out.at[:, :, pl.ds(pl.multiple_of(c * half, 128), half)]
    other = out.at[:, :, pl.ds(pl.multiple_of((1 - c) * half, 128), half)]
    pltpu.make_async_copy(mine, mine, own_out.at[0]).wait()
    theirs = rdma(other, other, send_out.at[0], recv_out.at[0], dev(member=sib))
    theirs.wait_send()
    theirs.wait_recv()
    pltpu.make_async_copy(infl_v, infl_out, small_sem.at[4]).wait()
    for i in range(1, nd):
        part_copy(i).wait_send()
    for j in range(1, nm):
        square_copy(j, me).wait_send()
    for g in range(1, ng):
        obs_copy(2 * g, me).wait_send()
    obs_forward(1, me, 0, 0, kk).wait_send()
    for g in range(1, ng):
        for i in range(1, nd):
            obs_swap(g, i, d).wait_send()
        for h in range(nd):
            obs_forward(1, cross(g), g, h, hk).wait_send()
    sib_pert(c).wait_send()
    for way in (0, 1):

        @pl.when(has_side[1 - way])
        def _():
            total_copy(way).wait_send()

    for side in (0, 1):

        @pl.when(has_side[side])
        def _():
            side_obs(side, me, 0, 0, kk).wait_send()
            obs_forward(2 * side, me, 0, 0, kk).wait_send()
            for g in range(1, ng):
                for h in range(nd):
                    side_obs(side, cross(g), g, h, hk).wait_send()
                obs_forward(2 * side, cross(g), g, 0, kk).wait_send()
            side_pert(side).wait_send()
            pert_forward(side, c).wait_send()
            stat_copy(side).wait_send()
            pos_copy(side).wait_send()


def hand_on(block, out):
    pass


def solution(mesh):
    nr, nd, nm = (mesh.shape[a] for a in ("region", "depth", "member"))

    def shards(ensemble, obs_weights, obs_tiles, obs_values, obs_error, obs_noise):
        nl, mm, tt = ensemble.shape
        kk = obs_tiles.shape[0]
        ng = nm // 2
        half = tt // 2
        rp = -(-nr // 8) * 8
        dma = pltpu.SemaphoreType.DMA
        vmem = pl.BlockSpec(memory_space=pltpu.VMEM)
        anywhere = pl.BlockSpec(memory_space=pl.ANY)
        analysis, inflation = pl.pallas_call(
            functools.partial(kernel, (nr, nd, nm, nl, mm, tt, kk)),
            out_shape=(
                pltpu.VMEM((nl, mm, tt), BF16),
                jax.ShapeDtypeStruct((1, 1), F32),
            ),
            in_specs=[anywhere] * 6,
            out_specs=(vmem, anywhere),
            scratch_shapes=[
                pltpu.SMEM((nl,), F32),
                pltpu.VMEM((1, kk), jnp.int32),
                pltpu.VMEM((1, kk), F32),
                pltpu.VMEM((1, kk), F32),
                pltpu.VMEM((nl, mm, tt), BF16),
                pltpu.VMEM((nl, nm, mm, half), BF16),
                pltpu.VMEM((mm, kk), F32),
                pltpu.VMEM((mm + 16, kk), BF16),
                pltpu.VMEM((nd, mm + 16, kk), BF16),
                pltpu.VMEM((nm, 2, kk), F32),
                pltpu.VMEM((2, rp, 128), F32),
                pltpu.VMEM((2, rp, 128), F32),
                pltpu.VMEM((3, 8, kk), F32),
                pltpu.VMEM((3, 8, kk), F32),
                pltpu.VMEM((nm, mm, 3 * kk), BF16),
                pltpu.VMEM((2, mm, 3 * kk), BF16),
                pltpu.VMEM((3 * kk, nm * mm), BF16),
                pltpu.VMEM((3 * kk, half), F32),
                pltpu.VMEM((nl, nm, mm, half), BF16),
                pltpu.VMEM((nl, 8, half), F32),
                pltpu.VMEM((nl, 3 * kk, half), BF16),
                pltpu.VMEM((nl, 2, mm, half), BF16),
                pltpu.VMEM((1, 128), F32),
                pltpu.VMEM((1, 1), F32),
                pltpu.SemaphoreType.REGULAR((2,)),
                dma((5,)),
                dma((3,)),
                dma((1,)),
                dma((nl - 1 + PIECES,)),
                dma((nd,)),
                dma((nd,)),
                dma((nm,)),
                dma((nm,)),
                dma((nm,)),
                dma((nm,)),
                dma((2,)),
                dma((2,)),
                dma((ng, nd)),
                dma((ng, nd)),
                dma((2, ng, nd)),
                dma((2, ng, nd)),
                dma((2,)),
                dma((2,)),
                dma((2,)),
                dma((2,)),
                dma((1,)),
                dma((1,)),
                dma((2,)),
                dma((2,)),
                dma((2,)),
                dma((2,)),
                dma((3, ng, nd)),
                dma((3, ng, nd)),
                dma((1,)),
                dma((1,)),
                dma((1,)),
            ],
            compiler_params=pltpu.CompilerParams(
                collective_id=0, has_side_effects=True, vmem_limit_bytes=56 * 1024 * 1024
            ),
        )(
            obs_weights,
            ensemble,
            obs_tiles.reshape(1, kk),
            obs_values.reshape(1, kk),
            obs_error.reshape(1, kk),
            obs_noise,
        )
        analysis = pl.pallas_call(
            hand_on,
            out_shape=jax.ShapeDtypeStruct((nl, mm, tt), BF16),
            in_specs=[anywhere],
            out_specs=anywhere,
            input_output_aliases={0: 0},
        )(analysis)
        return analysis, inflation.reshape(())

    return jax.shard_map(
        shards,
        mesh=mesh,
        in_specs=(
            P("depth", "member", "region"),
            P("depth"),
            P("region"),
            P("region"),
            P("region"),
            P("member", "region"),
        ),
        out_specs=(P("depth", "member", "region"), P()),
        check_vma=False,
    )
```

```python
import functools

import jax
import jax.numpy as jnp
from jax import lax
from jax.experimental import pallas as pl
from jax.experimental.pallas import tpu as pltpu
from jax.sharding import PartitionSpec as P

RADIUS = 1024
LEAD = 4
READY = 4
PIECES = 2
F32 = jnp.float32
BF16 = jnp.bfloat16
MESH = pl.DeviceIdType.MESH


def kernel(
    sizes,
    weights_hbm,
    ensemble,
    tiles_hbm,
    values_hbm,
    errors_hbm,
    noise,
    out,
    infl_out,
    weights,
    tiles,
    values,
    errors,
    own,
    gathered,
    noise_v,
    part,
    part_in,
    squares,
    tot_in,
    tot_out,
    pos,
    stats,
    obs,
    pert,
    obs_t,
    taper,
    anom,
    means,
    gain,
    result,
    scale,
    infl_v,
    answer,
    small_sem,
    local_sem,
    send_e,
    recv_e,
    send_p,
    recv_p,
    send_q,
    recv_q,
    send_o,
    recv_o,
    send_g,
    recv_g,
    send_y,
    recv_y,
    send_z,
    recv_z,
    send_st,
    recv_st,
    recv_pos,
    send_ps,
    recv_ps,
    send_pz,
    recv_pz,
    send_pf,
    recv_pf,
    send_f,
    recv_f,
    send_out,
    recv_out,
    own_out,
):
    nr, nd, nm, nl, mm, tt, kk = sizes
    ng = nm // 2
    half = tt // 2
    members = nm * mm
    r = lax.axis_index("region")
    d = lax.axis_index("depth")
    me = lax.axis_index("member")
    q = me // 2
    c = me % 2
    sib = 2 * q + (1 - c)
    has_side = (r > 0, r < nr - 1)

    def dev(region=None, depth=None, member=None):
        return {
            "region": r if region is None else region,
            "depth": d if depth is None else depth,
            "member": me if member is None else member,
        }

    def rdma(src, dst, ssem, rsem, device):
        return pltpu.make_async_remote_copy(
            src_ref=src,
            dst_ref=dst,
            send_sem=ssem,
            recv_sem=rsem,
            device_id=device,
            device_id_type=MESH,
        )

    barrier = pltpu.get_barrier_semaphore()
    for j in range(1, nm):
        pl.semaphore_signal(
            barrier, inc=1, device_id=dev(member=(me + j) % nm), device_id_type=MESH
        )
    for i in range(1, nd):

        @pl.when(d + i < nd)
        def _():
            pl.semaphore_signal(barrier, inc=1, device_id=dev(depth=d + i), device_id_type=MESH)

    @pl.when(has_side[1])
    def _():
        pl.semaphore_signal(barrier, inc=1, device_id=dev(region=r + 1), device_id_type=MESH)

    local_own = pltpu.make_async_copy(ensemble, own, local_sem.at[0])
    local_own.start()
    smalls = [
        pltpu.make_async_copy(a, b, small_sem.at[i])
        for i, (a, b) in enumerate(
            ((weights_hbm, weights), (tiles_hbm, tiles), (values_hbm, values), (errors_hbm, errors))
        )
    ]
    for copy in smalls:
        copy.start()
    local_half = pltpu.make_async_copy(
        ensemble.at[:, :, pl.ds(pl.multiple_of(c * half, 128), half)],
        gathered.at[:, me],
        local_sem.at[1],
    )
    local_half.start()
    local_noise = pltpu.make_async_copy(noise, noise_v, local_sem.at[2])
    local_noise.start()

    pl.semaphore_wait(barrier, nm - 1 + d + (r > 0).astype(jnp.int32))

    piece = half // PIECES
    small = half // 4
    last = nl - 1
    units = (
        [(0, 0, half)]
        + [(1, p * small, small) for p in range(4)]
        + [(l, 0, half) for l in range(2, last)]
        + [(last, p * piece, piece) for p in range(PIECES)]
    )

    def arrival(l, lo):
        return recv_e.at[l + lo // piece] if isinstance(l, int) and l == last else recv_e.at[l]

    def send_bulk(chosen):
        for l, lo, width in chosen:
            for j in range(1, nm):
                to = (me + j) % nm
                rdma(
                    ensemble.at[
                        l, :, pl.ds(pl.multiple_of((to % 2) * half + lo, 128), width)
                    ],
                    gathered.at[l, me, :, pl.ds(lo, width)],
                    send_e.at[0],
                    arrival(l, lo),
                    dev(member=to),
                ).start()

    def wait_bulk(l, lo, width):
        block = gathered.at[l, pl.ds(0, nm - 1), :, pl.ds(lo, width)]
        rdma(block, block, send_e.at[0], arrival(l, lo), dev(member=sib)).wait_recv()

    send_bulk(units[:LEAD])
    for i in range(1, nd):

        @pl.when(d >= i)
        def _():
            pl.semaphore_signal(
                answer.at[0], inc=1, device_id=dev(depth=d - i), device_id_type=MESH
            )

    @pl.when(has_side[0])
    def _():
        pl.semaphore_signal(answer.at[1], inc=1, device_id=dev(region=r - 1), device_id_type=MESH)

    for copy in smalls:
        copy.wait()
    local_own.wait()
    total = own[0].astype(F32) * weights[0]
    for l in range(1, nl):
        total = total + own[l].astype(F32) * weights[l]
    hi = total.astype(BF16)
    rest = total - hi.astype(F32)
    mid = rest.astype(BF16)
    low = (rest - mid.astype(F32)).astype(BF16)
    tile_ids = lax.broadcasted_iota(jnp.int32, (tt, kk), 0)
    onehot = jnp.where(tile_ids == tiles[...], 1.0, 0.0).astype(BF16)
    terms = jnp.dot(
        jnp.concatenate([hi, mid, low], axis=0), onehot, preferred_element_type=F32
    )
    picked = terms[0:mm] + terms[mm : 2 * mm] + terms[2 * mm : 3 * mm]
    part_mean = jnp.sum(picked, axis=0, keepdims=True) / mm
    top = part_mean.astype(BF16).astype(F32)
    second_row = (part_mean - top).astype(BF16).astype(F32)
    third_row = part_mean - top - second_row
    prow = lax.broadcasted_iota(jnp.int32, (16, kk), 0)
    split = jnp.where(prow == 0, top, jnp.where(prow == 1, second_row, third_row))
    part[0:mm] = (picked - part_mean).astype(BF16)
    part[mm : mm + 16] = jnp.where(prow < 3, split, 0.0).astype(BF16)

    def whole(block):
        values_of = block.astype(F32)
        return values_of[0:mm] + jnp.sum(values_of[mm : mm + 16], axis=0, keepdims=True)

    def part_copy(i):
        to = (d + i) % nd
        return rdma(part, part_in.at[d], send_p.at[i - 1], recv_p.at[i - 1], dev(depth=to))

    def part_from(i):
        frm = (d + i) % nd
        return rdma(
            part, part_in.at[frm], send_p.at[i - 1], recv_p.at[nd - i - 1], dev(depth=frm)
        )

    @pl.when(d < nd - 1)
    def _():
        pl.semaphore_wait(answer.at[0], nd - 1 - d)

    for i in range(1, nd):
        part_copy(i).start()

    pos[1] = jnp.broadcast_to(tiles[...].astype(F32), (8, kk))

    def pos_copy(side):
        return rdma(
            pos.at[1],
            pos.at[2 - 2 * side],
            send_st.at[side],
            recv_pos.at[1 - side],
            dev(region=r + (2 * side - 1)),
        )

    def pos_from(side):
        return rdma(
            pos.at[1],
            pos.at[2 * side],
            send_st.at[side],
            recv_pos.at[side],
            dev(region=r + (2 * side - 1)),
        )

    lane = (lax.broadcasted_iota(jnp.int32, (kk, half), 1) + c * half).astype(F32)

    def make_taper(w):
        position = pos[w].T[:, 0:1] + float((w - 1) * tt)
        close = jnp.maximum(0.0, 1.0 - jnp.abs(lane - position) * (1.0 / RADIUS))
        taper[w * kk : (w + 1) * kk] = close * close

    make_taper(1)

    @pl.when(has_side[1])
    def _():
        pl.semaphore_wait(answer.at[1], 1)

    for side in (0, 1):

        @pl.when(has_side[side])
        def _():
            pos_copy(side).start()

        @pl.when(jnp.logical_not(has_side[side]))
        def _():
            window = 0 if side == 0 else 2 * kk
            obs[:, :, window : window + kk] = jnp.zeros((nm, mm, kk), BF16)
            pert[:, :, window : window + kk] = jnp.zeros((2, mm, kk), BF16)
            stats[2 * side] = jnp.zeros((8, kk), F32)
            pos[2 * side] = jnp.zeros((8, kk), F32)

    predicted = whole(part[...])
    for i in range(1, nd):
        part_from(i).wait_recv()
        predicted = predicted + whole(part_in[(d + i) % nd])
    own_sum = jnp.sum(predicted, axis=0, keepdims=True)
    spread_in = predicted - own_sum / mm
    own_square = jnp.sum(spread_in * spread_in, axis=0, keepdims=True)
    qrow = lax.broadcasted_iota(jnp.int32, (2, kk), 0)
    squares[me] = jnp.where(qrow == 0, own_sum, own_square)
    obs[me, :, kk : 2 * kk] = spread_in.astype(BF16)

    def square_copy(j):
        return rdma(
            squares.at[me],
            squares.at[me],
            send_q.at[0],
            recv_q.at[0],
            dev(member=(me + j) % nm),
        )

    square_rest = squares.at[pl.ds(0, nm - 1)]
    square_all = rdma(square_rest, square_rest, send_q.at[0], recv_q.at[0], dev(member=sib))

    hk = kk // nd

    def obs_at(slot, w, h, width):
        return obs.at[slot, :, pl.ds(pl.multiple_of(w * kk + h * hk, 128), width)]

    def obs_copy(g):
        block = obs_at(me, 1, d, hk)
        return rdma(
            block, block, send_o.at[g - 1], recv_o.at[g - 1], dev(member=(me + 2 * g) % nm)
        )

    def obs_from(g):
        block = obs_at(cross(g), 1, d, hk)
        return rdma(block, block, send_o.at[g - 1], recv_o.at[ng - g - 1], dev(member=sib))

    def obs_swap(g, i):
        block = obs_at(cross(g), 1, d, hk)
        return rdma(
            block, block, send_y.at[g - 1, i - 1], recv_y.at[g - 1, i - 1], dev(depth=(d + i) % nd)
        )

    def swap_from(g, i):
        h = (d + i) % nd
        block = obs_at(cross(g), 1, h, hk)
        return rdma(
            block, block, send_y.at[g - 1, i - 1], recv_y.at[g - 1, nd - i - 1], dev(depth=h)
        )

    def side_obs(side, slot, h, width):
        return rdma(
            obs_at(slot, 1, h, width),
            obs_at(slot, 2 if side == 0 else 0, h, width),
            send_z.at[side],
            recv_z.at[1 - side],
            dev(region=r + (2 * side - 1)),
        )

    def side_all(side):
        block = obs.at[pl.ds(0, ng), :, pl.ds(kk, kk)]
        return rdma(
            block, block, send_z.at[side], recv_z.at[side], dev(region=r + (2 * side - 1))
        )

    def obs_forward(w, slot, h, width, number):
        block = obs_at(slot, w, h, width)
        return rdma(block, block, send_f.at[w], recv_f.at[number], dev(member=sib))

    def forward_all(w, wide, number):
        block = obs.at[pl.ds(0, wide[0]), :, pl.ds(0, wide[1])]
        return rdma(block, block, send_f.at[w], recv_f.at[number], dev(member=sib))

    def cross(g):
        return 2 * ((q + g) % ng) + c

    for j in range(1, nm):
        square_copy(j).start()
    for g in range(1, ng):
        obs_copy(g).start()
    obs_forward(1, me, 0, kk, 0).start()
    send_bulk(units[LEAD:])
    for side in (0, 1):

        @pl.when(has_side[side])
        def _():
            side_obs(side, me, 0, kk).start()
            pos_from(side).wait_recv()

        make_taper(2 * side)

    square_all.wait_recv()
    moments = [squares[j] for j in range(nm)]
    obs_mean = sum(m[0:1] for m in moments) / members
    deviation = predicted - obs_mean
    square_sum = sum(
        m[1:2] + mm * (m[0:1] / mm - obs_mean) * (m[0:1] / mm - obs_mean) for m in moments
    )
    spread = square_sum / (members - 1)
    error = errors[...]
    innovation = values[...] - obs_mean
    first = jnp.sum(innovation * innovation, axis=1, keepdims=True)
    second = jnp.sum(spread + error, axis=1, keepdims=True)
    rp = tot_in.shape[1]
    trow = lax.broadcasted_iota(jnp.int32, (rp, 128), 0)
    tlane = lax.broadcasted_iota(jnp.int32, (rp, 128), 1)
    own_total = jnp.where(tlane == 0, first, second)
    krow = lax.broadcasted_iota(jnp.int32, (8, kk), 0)
    shifts_of = jnp.zeros((8, kk), F32)
    for g in range(nm):
        shifts_of = jnp.where(krow == g, moments[g][0:1] / mm - obs_mean, shifts_of)
    stats[1] = shifts_of

    def stat_copy(side):
        return rdma(
            stats.at[1],
            stats.at[2 - 2 * side],
            send_st.at[side],
            recv_st.at[1 - side],
            dev(region=r + (2 * side - 1)),
        )

    def total_copy(way):
        return rdma(
            tot_out.at[way],
            tot_in.at[way],
            send_g.at[way],
            recv_g.at[way],
            dev(region=r + (1 - 2 * way)),
        )

    def total_from(way):
        return rdma(
            tot_out.at[way],
            tot_in.at[way],
            send_g.at[way],
            recv_g.at[way],
            dev(region=r - (1 - 2 * way)),
        )

    def relay(way):
        @pl.when(has_side[way])
        def _():
            total_from(way).wait_recv()

        behind = trow < r if way == 0 else trow > r
        tot_out[way] = jnp.where(
            behind, tot_in[way], jnp.where(trow == r, own_total, 0.0)
        )

        @pl.when(has_side[1 - way])
        def _():
            total_copy(way).start()

    low_end = r == 0
    high_end = r == nr - 1

    @pl.when(low_end)
    def _():
        relay(0)

    @pl.when(high_end)
    def _():
        relay(1)

    for side in (0, 1):

        @pl.when(has_side[side])
        def _():
            stat_copy(side).start()

    def hand_part(g, i):
        h = (d + i) % nd
        for side in (0, 1):

            @pl.when(has_side[side])
            def _():
                side_obs(side, cross(g), h, hk).start()

        obs_forward(1, cross(g), h, hk, i).start()

    for g in range(1, ng):
        obs_from(g).wait_recv()
        for i in range(1, nd):
            obs_swap(g, i).start()
        hand_part(g, 0)

    def transpose_part(w, h, width):
        at = pl.multiple_of(h * hk, 128)
        rows_of = pl.ds(pl.multiple_of(w * kk + at, 128), width)
        shifts = stats[w, :, pl.ds(at, width)].T
        for g in range(nm):
            block = obs[g, :, rows_of].astype(F32).T + shifts[:, g : g + 1]
            obs_t[rows_of, g * mm : (g + 1) * mm] = block.astype(BF16)

    everything = (0, half)

    def gain_rows(l, windows, columns=everything):
        cols = slice(*columns)
        right = anom[l, :, :, cols].reshape(members, columns[1] - columns[0])
        for w in windows:
            rows_of = slice(w * kk, (w + 1) * kk)
            cov = jnp.dot(obs_t[rows_of], right, preferred_element_type=F32)
            gain[l, rows_of, cols] = (cov * taper[rows_of, cols]).astype(BF16)

    def gain_part(l, h):
        at = pl.ds(pl.multiple_of(kk + h * hk, 128), hk)
        cov = jnp.dot(
            obs_t[at], anom[l].reshape(members, half), preferred_element_type=F32
        )
        gain[l, at] = (cov * taper[at]).astype(BF16)

    def center(l, columns=everything):
        cols = slice(*columns)
        wait_bulk(l, columns[0], columns[1] - columns[0])
        raw = gathered[l, :, :, cols].astype(F32)
        mean = jnp.sum(jnp.sum(raw, axis=0), axis=0, keepdims=True) / members
        means[l, :, cols] = jnp.broadcast_to(mean, (8, columns[1] - columns[0]))
        anom[l, :, :, cols] = (raw - mean[None]).astype(BF16)

    def own_window(l, windows, columns=everything):
        center(l, columns)
        gain_rows(l, windows, columns)

    def sib_pert(slot):
        block = pert.at[slot, :, pl.ds(kk, kk)]
        return rdma(block, block, send_ps.at[0], recv_ps.at[0], dev(member=sib))

    def side_pert(side):
        window = 2 * kk if side == 0 else 0
        return rdma(
            pert.at[c, :, pl.ds(kk, kk)],
            pert.at[c, :, pl.ds(window, kk)],
            send_pz.at[side],
            recv_pz.at[1 - side],
            dev(region=r + (2 * side - 1)),
        )

    def pert_forward(side, slot):
        block = pert.at[slot, :, pl.ds(2 * kk * side, kk)]
        return rdma(block, block, send_pf.at[side], recv_pf.at[side], dev(member=sib))

    def make_pert():
        everyone = jnp.where(trow < r, tot_in[0], jnp.where(trow > r, tot_in[1], own_total))
        grand = everyone[0:1]
        for i in range(1, nr):
            grand = grand + everyone[i : i + 1]
        inflation = grand[0:1, 0:1] / grand[0:1, 1:2]
        root = jnp.sqrt(inflation)
        infl_v[...] = inflation
        pltpu.make_async_copy(infl_v, infl_out, small_sem.at[4]).start()
        scale[...] = jnp.broadcast_to(root, (1, 128))
        factor = inflation / (inflation * spread + error)
        local_noise.wait()
        pert[c, :, kk : 2 * kk] = (
            (innovation + jnp.sqrt(error) * noise_v[...] - root * deviation)
            * (factor / (members - 1))
        ).astype(BF16)

        sib_pert(c).start()
        for side in (0, 1):

            @pl.when(has_side[side])
            def _():
                side_pert(side).start()

    mid_low = jnp.logical_and(r > 0, 2 * r < nr)
    mid_high = jnp.logical_and(r < nr - 1, 2 * r >= nr)

    @pl.when(mid_low)
    def _():
        relay(0)

    @pl.when(mid_high)
    def _():
        relay(1)

    forward_all(1, (1, kk + (ng - 1) * hk), 0).wait_recv()
    transpose_part(1, d, hk)
    local_half.wait()
    center(0)
    gain_part(0, d)
    for i in range(1, nd):
        for g in range(1, ng):
            swap_from(g, i).wait_recv()
            hand_part(g, i)
    center(1)
    gain_part(1, d)

    @pl.when(mid_low)
    def _():
        relay(1)
        make_pert()

    @pl.when(mid_high)
    def _():
        relay(0)
        make_pert()

    for i in range(1, nd):
        h = (d + i) % nd
        forward_all(1, (1, (ng - 1) * hk), i).wait_recv()
        transpose_part(1, h, hk)
        gain_part(0, h)
        gain_part(1, h)
    own_window(2, (1,))

    for side in (0, 1):

        @pl.when(has_side[side])
        def _():
            side_all(side).wait_recv()
            for g in range(ng):
                obs_forward(2 * side, cross(g), 0, kk, nd + side).start()


    @pl.when(low_end)
    def _():
        relay(1)
        make_pert()

    @pl.when(high_end)
    def _():
        relay(0)
        make_pert()

    for side in (0, 1):

        @pl.when(has_side[side])
        def _():
            rdma(
                stats.at[1],
                stats.at[2 * side],
                send_st.at[side],
                recv_st.at[side],
                dev(region=r + (2 * side - 1)),
            ).wait_recv()
            forward_all(2 * side, (ng, kk), nd + side).wait_recv()

        transpose_part(2 * side, 0, kk)

    def out_block(l, which, columns):
        lo, width = columns[0], columns[1] - columns[0]
        return out.at[l, :, pl.ds(pl.multiple_of(which * half + lo, 128), width)]

    def out_copies(l, columns):
        cols = slice(*columns)
        there = rdma(
            result.at[l, 1 - c, :, cols],
            out_block(l, c, columns),
            send_out.at[0],
            recv_out.at[0],
            dev(member=sib),
        )
        here = pltpu.make_async_copy(
            result.at[l, c, :, cols], out_block(l, c, columns), own_out.at[0]
        )
        return there, here

    def finish_variable(l, columns=everything):
        cols = slice(*columns)
        width = columns[1] - columns[0]
        increment = jnp.dot(
            pert[...].reshape(2 * mm, 3 * kk), gain[l, :, cols], preferred_element_type=F32
        )
        base = means[l, 0:1, cols][None] + root[None] * anom[l, pl.ds(2 * q, 2), :, cols].astype(F32)
        result[l, :, :, cols] = (base + increment.reshape(2, mm, width)).astype(BF16)
        for copy in out_copies(l, columns):
            copy.start()

    def side_gain(l, carry):
        gain_rows(l, (0, 2))
        return carry

    lax.fori_loop(0, 3, side_gain, 0)

    for side in (0, 1):

        @pl.when(has_side[side])
        def _():
            side_pert(1 - side).wait_recv()
            pert_forward(side, c).start()

    own_window(3, (0, 1, 2))

    root = scale[0:1, 0:1]
    ready = min(READY, last)

    def ahead(l, carry):
        own_window(l, (0, 1, 2))
        return carry

    lax.fori_loop(4, ready, ahead, 0)
    sib_pert(1 - c).wait_recv()
    for side in (0, 1):

        @pl.when(has_side[side])
        def _():
            pert_forward(side, 1 - c).wait_recv()

    def late_variable(l, carry):
        finish_variable(l)
        return carry

    lax.fori_loop(0, ready, late_variable, 0)

    def one_variable(l, carry):
        own_window(l, (0, 1, 2))
        finish_variable(l)
        return carry

    lax.fori_loop(ready, last, one_variable, 0)
    for p in range(PIECES):
        columns = (p * piece, (p + 1) * piece)
        own_window(last, (0, 1, 2), columns)
        finish_variable(last, columns)

    sent = gathered.at[:, pl.ds(0, nm - 1)]
    rdma(sent, sent, send_e.at[0], recv_e.at[0], dev(member=sib)).wait_send()
    mine = out.at[:, :, pl.ds(pl.multiple_of(c * half, 128), half)]
    other = out.at[:, :, pl.ds(pl.multiple_of((1 - c) * half, 128), half)]
    pltpu.make_async_copy(mine, mine, own_out.at[0]).wait()
    theirs = rdma(other, other, send_out.at[0], recv_out.at[0], dev(member=sib))
    theirs.wait_send()
    theirs.wait_recv()
    pltpu.make_async_copy(infl_v, infl_out, small_sem.at[4]).wait()
    for i in range(1, nd):
        part_copy(i).wait_send()
    square_all.wait_send()
    for g in range(1, ng):
        obs_copy(g).wait_send()
        for i in range(1, nd):
            obs_swap(g, i).wait_send()
    forward_all(1, (ng, kk), 0).wait_send()
    sib_pert(c).wait_send()
    for way in (0, 1):

        @pl.when(has_side[1 - way])
        def _():
            total_copy(way).wait_send()

    for side in (0, 1):

        @pl.when(has_side[side])
        def _():
            side_all(side).wait_send()
            forward_all(2 * side, (ng, kk), nd + side).wait_send()
            side_pert(side).wait_send()
            pert_forward(side, c).wait_send()
            both = stats.at[pl.ds(0, 2)]
            rdma(
                both, both, send_st.at[side], recv_st.at[side], dev(region=r + (2 * side - 1))
            ).wait_send()


def hand_on(block, out):
    pass


def solution(mesh):
    nr, nd, nm = (mesh.shape[a] for a in ("region", "depth", "member"))

    def shards(ensemble, obs_weights, obs_tiles, obs_values, obs_error, obs_noise):
        nl, mm, tt = ensemble.shape
        kk = obs_tiles.shape[0]
        ng = nm // 2
        half = tt // 2
        rp = -(-nr // 8) * 8
        dma = pltpu.SemaphoreType.DMA
        vmem = pl.BlockSpec(memory_space=pltpu.VMEM)
        anywhere = pl.BlockSpec(memory_space=pl.ANY)
        analysis, inflation = pl.pallas_call(
            functools.partial(kernel, (nr, nd, nm, nl, mm, tt, kk)),
            out_shape=(
                pltpu.VMEM((nl, mm, tt), BF16),
                jax.ShapeDtypeStruct((1, 1), F32),
            ),
            in_specs=[anywhere] * 6,
            out_specs=(vmem, anywhere),
            scratch_shapes=[
                pltpu.SMEM((nl,), F32),
                pltpu.VMEM((1, kk), jnp.int32),
                pltpu.VMEM((1, kk), F32),
                pltpu.VMEM((1, kk), F32),
                pltpu.VMEM((nl, mm, tt), BF16),
                pltpu.VMEM((nl, nm, mm, half), BF16),
                pltpu.VMEM((mm, kk), F32),
                pltpu.VMEM((mm + 16, kk), BF16),
                pltpu.VMEM((nd, mm + 16, kk), BF16),
                pltpu.VMEM((nm, 2, kk), F32),
                pltpu.VMEM((2, rp, 128), F32),
                pltpu.VMEM((2, rp, 128), F32),
                pltpu.VMEM((3, 8, kk), F32),
                pltpu.VMEM((3, 8, kk), F32),
                pltpu.VMEM((nm, mm, 3 * kk), BF16),
                pltpu.VMEM((2, mm, 3 * kk), BF16),
                pltpu.VMEM((3 * kk, nm * mm), BF16),
                pltpu.VMEM((3 * kk, half), F32),
                pltpu.VMEM((nl, nm, mm, half), BF16),
                pltpu.VMEM((nl, 8, half), F32),
                pltpu.VMEM((nl, 3 * kk, half), BF16),
                pltpu.VMEM((nl, 2, mm, half), BF16),
                pltpu.VMEM((1, 128), F32),
                pltpu.VMEM((1, 1), F32),
                pltpu.SemaphoreType.REGULAR((2,)),
                dma((5,)),
                dma((3,)),
                dma((1,)),
                dma((nl - 1 + PIECES,)),
                dma((nd - 1,)),
                dma((nd - 1,)),
                dma((1,)),
                dma((1,)),
                dma((ng - 1,)),
                dma((ng - 1,)),
                dma((2,)),
                dma((2,)),
                dma((ng - 1, nd - 1)),
                dma((ng - 1, nd - 1)),
                dma((2,)),
                dma((2,)),
                dma((2,)),
                dma((2,)),
                dma((2,)),
                dma((1,)),
                dma((1,)),
                dma((2,)),
                dma((2,)),
                dma((2,)),
                dma((2,)),
                dma((3,)),
                dma((nd + 2,)),
                dma((1,)),
                dma((1,)),
                dma((1,)),
            ],
            compiler_params=pltpu.CompilerParams(
                collective_id=0, has_side_effects=True, vmem_limit_bytes=56 * 1024 * 1024
            ),
        )(
            obs_weights,
            ensemble,
            obs_tiles.reshape(1, kk),
            obs_values.reshape(1, kk),
            obs_error.reshape(1, kk),
            obs_noise,
        )
        analysis = pl.pallas_call(
            hand_on,
            out_shape=jax.ShapeDtypeStruct((nl, mm, tt), BF16),
            in_specs=[anywhere],
            out_specs=anywhere,
            input_output_aliases={0: 0},
        )(analysis)
        return analysis, inflation.reshape(())

    return jax.shard_map(
        shards,
        mesh=mesh,
        in_specs=(
            P("depth", "member", "region"),
            P("depth"),
            P("region"),
            P("region"),
            P("region"),
            P("member", "region"),
        ),
        out_specs=(P("depth", "member", "region"), P()),
        check_vma=False,
    )
```

```python
import functools

import jax
import jax.numpy as jnp
from jax import lax
from jax.experimental import pallas as pl
from jax.experimental.pallas import tpu as pltpu
from jax.sharding import PartitionSpec as P

RADIUS = 1024
LEAD = 2
READY = 4
PIECES = 2
F32 = jnp.float32
BF16 = jnp.bfloat16
MESH = pl.DeviceIdType.MESH


def kernel(
    sizes,
    weights_hbm,
    ensemble,
    tiles_hbm,
    values_hbm,
    errors_hbm,
    noise,
    out,
    infl_out,
    weights,
    tiles,
    values,
    errors,
    own,
    gathered,
    noise_v,
    part,
    part_in,
    squares,
    tot_in,
    tot_out,
    pos,
    stats,
    obs,
    pert,
    obs_t,
    taper,
    anom,
    means,
    gain,
    result,
    scale,
    answer,
    small_sem,
    local_sem,
    send_e,
    recv_e,
    send_p,
    recv_p,
    send_q,
    recv_q,
    send_o,
    recv_o,
    send_g,
    recv_g,
    send_y,
    recv_y,
    send_z,
    recv_z,
    send_st,
    recv_st,
    recv_pos,
    send_ps,
    recv_ps,
    send_pz,
    recv_pz,
    send_pf,
    recv_pf,
    send_f,
    recv_f,
    send_out,
    recv_out,
    own_out,
):
    nr, nd, nm, nl, mm, tt, kk = sizes
    ng = nm // 2
    half = tt // 2
    members = nm * mm
    r = lax.axis_index("region")
    d = lax.axis_index("depth")
    me = lax.axis_index("member")
    q = me // 2
    c = me % 2
    sib = 2 * q + (1 - c)
    has_side = (r > 0, r < nr - 1)

    def dev(region=None, depth=None, member=None):
        return {
            "region": r if region is None else region,
            "depth": d if depth is None else depth,
            "member": me if member is None else member,
        }

    def rdma(src, dst, ssem, rsem, device):
        return pltpu.make_async_remote_copy(
            src_ref=src,
            dst_ref=dst,
            send_sem=ssem,
            recv_sem=rsem,
            device_id=device,
            device_id_type=MESH,
        )

    barrier = pltpu.get_barrier_semaphore()
    for j in range(1, nm):
        pl.semaphore_signal(
            barrier, inc=1, device_id=dev(member=(me + j) % nm), device_id_type=MESH
        )
    for i in range(1, nd):

        @pl.when(d + i < nd)
        def _():
            pl.semaphore_signal(barrier, inc=1, device_id=dev(depth=d + i), device_id_type=MESH)

    @pl.when(has_side[1])
    def _():
        pl.semaphore_signal(barrier, inc=1, device_id=dev(region=r + 1), device_id_type=MESH)

    local_own = pltpu.make_async_copy(ensemble, own, local_sem.at[0])
    local_own.start()
    smalls = [
        pltpu.make_async_copy(a, b, small_sem.at[i])
        for i, (a, b) in enumerate(
            ((weights_hbm, weights), (tiles_hbm, tiles), (values_hbm, values), (errors_hbm, errors))
        )
    ]
    for copy in smalls:
        copy.start()
    local_half = pltpu.make_async_copy(
        ensemble.at[:, :, pl.ds(pl.multiple_of(c * half, 128), half)],
        gathered.at[:, me],
        local_sem.at[1],
    )
    local_half.start()
    local_noise = pltpu.make_async_copy(noise, noise_v, local_sem.at[2])
    local_noise.start()

    pl.semaphore_wait(barrier, nm - 1 + d + (r > 0).astype(jnp.int32))

    piece = half // PIECES
    small = half // 4
    last = nl - 1
    units = (
        [(0, 0, half)]
        + [(1, p * piece, piece) for p in range(PIECES)]
        + [(l, 0, half) for l in range(2, last)]
        + [(last, p * piece, piece) for p in range(PIECES)]
    )

    def arrival(l, lo):
        return recv_e.at[l + lo // piece] if isinstance(l, int) and l == last else recv_e.at[l]

    def send_bulk(chosen):
        for l, lo, width in chosen:
            for to in [(me + 2 * g) % nm for g in range(1, ng)] + [(sib + 2 * g) % nm for g in range(ng)]:
                rdma(
                    ensemble.at[
                        l, :, pl.ds(pl.multiple_of((to % 2) * half + lo, 128), width)
                    ],
                    gathered.at[l, me, :, pl.ds(lo, width)],
                    send_e.at[0],
                    arrival(l, lo),
                    dev(member=to),
                ).start()

    def wait_bulk(l, lo, width):
        block = gathered.at[l, pl.ds(0, nm - 1), :, pl.ds(lo, width)]
        rdma(block, block, send_e.at[0], arrival(l, lo), dev(member=sib)).wait_recv()

    send_bulk(units[:LEAD])
    for i in range(1, nd):

        @pl.when(d >= i)
        def _():
            pl.semaphore_signal(
                answer.at[0], inc=1, device_id=dev(depth=d - i), device_id_type=MESH
            )

    @pl.when(has_side[0])
    def _():
        pl.semaphore_signal(answer.at[1], inc=1, device_id=dev(region=r - 1), device_id_type=MESH)

    for copy in smalls:
        copy.wait()
    local_own.wait()
    total = own[0].astype(F32) * weights[0]
    for l in range(1, nl):
        total = total + own[l].astype(F32) * weights[l]
    hi = total.astype(BF16)
    rest = total - hi.astype(F32)
    mid = rest.astype(BF16)
    low = (rest - mid.astype(F32)).astype(BF16)
    tile_ids = lax.broadcasted_iota(jnp.int32, (tt, kk), 0)
    onehot = jnp.where(tile_ids == tiles[...], 1.0, 0.0).astype(BF16)
    terms = jnp.dot(
        jnp.concatenate([hi, mid, low], axis=0), onehot, preferred_element_type=F32
    )
    picked = terms[0:mm] + terms[mm : 2 * mm] + terms[2 * mm : 3 * mm]
    part_mean = jnp.sum(picked, axis=0, keepdims=True) / mm
    top = part_mean.astype(BF16).astype(F32)
    second_row = (part_mean - top).astype(BF16).astype(F32)
    third_row = part_mean - top - second_row
    prow = lax.broadcasted_iota(jnp.int32, (16, kk), 0)
    split = jnp.where(prow == 0, top, jnp.where(prow == 1, second_row, third_row))
    part[0:mm] = (picked - part_mean).astype(BF16)
    part[mm : mm + 16] = jnp.where(prow < 3, split, 0.0).astype(BF16)

    def whole(block):
        values_of = block.astype(F32)
        return values_of[0:mm] + jnp.sum(values_of[mm : mm + 16], axis=0, keepdims=True)

    def part_copy(i):
        to = (d + i) % nd
        return rdma(part, part_in.at[d], send_p.at[i - 1], recv_p.at[i - 1], dev(depth=to))

    def part_from(i):
        frm = (d + i) % nd
        return rdma(
            part, part_in.at[frm], send_p.at[i - 1], recv_p.at[nd - i - 1], dev(depth=frm)
        )

    @pl.when(d < nd - 1)
    def _():
        pl.semaphore_wait(answer.at[0], nd - 1 - d)

    for i in range(1, nd):
        part_copy(i).start()

    pos[1] = jnp.broadcast_to(tiles[...].astype(F32), (8, kk))

    def pos_copy(side):
        return rdma(
            pos.at[1],
            pos.at[2 - 2 * side],
            send_st.at[side],
            recv_pos.at[1 - side],
            dev(region=r + (2 * side - 1)),
        )

    def pos_from(side):
        return rdma(
            pos.at[1],
            pos.at[2 * side],
            send_st.at[side],
            recv_pos.at[side],
            dev(region=r + (2 * side - 1)),
        )

    lane = (lax.broadcasted_iota(jnp.int32, (kk, half), 1) + c * half).astype(F32)

    def make_taper(w):
        position = pos[w].T[:, 0:1] + float((w - 1) * tt)
        close = jnp.maximum(0.0, 1.0 - jnp.abs(lane - position) * (1.0 / RADIUS))
        taper[w * kk : (w + 1) * kk] = close * close

    make_taper(1)

    @pl.when(has_side[1])
    def _():
        pl.semaphore_wait(answer.at[1], 1)

    for side in (0, 1):

        @pl.when(has_side[side])
        def _():
            pos_copy(side).start()

        @pl.when(jnp.logical_not(has_side[side]))
        def _():
            window = 0 if side == 0 else 2 * kk
            obs[:, :, window : window + kk] = jnp.zeros((nm, mm, kk), BF16)
            pert[:, :, window : window + kk] = jnp.zeros((2, mm, kk), BF16)
            stats[2 * side] = jnp.zeros((8, kk), F32)
            pos[2 * side] = jnp.zeros((8, kk), F32)

    predicted = whole(part[...])
    for i in range(1, nd):
        part_from(i).wait_recv()
        predicted = predicted + whole(part_in[(d + i) % nd])
    own_sum = jnp.sum(predicted, axis=0, keepdims=True)
    spread_in = predicted - own_sum / mm
    own_square = jnp.sum(spread_in * spread_in, axis=0, keepdims=True)
    qrow = lax.broadcasted_iota(jnp.int32, (2, kk), 0)
    squares[me] = jnp.where(qrow == 0, own_sum, own_square)
    obs[me, :, kk : 2 * kk] = spread_in.astype(BF16)

    def square_copy(j):
        return rdma(
            squares.at[me],
            squares.at[me],
            send_q.at[0],
            recv_q.at[0],
            dev(member=(me + j) % nm),
        )

    square_rest = squares.at[pl.ds(0, nm - 1)]
    square_all = rdma(square_rest, square_rest, send_q.at[0], recv_q.at[0], dev(member=sib))

    hk = kk // nd

    def obs_at(slot, w, h, width):
        return obs.at[slot, :, pl.ds(pl.multiple_of(w * kk + h * hk, 128), width)]

    def obs_copy(g):
        block = obs_at(me, 1, d, hk)
        return rdma(
            block, block, send_o.at[g - 1], recv_o.at[g - 1], dev(member=(me + 2 * g) % nm)
        )

    def obs_from(g):
        block = obs_at(cross(g), 1, d, hk)
        return rdma(block, block, send_o.at[g - 1], recv_o.at[ng - g - 1], dev(member=sib))

    def obs_swap(g, i):
        block = obs_at(cross(g), 1, d, hk)
        return rdma(
            block, block, send_y.at[g - 1, i - 1], recv_y.at[g - 1, i - 1], dev(depth=(d + i) % nd)
        )

    def swap_from(g, i):
        h = (d + i) % nd
        block = obs_at(cross(g), 1, h, hk)
        return rdma(
            block, block, send_y.at[g - 1, i - 1], recv_y.at[g - 1, nd - i - 1], dev(depth=h)
        )

    def side_obs(side, slot, h, width):
        return rdma(
            obs_at(slot, 1, h, width),
            obs_at(slot, 2 if side == 0 else 0, h, width),
            send_z.at[side],
            recv_z.at[1 - side],
            dev(region=r + (2 * side - 1)),
        )

    def side_all(side):
        block = obs.at[pl.ds(0, ng), :, pl.ds(kk, kk)]
        return rdma(
            block, block, send_z.at[side], recv_z.at[side], dev(region=r + (2 * side - 1))
        )

    def obs_forward(w, slot, h, width, number):
        block = obs_at(slot, w, h, width)
        return rdma(block, block, send_f.at[w], recv_f.at[number], dev(member=sib))

    def forward_all(w, wide, number):
        block = obs.at[pl.ds(0, wide[0]), :, pl.ds(0, wide[1])]
        return rdma(block, block, send_f.at[w], recv_f.at[number], dev(member=sib))

    def cross(g):
        return 2 * ((q + g) % ng) + c

    for j in range(1, nm):
        square_copy(j).start()
    for g in range(1, ng):
        obs_copy(g).start()
    obs_forward(1, me, 0, kk, 0).start()
    send_bulk(units[LEAD:])
    for side in (0, 1):

        @pl.when(has_side[side])
        def _():
            side_obs(side, me, 0, kk).start()
            pos_from(side).wait_recv()

        make_taper(2 * side)

    square_all.wait_recv()
    moments = [squares[j] for j in range(nm)]
    obs_mean = sum(m[0:1] for m in moments) / members
    deviation = predicted - obs_mean
    square_sum = sum(
        m[1:2] + mm * (m[0:1] / mm - obs_mean) * (m[0:1] / mm - obs_mean) for m in moments
    )
    spread = square_sum / (members - 1)
    error = errors[...]
    innovation = values[...] - obs_mean
    first = jnp.sum(innovation * innovation, axis=1, keepdims=True)
    second = jnp.sum(spread + error, axis=1, keepdims=True)
    rp = tot_in.shape[1]
    trow = lax.broadcasted_iota(jnp.int32, (rp, 128), 0)
    tlane = lax.broadcasted_iota(jnp.int32, (rp, 128), 1)
    own_total = jnp.where(tlane == 0, first, second)
    krow = lax.broadcasted_iota(jnp.int32, (8, kk), 0)
    shifts_of = jnp.zeros((8, kk), F32)
    for g in range(nm):
        shifts_of = jnp.where(krow == g, moments[g][0:1] / mm - obs_mean, shifts_of)
    stats[1] = shifts_of

    def stat_copy(side):
        return rdma(
            stats.at[1],
            stats.at[2 - 2 * side],
            send_st.at[side],
            recv_st.at[1 - side],
            dev(region=r + (2 * side - 1)),
        )

    def total_copy(way):
        return rdma(
            tot_out.at[way],
            tot_in.at[way],
            send_g.at[way],
            recv_g.at[way],
            dev(region=r + (1 - 2 * way)),
        )

    def total_from(way):
        return rdma(
            tot_out.at[way],
            tot_in.at[way],
            send_g.at[way],
            recv_g.at[way],
            dev(region=r - (1 - 2 * way)),
        )

    def relay(way):
        @pl.when(has_side[way])
        def _():
            total_from(way).wait_recv()

        behind = trow < r if way == 0 else trow > r
        tot_out[way] = jnp.where(
            behind, tot_in[way], jnp.where(trow == r, own_total, 0.0)
        )

        @pl.when(has_side[1 - way])
        def _():
            total_copy(way).start()

    low_end = r == 0
    high_end = r == nr - 1

    @pl.when(low_end)
    def _():
        relay(0)

    @pl.when(high_end)
    def _():
        relay(1)

    for side in (0, 1):

        @pl.when(has_side[side])
        def _():
            stat_copy(side).start()

    def hand_part(g, i):
        h = (d + i) % nd
        for side in (0, 1):

            @pl.when(has_side[side])
            def _():
                side_obs(side, cross(g), h, hk).start()

        obs_forward(1, cross(g), h, hk, i).start()

    for g in range(1, ng):
        obs_from(g).wait_recv()
        for i in range(1, nd):
            obs_swap(g, i).start()
        hand_part(g, 0)

    def transpose_part(w, h, width):
        at = pl.multiple_of(h * hk, 128)
        rows_of = pl.ds(pl.multiple_of(w * kk + at, 128), width)
        shifts = stats[w, :, pl.ds(at, width)].T
        for g in range(nm):
            block = obs[g, :, rows_of].astype(F32).T + shifts[:, g : g + 1]
            obs_t[rows_of, g * mm : (g + 1) * mm] = block.astype(BF16)

    everything = (0, half)

    def gain_rows(l, windows, columns=everything):
        cols = slice(*columns)
        right = anom[l, :, :, cols].reshape(members, columns[1] - columns[0])
        for w in windows:
            rows_of = slice(w * kk, (w + 1) * kk)
            cov = jnp.dot(obs_t[rows_of], right, preferred_element_type=F32)
            gain[l, rows_of, cols] = (cov * taper[rows_of, cols]).astype(BF16)

    def gain_part(l, h):
        at = pl.ds(pl.multiple_of(kk + h * hk, 128), hk)
        cov = jnp.dot(
            obs_t[at], anom[l].reshape(members, half), preferred_element_type=F32
        )
        gain[l, at] = (cov * taper[at]).astype(BF16)

    def center(l, columns=everything):
        cols = slice(*columns)
        wait_bulk(l, columns[0], columns[1] - columns[0])
        raw = gathered[l, :, :, cols].astype(F32)
        mean = jnp.sum(jnp.sum(raw, axis=0), axis=0, keepdims=True) / members
        means[l, :, cols] = jnp.broadcast_to(mean, (8, columns[1] - columns[0]))
        anom[l, :, :, cols] = (raw - mean[None]).astype(BF16)

    def own_window(l, windows, columns=everything):
        center(l, columns)
        gain_rows(l, windows, columns)

    def sib_pert(slot):
        block = pert.at[slot, :, pl.ds(kk, kk)]
        return rdma(block, block, send_ps.at[0], recv_ps.at[0], dev(member=sib))

    def side_pert(side):
        window = 2 * kk if side == 0 else 0
        return rdma(
            pert.at[c, :, pl.ds(kk, kk)],
            pert.at[c, :, pl.ds(window, kk)],
            send_pz.at[side],
            recv_pz.at[1 - side],
            dev(region=r + (2 * side - 1)),
        )

    def pert_forward(side, slot):
        block = pert.at[slot, :, pl.ds(2 * kk * side, kk)]
        return rdma(block, block, send_pf.at[side], recv_pf.at[side], dev(member=sib))

    def make_pert():
        everyone = jnp.where(trow < r, tot_in[0], jnp.where(trow > r, tot_in[1], own_total))
        grand = everyone[0:1]
        for i in range(1, nr):
            grand = grand + everyone[i : i + 1]
        inflation = grand[0:1, 0:1] / grand[0:1, 1:2]
        root = jnp.sqrt(inflation)
        infl_out[...] = inflation
        scale[...] = jnp.broadcast_to(root, (1, 128))
        factor = inflation / (inflation * spread + error)
        local_noise.wait()
        pert[c, :, kk : 2 * kk] = (
            (innovation + jnp.sqrt(error) * noise_v[...] - root * deviation)
            * (factor / (members - 1))
        ).astype(BF16)

        sib_pert(c).start()
        for side in (0, 1):

            @pl.when(has_side[side])
            def _():
                side_pert(side).start()

    mid_low = jnp.logical_and(r > 0, 2 * r < nr)
    mid_high = jnp.logical_and(r < nr - 1, 2 * r >= nr)

    @pl.when(mid_low)
    def _():
        relay(0)

    @pl.when(mid_high)
    def _():
        relay(1)

    forward_all(1, (1, kk + (ng - 1) * hk), 0).wait_recv()
    transpose_part(1, d, hk)
    local_half.wait()
    center(0)
    gain_part(0, d)
    for i in range(1, nd):
        for g in range(1, ng):
            swap_from(g, i).wait_recv()
            hand_part(g, i)
    center(1)
    gain_part(1, d)

    @pl.when(mid_low)
    def _():
        relay(1)
        make_pert()

    @pl.when(mid_high)
    def _():
        relay(0)
        make_pert()

    for i in range(1, nd):
        h = (d + i) % nd
        forward_all(1, (1, (ng - 1) * hk), i).wait_recv()
        transpose_part(1, h, hk)
        gain_part(0, h)
        gain_part(1, h)
    own_window(2, (1,))

    for side in (0, 1):

        @pl.when(has_side[side])
        def _():
            side_all(side).wait_recv()
            for g in range(ng):
                obs_forward(2 * side, cross(g), 0, kk, nd + side).start()


    @pl.when(low_end)
    def _():
        relay(1)
        make_pert()

    @pl.when(high_end)
    def _():
        relay(0)
        make_pert()

    for side in (0, 1):

        @pl.when(has_side[side])
        def _():
            rdma(
                stats.at[1],
                stats.at[2 * side],
                send_st.at[side],
                recv_st.at[side],
                dev(region=r + (2 * side - 1)),
            ).wait_recv()
            forward_all(2 * side, (ng, kk), nd + side).wait_recv()

        transpose_part(2 * side, 0, kk)

    def out_block(l, which, columns):
        lo, width = columns[0], columns[1] - columns[0]
        return out.at[l, :, pl.ds(pl.multiple_of(which * half + lo, 128), width)]

    def out_copies(l, columns):
        cols = slice(*columns)
        there = rdma(
            result.at[l, 1 - c, :, cols],
            out_block(l, c, columns),
            send_out.at[0],
            recv_out.at[0],
            dev(member=sib),
        )
        here = pltpu.make_async_copy(
            result.at[l, c, :, cols], out_block(l, c, columns), own_out.at[0]
        )
        return there, here

    def finish_variable(l, columns=everything):
        cols = slice(*columns)
        width = columns[1] - columns[0]
        increment = jnp.dot(
            pert[...].reshape(2 * mm, 3 * kk), gain[l, :, cols], preferred_element_type=F32
        )
        base = means[l, 0:1, cols][None] + root[None] * anom[l, pl.ds(2 * q, 2), :, cols].astype(F32)
        result[l, :, :, cols] = (base + increment.reshape(2, mm, width)).astype(BF16)
        for copy in out_copies(l, columns):
            copy.start()

    def side_gain(l, carry):
        gain_rows(l, (0, 2))
        return carry

    lax.fori_loop(0, 3, side_gain, 0)

    for side in (0, 1):

        @pl.when(has_side[side])
        def _():
            side_pert(1 - side).wait_recv()
            pert_forward(side, c).start()

    own_window(3, (0, 1, 2))

    root = scale[0:1, 0:1]
    ready = min(READY, last)

    def ahead(l, carry):
        own_window(l, (0, 1, 2))
        return carry

    lax.fori_loop(4, ready, ahead, 0)
    sib_pert(1 - c).wait_recv()
    for side in (0, 1):

        @pl.when(has_side[side])
        def _():
            pert_forward(side, 1 - c).wait_recv()

    def late_variable(l, carry):
        finish_variable(l)
        return carry

    lax.fori_loop(0, ready, late_variable, 0)

    def one_variable(l, carry):
        own_window(l, (0, 1, 2))
        finish_variable(l)
        return carry

    lax.fori_loop(ready, last, one_variable, 0)
    for p in range(PIECES):
        columns = (p * piece, (p + 1) * piece)
        own_window(last, (0, 1, 2), columns)
        finish_variable(last, columns)

    sent = gathered.at[:, pl.ds(0, nm - 1)]
    rdma(sent, sent, send_e.at[0], recv_e.at[0], dev(member=sib)).wait_send()
    mine = out.at[:, :, pl.ds(pl.multiple_of(c * half, 128), half)]
    other = out.at[:, :, pl.ds(pl.multiple_of((1 - c) * half, 128), half)]
    pltpu.make_async_copy(mine, mine, own_out.at[0]).wait()
    theirs = rdma(other, other, send_out.at[0], recv_out.at[0], dev(member=sib))
    theirs.wait_send()
    theirs.wait_recv()
    for i in range(1, nd):
        part_copy(i).wait_send()
    square_all.wait_send()
    for g in range(1, ng):
        obs_copy(g).wait_send()
        for i in range(1, nd):
            obs_swap(g, i).wait_send()
    forward_all(1, (ng, kk), 0).wait_send()
    sib_pert(c).wait_send()
    for way in (0, 1):

        @pl.when(has_side[1 - way])
        def _():
            total_copy(way).wait_send()

    for side in (0, 1):

        @pl.when(has_side[side])
        def _():
            side_all(side).wait_send()
            forward_all(2 * side, (ng, kk), nd + side).wait_send()
            side_pert(side).wait_send()
            pert_forward(side, c).wait_send()
            both = stats.at[pl.ds(0, 2)]
            rdma(
                both, both, send_st.at[side], recv_st.at[side], dev(region=r + (2 * side - 1))
            ).wait_send()


def hand_on(block, out):
    pass


def solution(mesh):
    nr, nd, nm = (mesh.shape[a] for a in ("region", "depth", "member"))

    def shards(ensemble, obs_weights, obs_tiles, obs_values, obs_error, obs_noise):
        nl, mm, tt = ensemble.shape
        kk = obs_tiles.shape[0]
        ng = nm // 2
        half = tt // 2
        rp = -(-nr // 8) * 8
        dma = pltpu.SemaphoreType.DMA
        vmem = pl.BlockSpec(memory_space=pltpu.VMEM)
        anywhere = pl.BlockSpec(memory_space=pl.ANY)
        analysis, inflation = pl.pallas_call(
            functools.partial(kernel, (nr, nd, nm, nl, mm, tt, kk)),
            out_shape=(
                pltpu.VMEM((nl, mm, tt), BF16),
                pltpu.VMEM((1, 1), F32),
            ),
            in_specs=[anywhere] * 6,
            out_specs=(vmem, vmem),
            scratch_shapes=[
                pltpu.SMEM((nl,), F32),
                pltpu.VMEM((1, kk), jnp.int32),
                pltpu.VMEM((1, kk), F32),
                pltpu.VMEM((1, kk), F32),
                pltpu.VMEM((nl, mm, tt), BF16),
                pltpu.VMEM((nl, nm, mm, half), BF16),
                pltpu.VMEM((mm, kk), F32),
                pltpu.VMEM((mm + 16, kk), BF16),
                pltpu.VMEM((nd, mm + 16, kk), BF16),
                pltpu.VMEM((nm, 2, kk), F32),
                pltpu.VMEM((2, rp, 128), F32),
                pltpu.VMEM((2, rp, 128), F32),
                pltpu.VMEM((3, 8, kk), F32),
                pltpu.VMEM((3, 8, kk), F32),
                pltpu.VMEM((nm, mm, 3 * kk), BF16),
                pltpu.VMEM((2, mm, 3 * kk), BF16),
                pltpu.VMEM((3 * kk, nm * mm), BF16),
                pltpu.VMEM((3 * kk, half), F32),
                pltpu.VMEM((nl, nm, mm, half), BF16),
                pltpu.VMEM((nl, 8, half), F32),
                pltpu.VMEM((nl, 3 * kk, half), BF16),
                pltpu.VMEM((nl, 2, mm, half), BF16),
                pltpu.VMEM((1, 128), F32),
                pltpu.SemaphoreType.REGULAR((2,)),
                dma((4,)),
                dma((3,)),
                dma((1,)),
                dma((nl - 1 + PIECES,)),
                dma((nd - 1,)),
                dma((nd - 1,)),
                dma((1,)),
                dma((1,)),
                dma((ng - 1,)),
                dma((ng - 1,)),
                dma((2,)),
                dma((2,)),
                dma((ng - 1, nd - 1)),
                dma((ng - 1, nd - 1)),
                dma((2,)),
                dma((2,)),
                dma((2,)),
                dma((2,)),
                dma((2,)),
                dma((1,)),
                dma((1,)),
                dma((2,)),
                dma((2,)),
                dma((2,)),
                dma((2,)),
                dma((3,)),
                dma((nd + 2,)),
                dma((1,)),
                dma((1,)),
                dma((1,)),
            ],
            compiler_params=pltpu.CompilerParams(
                collective_id=0, has_side_effects=True, vmem_limit_bytes=56 * 1024 * 1024
            ),
        )(
            obs_weights,
            ensemble,
            obs_tiles.reshape(1, kk),
            obs_values.reshape(1, kk),
            obs_error.reshape(1, kk),
            obs_noise,
        )
        analysis = pl.pallas_call(
            hand_on,
            out_shape=jax.ShapeDtypeStruct((nl, mm, tt), BF16),
            in_specs=[anywhere],
            out_specs=anywhere,
            input_output_aliases={0: 0},
        )(analysis)
        return analysis, inflation.reshape(())

    return jax.shard_map(
        shards,
        mesh=mesh,
        in_specs=(
            P("depth", "member", "region"),
            P("depth"),
            P("region"),
            P("region"),
            P("region"),
            P("member", "region"),
        ),
        out_specs=(P("depth", "member", "region"), P()),
        check_vma=False,
    )
```

```python
import functools

import jax
import jax.numpy as jnp
from jax import lax
from jax.experimental import pallas as pl
from jax.experimental.pallas import tpu as pltpu
from jax.sharding import PartitionSpec as P

RADIUS = 1024
LEAD = 2
READY = 4
PIECES = 2
F32 = jnp.float32
BF16 = jnp.bfloat16
MESH = pl.DeviceIdType.MESH


def kernel(
    sizes,
    weights_hbm,
    ensemble,
    tiles_hbm,
    values_hbm,
    errors_hbm,
    noise,
    out,
    infl_out,
    weights,
    tiles,
    values,
    errors,
    own,
    gathered,
    noise_v,
    part,
    part_in,
    squares,
    tot_in,
    tot_out,
    pos,
    stats,
    obs,
    pert,
    obs_t,
    taper,
    anom,
    means,
    gain,
    result,
    scale,
    answer,
    small_sem,
    local_sem,
    send_e,
    recv_e,
    send_p,
    recv_p,
    send_q,
    recv_q,
    send_o,
    recv_o,
    send_g,
    recv_g,
    send_y,
    recv_y,
    send_z,
    recv_z,
    send_st,
    recv_st,
    recv_pos,
    send_ps,
    recv_ps,
    send_pz,
    recv_pz,
    send_pf,
    recv_pf,
    send_f,
    recv_f,
    send_out,
    recv_out,
    own_out,
):
    nr, nd, nm, nl, mm, tt, kk = sizes
    ng = nm // 2
    half = tt // 2
    members = nm * mm
    r = lax.axis_index("region")
    d = lax.axis_index("depth")
    me = lax.axis_index("member")
    q = me // 2
    c = me % 2
    sib = 2 * q + (1 - c)
    has_side = (r > 0, r < nr - 1)

    def dev(region=None, depth=None, member=None):
        return {
            "region": r if region is None else region,
            "depth": d if depth is None else depth,
            "member": me if member is None else member,
        }

    def rdma(src, dst, ssem, rsem, device):
        return pltpu.make_async_remote_copy(
            src_ref=src,
            dst_ref=dst,
            send_sem=ssem,
            recv_sem=rsem,
            device_id=device,
            device_id_type=MESH,
        )

    barrier = pltpu.get_barrier_semaphore()
    for j in range(1, nm):
        pl.semaphore_signal(
            barrier, inc=1, device_id=dev(member=(me + j) % nm), device_id_type=MESH
        )
    for i in range(1, nd):

        @pl.when(d + i < nd)
        def _():
            pl.semaphore_signal(barrier, inc=1, device_id=dev(depth=d + i), device_id_type=MESH)

    @pl.when(has_side[1])
    def _():
        pl.semaphore_signal(barrier, inc=1, device_id=dev(region=r + 1), device_id_type=MESH)

    local_own = pltpu.make_async_copy(ensemble, own, local_sem.at[0])
    local_own.start()
    smalls = [
        pltpu.make_async_copy(a, b, small_sem.at[i])
        for i, (a, b) in enumerate(
            ((weights_hbm, weights), (tiles_hbm, tiles), (values_hbm, values), (errors_hbm, errors))
        )
    ]
    for copy in smalls:
        copy.start()
    local_half = pltpu.make_async_copy(
        ensemble.at[:, :, pl.ds(pl.multiple_of(c * half, 128), half)],
        gathered.at[:, me],
        local_sem.at[1],
    )
    local_half.start()
    local_noise = pltpu.make_async_copy(noise, noise_v, local_sem.at[2])
    local_noise.start()

    pl.semaphore_wait(barrier, nm - 1 + d + (r > 0).astype(jnp.int32))

    piece = half // PIECES
    small = half // 4
    last = nl - 1
    units = (
        [(0, 0, half)]
        + [(1, p * piece, piece) for p in range(PIECES)]
        + [(l, 0, half) for l in range(2, last)]
        + [(last, p * piece, piece) for p in range(PIECES)]
    )

    def arrival(l, lo):
        return recv_e.at[l + lo // piece] if isinstance(l, int) and l == last else recv_e.at[l]

    def send_bulk(chosen):
        for l, lo, width in chosen:
            for to in [(me + 2 * g) % nm for g in range(1, ng)] + [(sib + 2 * g) % nm for g in range(ng)]:
                rdma(
                    ensemble.at[
                        l, :, pl.ds(pl.multiple_of((to % 2) * half + lo, 128), width)
                    ],
                    gathered.at[l, me, :, pl.ds(lo, width)],
                    send_e.at[0],
                    arrival(l, lo),
                    dev(member=to),
                ).start()

    def wait_bulk(l, lo, width):
        block = gathered.at[l, pl.ds(0, nm - 1), :, pl.ds(lo, width)]
        rdma(block, block, send_e.at[0], arrival(l, lo), dev(member=sib)).wait_recv()

    send_bulk(units[:LEAD])
    for i in range(1, nd):

        @pl.when(d >= i)
        def _():
            pl.semaphore_signal(
                answer.at[0], inc=1, device_id=dev(depth=d - i), device_id_type=MESH
            )

    @pl.when(has_side[0])
    def _():
        pl.semaphore_signal(answer.at[1], inc=1, device_id=dev(region=r - 1), device_id_type=MESH)

    for copy in smalls:
        copy.wait()
    local_own.wait()
    total = own[0].astype(F32) * weights[0]
    for l in range(1, nl):
        total = total + own[l].astype(F32) * weights[l]
    hi = total.astype(BF16)
    rest = total - hi.astype(F32)
    mid = rest.astype(BF16)
    low = (rest - mid.astype(F32)).astype(BF16)
    tile_ids = lax.broadcasted_iota(jnp.int32, (tt, kk), 0)
    onehot = jnp.where(tile_ids == tiles[...], 1.0, 0.0).astype(BF16)
    terms = jnp.dot(
        jnp.concatenate([hi, mid, low], axis=0), onehot, preferred_element_type=F32
    )
    picked = terms[0:mm] + terms[mm : 2 * mm] + terms[2 * mm : 3 * mm]
    part_mean = jnp.sum(picked, axis=0, keepdims=True) / mm
    top = part_mean.astype(BF16).astype(F32)
    second_row = (part_mean - top).astype(BF16).astype(F32)
    third_row = part_mean - top - second_row
    prow = lax.broadcasted_iota(jnp.int32, (16, kk), 0)
    split = jnp.where(prow == 0, top, jnp.where(prow == 1, second_row, third_row))
    part[0:mm] = (picked - part_mean).astype(BF16)
    part[mm : mm + 16] = jnp.where(prow < 3, split, 0.0).astype(BF16)

    def whole(block):
        values_of = block.astype(F32)
        return values_of[0:mm] + jnp.sum(values_of[mm : mm + 16], axis=0, keepdims=True)

    def part_copy(i):
        to = (d + i) % nd
        return rdma(part, part_in.at[d], send_p.at[i - 1], recv_p.at[i - 1], dev(depth=to))

    def part_from(i):
        frm = (d + i) % nd
        return rdma(
            part, part_in.at[frm], send_p.at[i - 1], recv_p.at[nd - i - 1], dev(depth=frm)
        )

    @pl.when(d < nd - 1)
    def _():
        pl.semaphore_wait(answer.at[0], nd - 1 - d)

    for i in range(1, nd):
        part_copy(i).start()

    pos[1] = jnp.broadcast_to(tiles[...].astype(F32), (8, kk))

    def pos_copy(side):
        return rdma(
            pos.at[1],
            pos.at[2 - 2 * side],
            send_st.at[side],
            recv_pos.at[1 - side],
            dev(region=r + (2 * side - 1)),
        )

    def pos_from(side):
        return rdma(
            pos.at[1],
            pos.at[2 * side],
            send_st.at[side],
            recv_pos.at[side],
            dev(region=r + (2 * side - 1)),
        )

    lane = (lax.broadcasted_iota(jnp.int32, (kk, half), 1) + c * half).astype(F32)

    def make_taper(w):
        position = pos[w].T[:, 0:1] + float((w - 1) * tt)
        close = jnp.maximum(0.0, 1.0 - jnp.abs(lane - position) * (1.0 / RADIUS))
        taper[w * kk : (w + 1) * kk] = close * close

    make_taper(1)

    @pl.when(has_side[1])
    def _():
        pl.semaphore_wait(answer.at[1], 1)

    for side in (0, 1):

        @pl.when(has_side[side])
        def _():
            pos_copy(side).start()

    predicted = whole(part[...])
    for i in range(1, nd):
        part_from(i).wait_recv()
        predicted = predicted + whole(part_in[(d + i) % nd])
    own_sum = jnp.sum(predicted, axis=0, keepdims=True)
    spread_in = predicted - own_sum / mm
    own_square = jnp.sum(spread_in * spread_in, axis=0, keepdims=True)
    qrow = lax.broadcasted_iota(jnp.int32, (2, kk), 0)
    squares[me] = jnp.where(qrow == 0, own_sum, own_square)
    obs[me, :, kk : 2 * kk] = spread_in.astype(BF16)

    def square_copy(j):
        return rdma(
            squares.at[me],
            squares.at[me],
            send_q.at[0],
            recv_q.at[0],
            dev(member=(me + j) % nm),
        )

    square_rest = squares.at[pl.ds(0, nm - 1)]
    square_all = rdma(square_rest, square_rest, send_q.at[0], recv_q.at[0], dev(member=sib))

    first_part = kk // (2 * nd)
    cuts = [0] + [first_part + (kk - first_part) * h // (nd - 1) for h in range(nd)]
    parts = [(cuts[h], cuts[h + 1] - cuts[h]) for h in range(nd)]
    whole_slot = (0, kk)

    def by_depth(step, ahead=0):
        for h in range(nd):

            @pl.when(d == (h - ahead) % nd)
            def _():
                step(h)

    def obs_at(slot, w, extent):
        return obs.at[slot, :, pl.ds(w * kk + extent[0], extent[1])]

    def obs_copy(g, h):
        block = obs_at(me, 1, parts[h])
        return rdma(
            block, block, send_o.at[g - 1], recv_o.at[g - 1], dev(member=(me + 2 * g) % nm)
        )

    def obs_from(g, h):
        block = obs_at(cross(g), 1, parts[h])
        return rdma(block, block, send_o.at[g - 1], recv_o.at[ng - g - 1], dev(member=sib))

    def obs_swap(g, i, h):
        block = obs_at(cross(g), 1, parts[h])
        return rdma(
            block, block, send_y.at[g - 1, i - 1], recv_y.at[g - 1, i - 1], dev(depth=(d + i) % nd)
        )

    def swap_from(g, i, h):
        block = obs_at(cross(g), 1, parts[h])
        return rdma(
            block, block, send_y.at[g - 1, i - 1], recv_y.at[g - 1, nd - i - 1], dev(depth=h)
        )

    def side_obs(side, slot, extent):
        return rdma(
            obs_at(slot, 1, extent),
            obs_at(slot, 2 if side == 0 else 0, extent),
            send_z.at[side],
            recv_z.at[1 - side],
            dev(region=r + (2 * side - 1)),
        )

    def side_all(side):
        block = obs.at[pl.ds(0, ng), :, pl.ds(kk, kk)]
        return rdma(
            block, block, send_z.at[side], recv_z.at[side], dev(region=r + (2 * side - 1))
        )

    def obs_forward(w, slot, extent, number):
        block = obs_at(slot, w, extent)
        return rdma(block, block, send_f.at[w], recv_f.at[number], dev(member=sib))

    def forward_all(w, wide, number):
        block = obs.at[pl.ds(0, wide[0]), :, pl.ds(0, wide[1])]
        return rdma(block, block, send_f.at[w], recv_f.at[number], dev(member=sib))

    def cross(g):
        return 2 * ((q + g) % ng) + c

    for j in range(1, nm):
        square_copy(j).start()
    by_depth(lambda h: [obs_copy(g, h).start() for g in range(1, ng)])
    obs_forward(1, me, whole_slot, 0).start()
    send_bulk(units[LEAD:])
    for side in (0, 1):

        @pl.when(has_side[side])
        def _():
            side_obs(side, me, whole_slot).start()
            pos_from(side).wait_recv()
            make_taper(2 * side)

    square_all.wait_recv()
    moments = [squares[j] for j in range(nm)]
    obs_mean = sum(m[0:1] for m in moments) / members
    deviation = predicted - obs_mean
    square_sum = sum(
        m[1:2] + mm * (m[0:1] / mm - obs_mean) * (m[0:1] / mm - obs_mean) for m in moments
    )
    spread = square_sum / (members - 1)
    error = errors[...]
    innovation = values[...] - obs_mean
    first = jnp.sum(innovation * innovation, axis=1, keepdims=True)
    second = jnp.sum(spread + error, axis=1, keepdims=True)
    rp = tot_in.shape[1]
    trow = lax.broadcasted_iota(jnp.int32, (rp, 128), 0)
    tlane = lax.broadcasted_iota(jnp.int32, (rp, 128), 1)
    own_total = jnp.where(tlane == 0, first, second)
    krow = lax.broadcasted_iota(jnp.int32, (8, kk), 0)
    shifts_of = jnp.zeros((8, kk), F32)
    for g in range(nm):
        shifts_of = jnp.where(krow == g, moments[g][0:1] / mm - obs_mean, shifts_of)
    stats[1] = shifts_of

    def stat_copy(side):
        return rdma(
            stats.at[1],
            stats.at[2 - 2 * side],
            send_st.at[side],
            recv_st.at[1 - side],
            dev(region=r + (2 * side - 1)),
        )

    def total_copy(way):
        return rdma(
            tot_out.at[way],
            tot_in.at[way],
            send_g.at[way],
            recv_g.at[way],
            dev(region=r + (1 - 2 * way)),
        )

    def total_from(way):
        return rdma(
            tot_out.at[way],
            tot_in.at[way],
            send_g.at[way],
            recv_g.at[way],
            dev(region=r - (1 - 2 * way)),
        )

    def relay(way):
        @pl.when(has_side[way])
        def _():
            total_from(way).wait_recv()

        behind = trow < r if way == 0 else trow > r
        tot_out[way] = jnp.where(
            behind, tot_in[way], jnp.where(trow == r, own_total, 0.0)
        )

        @pl.when(has_side[1 - way])
        def _():
            total_copy(way).start()

    low_end = r == 0
    high_end = r == nr - 1

    @pl.when(low_end)
    def _():
        relay(0)

    @pl.when(high_end)
    def _():
        relay(1)

    for side in (0, 1):

        @pl.when(has_side[side])
        def _():
            stat_copy(side).start()

    def hand_part(g, i, h):
        for side in (0, 1):

            @pl.when(has_side[side])
            def _():
                side_obs(side, cross(g), parts[h]).start()

        obs_forward(1, cross(g), parts[h], i).start()

    def take_part(h):
        for g in range(1, ng):
            obs_from(g, h).wait_recv()
            for i in range(1, nd):
                obs_swap(g, i, h).start()
            hand_part(g, 0, h)

    by_depth(take_part)

    def transpose_part(w, extent):
        lo, width = extent
        rows_of = pl.ds(w * kk + lo, width)
        shifts = stats[w, :, lo : lo + width].T
        for g in range(nm):
            block = obs[g, :, rows_of].astype(F32).T + shifts[:, g : g + 1]
            obs_t[rows_of, g * mm : (g + 1) * mm] = block.astype(BF16)

    everything = (0, half)

    middle = jnp.logical_and(has_side[0], has_side[1])
    beside = jnp.where(has_side[0], 0, 2)

    def by_place(step):
        @pl.when(middle)
        def _():
            step((0, 2))

        @pl.when(jnp.logical_not(middle))
        def _():
            step((beside,))

    def span(w):
        return pl.ds(w * kk if isinstance(w, int) else pl.multiple_of(w * kk, 128), kk)

    def gain_rows(l, windows, columns=everything):
        cols = slice(*columns)
        right = anom[l, :, :, cols].reshape(members, columns[1] - columns[0])
        for w in windows:
            cov = jnp.dot(obs_t[span(w)], right, preferred_element_type=F32)
            gain[l, span(w), cols] = (cov * taper[span(w), cols]).astype(BF16)

    def gain_part(l, h):
        at = pl.ds(kk + parts[h][0], parts[h][1])
        cov = jnp.dot(
            obs_t[at], anom[l].reshape(members, half), preferred_element_type=F32
        )
        gain[l, at] = (cov * taper[at]).astype(BF16)

    def wait_variable(l, columns=everything):
        wait_bulk(l, columns[0], columns[1] - columns[0])

    def center(l, columns=everything):
        cols = slice(*columns)
        raw = gathered[l, :, :, cols].astype(F32)
        mean = jnp.sum(jnp.sum(raw, axis=0), axis=0, keepdims=True) / members
        means[l, :, cols] = jnp.broadcast_to(mean, (8, columns[1] - columns[0]))
        anom[l, :, :, cols] = (raw - mean[None]).astype(BF16)

    def own_window(l, windows, columns=everything):
        center(l, columns)
        gain_rows(l, windows, columns)

    def sib_pert(slot):
        block = pert.at[slot, :, pl.ds(kk, kk)]
        return rdma(block, block, send_ps.at[0], recv_ps.at[0], dev(member=sib))

    def side_pert(side):
        window = 2 * kk if side == 0 else 0
        return rdma(
            pert.at[c, :, pl.ds(kk, kk)],
            pert.at[c, :, pl.ds(window, kk)],
            send_pz.at[side],
            recv_pz.at[1 - side],
            dev(region=r + (2 * side - 1)),
        )

    def pert_forward(side, slot):
        block = pert.at[slot, :, pl.ds(2 * kk * side, kk)]
        return rdma(block, block, send_pf.at[side], recv_pf.at[side], dev(member=sib))

    def make_pert():
        everyone = jnp.where(trow < r, tot_in[0], jnp.where(trow > r, tot_in[1], own_total))
        grand = everyone[0:1]
        for i in range(1, nr):
            grand = grand + everyone[i : i + 1]
        inflation = grand[0:1, 0:1] / grand[0:1, 1:2]
        root = jnp.sqrt(inflation)
        infl_out[...] = inflation
        scale[...] = jnp.broadcast_to(root, (1, 128))
        factor = inflation / (inflation * spread + error)
        local_noise.wait()
        pert[c, :, kk : 2 * kk] = (
            (innovation + jnp.sqrt(error) * noise_v[...] - root * deviation)
            * (factor / (members - 1))
        ).astype(BF16)

        sib_pert(c).start()
        for side in (0, 1):

            @pl.when(has_side[side])
            def _():
                side_pert(side).start()

    mid_low = jnp.logical_and(r > 0, 2 * r < nr)
    mid_high = jnp.logical_and(r < nr - 1, 2 * r >= nr)

    @pl.when(mid_low)
    def _():
        relay(0)

    @pl.when(mid_high)
    def _():
        relay(1)

    local_half.wait()
    wait_variable(0)
    center(0)

    def own_part(h):
        forward_all(1, (1, kk + (ng - 1) * parts[h][1]), 0).wait_recv()
        transpose_part(1, parts[h])
        gain_part(0, h)

    by_depth(own_part)

    def swap_part(i, h):
        for g in range(1, ng):
            swap_from(g, i, h).wait_recv()
            hand_part(g, i, h)

    for i in range(1, nd):
        by_depth(functools.partial(swap_part, i), i)
    wait_variable(1)
    center(1)
    by_depth(lambda h: gain_part(1, h))

    @pl.when(mid_low)
    def _():
        relay(1)
        make_pert()

    @pl.when(mid_high)
    def _():
        relay(0)
        make_pert()

    def other_part(i, h):
        forward_all(1, (1, (ng - 1) * parts[h][1]), i).wait_recv()
        transpose_part(1, parts[h])
        gain_part(0, h)
        gain_part(1, h)

    for i in range(1, nd):
        by_depth(functools.partial(other_part, i), i)
    wait_variable(2)
    own_window(2, (1,))

    for side in (0, 1):

        @pl.when(has_side[side])
        def _():
            side_all(side).wait_recv()
            for g in range(ng):
                obs_forward(2 * side, cross(g), whole_slot, nd + side).start()


    @pl.when(low_end)
    def _():
        relay(1)
        make_pert()

    @pl.when(high_end)
    def _():
        relay(0)
        make_pert()

    for side in (0, 1):

        @pl.when(has_side[side])
        def _():
            rdma(
                stats.at[1],
                stats.at[2 * side],
                send_st.at[side],
                recv_st.at[side],
                dev(region=r + (2 * side - 1)),
            ).wait_recv()
            forward_all(2 * side, (ng, kk), nd + side).wait_recv()

            transpose_part(2 * side, whole_slot)

    def out_block(l, which, columns):
        lo, width = columns[0], columns[1] - columns[0]
        return out.at[l, :, pl.ds(pl.multiple_of(which * half + lo, 128), width)]

    def out_copies(l, columns):
        cols = slice(*columns)
        there = rdma(
            result.at[l, 1 - c, :, cols],
            out_block(l, c, columns),
            send_out.at[0],
            recv_out.at[0],
            dev(member=sib),
        )
        here = pltpu.make_async_copy(
            result.at[l, c, :, cols], out_block(l, c, columns), own_out.at[0]
        )
        return there, here

    def finish_variable(l, sides, columns=everything):
        cols = slice(*columns)
        width = columns[1] - columns[0]
        if len(sides) == 2:
            increment = jnp.dot(
                pert[...].reshape(2 * mm, 3 * kk), gain[l, :, cols], preferred_element_type=F32
            )
        else:
            increment = jnp.zeros((2 * mm, width), F32)
            for w in (1,) + sides:
                increment = increment + jnp.dot(
                    pert[:, :, span(w)].reshape(2 * mm, kk),
                    gain[l, span(w), cols],
                    preferred_element_type=F32,
                )
        base = means[l, 0:1, cols][None] + scale[0:1, 0:1][None] * anom[
            l, pl.ds(2 * q, 2), :, cols
        ].astype(F32)
        result[l, :, :, cols] = (base + increment.reshape(2, mm, width)).astype(BF16)

    def send_result(l, columns=everything):
        for copy in out_copies(l, columns):
            copy.start()

    def early_gain(sides):
        def step(l, carry):
            gain_rows(l, sides)
            return carry

        lax.fori_loop(0, 3, step, 0)

    by_place(early_gain)
    for side in (0, 1):

        @pl.when(has_side[side])
        def _():
            side_pert(1 - side).wait_recv()
            pert_forward(side, c).start()

    ready = min(READY, last)

    def ahead(l, carry):
        wait_variable(l)
        by_place(lambda sides: own_window(l, (1,) + sides))
        return carry

    lax.fori_loop(3, ready, ahead, 0)
    sib_pert(1 - c).wait_recv()
    for side in (0, 1):

        @pl.when(has_side[side])
        def _():
            pert_forward(side, 1 - c).wait_recv()

    def late_variable(l, carry):
        by_place(lambda sides: finish_variable(l, sides))
        send_result(l)
        return carry

    lax.fori_loop(0, ready, late_variable, 0)

    def whole_variable(l, columns=everything):
        wait_variable(l, columns)

        def step(sides):
            own_window(l, (1,) + sides, columns)
            finish_variable(l, sides, columns)

        by_place(step)
        send_result(l, columns)

    def one_variable(l, carry):
        whole_variable(l)
        return carry

    lax.fori_loop(ready, last, one_variable, 0)
    for p in range(PIECES):
        whole_variable(last, (p * piece, (p + 1) * piece))

    sent = gathered.at[:, pl.ds(0, nm - 1)]
    rdma(sent, sent, send_e.at[0], recv_e.at[0], dev(member=sib)).wait_send()
    mine = out.at[:, :, pl.ds(pl.multiple_of(c * half, 128), half)]
    other = out.at[:, :, pl.ds(pl.multiple_of((1 - c) * half, 128), half)]
    pltpu.make_async_copy(mine, mine, own_out.at[0]).wait()
    theirs = rdma(other, other, send_out.at[0], recv_out.at[0], dev(member=sib))
    theirs.wait_send()
    theirs.wait_recv()
    for i in range(1, nd):
        part_copy(i).wait_send()
    square_all.wait_send()
    def parts_sent(h):
        for g in range(1, ng):
            obs_copy(g, h).wait_send()
            for i in range(1, nd):
                obs_swap(g, i, h).wait_send()

    by_depth(parts_sent)
    forward_all(1, (ng, kk), 0).wait_send()
    sib_pert(c).wait_send()
    for way in (0, 1):

        @pl.when(has_side[1 - way])
        def _():
            total_copy(way).wait_send()

    for side in (0, 1):

        @pl.when(has_side[side])
        def _():
            side_all(side).wait_send()
            forward_all(2 * side, (ng, kk), nd + side).wait_send()
            side_pert(side).wait_send()
            pert_forward(side, c).wait_send()
            both = stats.at[pl.ds(0, 2)]
            rdma(
                both, both, send_st.at[side], recv_st.at[side], dev(region=r + (2 * side - 1))
            ).wait_send()


def hand_on(block, out):
    pass


def solution(mesh):
    nr, nd, nm = (mesh.shape[a] for a in ("region", "depth", "member"))

    def shards(ensemble, obs_weights, obs_tiles, obs_values, obs_error, obs_noise):
        nl, mm, tt = ensemble.shape
        kk = obs_tiles.shape[0]
        ng = nm // 2
        half = tt // 2
        rp = -(-nr // 8) * 8
        dma = pltpu.SemaphoreType.DMA
        vmem = pl.BlockSpec(memory_space=pltpu.VMEM)
        anywhere = pl.BlockSpec(memory_space=pl.ANY)
        analysis, inflation = pl.pallas_call(
            functools.partial(kernel, (nr, nd, nm, nl, mm, tt, kk)),
            out_shape=(
                pltpu.VMEM((nl, mm, tt), BF16),
                pltpu.VMEM((1, 1), F32),
            ),
            in_specs=[anywhere] * 6,
            out_specs=(vmem, vmem),
            scratch_shapes=[
                pltpu.SMEM((nl,), F32),
                pltpu.VMEM((1, kk), jnp.int32),
                pltpu.VMEM((1, kk), F32),
                pltpu.VMEM((1, kk), F32),
                pltpu.VMEM((nl, mm, tt), BF16),
                pltpu.VMEM((nl, nm, mm, half), BF16),
                pltpu.VMEM((mm, kk), F32),
                pltpu.VMEM((mm + 16, kk), BF16),
                pltpu.VMEM((nd, mm + 16, kk), BF16),
                pltpu.VMEM((nm, 2, kk), F32),
                pltpu.VMEM((2, rp, 128), F32),
                pltpu.VMEM((2, rp, 128), F32),
                pltpu.VMEM((3, 8, kk), F32),
                pltpu.VMEM((3, 8, kk), F32),
                pltpu.VMEM((nm, mm, 3 * kk), BF16),
                pltpu.VMEM((2, mm, 3 * kk), BF16),
                pltpu.VMEM((3 * kk, nm * mm), BF16),
                pltpu.VMEM((3 * kk, half), F32),
                pltpu.VMEM((nl, nm, mm, half), BF16),
                pltpu.VMEM((nl, 8, half), F32),
                pltpu.VMEM((nl, 3 * kk, half), BF16),
                pltpu.VMEM((nl, 2, mm, half), BF16),
                pltpu.VMEM((1, 128), F32),
                pltpu.SemaphoreType.REGULAR((2,)),
                dma((4,)),
                dma((3,)),
                dma((1,)),
                dma((nl - 1 + PIECES,)),
                dma((nd - 1,)),
                dma((nd - 1,)),
                dma((1,)),
                dma((1,)),
                dma((ng - 1,)),
                dma((ng - 1,)),
                dma((2,)),
                dma((2,)),
                dma((ng - 1, nd - 1)),
                dma((ng - 1, nd - 1)),
                dma((2,)),
                dma((2,)),
                dma((2,)),
                dma((2,)),
                dma((2,)),
                dma((1,)),
                dma((1,)),
                dma((2,)),
                dma((2,)),
                dma((2,)),
                dma((2,)),
                dma((3,)),
                dma((nd + 2,)),
                dma((1,)),
                dma((1,)),
                dma((1,)),
            ],
            compiler_params=pltpu.CompilerParams(
                collective_id=0, has_side_effects=True, vmem_limit_bytes=56 * 1024 * 1024
            ),
        )(
            obs_weights,
            ensemble,
            obs_tiles.reshape(1, kk),
            obs_values.reshape(1, kk),
            obs_error.reshape(1, kk),
            obs_noise,
        )
        analysis = pl.pallas_call(
            hand_on,
            out_shape=jax.ShapeDtypeStruct((nl, mm, tt), BF16),
            in_specs=[anywhere],
            out_specs=anywhere,
            input_output_aliases={0: 0},
        )(analysis)
        return analysis, inflation.reshape(())

    return jax.shard_map(
        shards,
        mesh=mesh,
        in_specs=(
            P("depth", "member", "region"),
            P("depth"),
            P("region"),
            P("region"),
            P("region"),
            P("member", "region"),
        ),
        out_specs=(P("depth", "member", "region"), P()),
        check_vma=False,
    )
```

```python
import functools

import jax
import jax.numpy as jnp
from jax import lax
from jax.experimental import pallas as pl
from jax.experimental.pallas import tpu as pltpu
from jax.sharding import PartitionSpec as P

RADIUS = 1024
LEAD = 2
READY = 4
PIECES = 2
F32 = jnp.float32
BF16 = jnp.bfloat16
MESH = pl.DeviceIdType.MESH


def kernel(
    sizes,
    weights_hbm,
    ensemble,
    tiles_hbm,
    values_hbm,
    errors_hbm,
    noise,
    out,
    infl_out,
    weights,
    tiles,
    values,
    errors,
    own,
    gathered,
    noise_v,
    part,
    part_in,
    squares,
    tot_in,
    tot_out,
    pos,
    stats,
    obs,
    pert,
    obs_t,
    taper,
    anom,
    means,
    gain,
    result,
    scale,
    answer,
    plane_sent,
    side_sent,
    recv_pert,
    small_sem,
    local_sem,
    send_e,
    recv_e,
    recv_p,
    send_q,
    recv_q,
    recv_o,
    send_g,
    recv_g,
    recv_y,
    recv_z,
    recv_pos,
    recv_pz,
    recv_f,
    send_out,
    recv_out,
):
    nr, nd, nm, nl, mm, tt, kk = sizes
    ng = nm // 2
    half = tt // 2
    members = nm * mm
    r = lax.axis_index("region")
    d = lax.axis_index("depth")
    me = lax.axis_index("member")
    q = me // 2
    c = me % 2
    sib = 2 * q + (1 - c)
    has_side = (r > 0, r < nr - 1)

    def dev(region=None, depth=None, member=None):
        return {
            "region": r if region is None else region,
            "depth": d if depth is None else depth,
            "member": me if member is None else member,
        }

    def rdma(src, dst, ssem, rsem, device):
        return pltpu.make_async_remote_copy(
            src_ref=src,
            dst_ref=dst,
            send_sem=ssem,
            recv_sem=rsem,
            device_id=device,
            device_id_type=MESH,
        )

    barrier = pltpu.get_barrier_semaphore()
    for j in range(1, nm):
        pl.semaphore_signal(
            barrier, inc=1, device_id=dev(member=(me + j) % nm), device_id_type=MESH
        )
    for i in range(1, nd):

        @pl.when(d + i < nd)
        def _():
            pl.semaphore_signal(barrier, inc=1, device_id=dev(depth=d + i), device_id_type=MESH)

    @pl.when(has_side[1])
    def _():
        pl.semaphore_signal(barrier, inc=1, device_id=dev(region=r + 1), device_id_type=MESH)

    local_own = pltpu.make_async_copy(ensemble, own, local_sem.at[0])
    local_own.start()
    smalls = [
        pltpu.make_async_copy(a, b, small_sem.at[i])
        for i, (a, b) in enumerate(
            ((weights_hbm, weights), (tiles_hbm, tiles), (values_hbm, values), (errors_hbm, errors))
        )
    ]
    for copy in smalls:
        copy.start()
    local_half = pltpu.make_async_copy(
        ensemble.at[:, :, pl.ds(pl.multiple_of(c * half, 128), half)],
        gathered.at[:, me],
        local_sem.at[1],
    )
    local_half.start()
    local_noise = pltpu.make_async_copy(noise, noise_v, local_sem.at[2])
    local_noise.start()

    pl.semaphore_wait(barrier, nm - 1 + d + (r > 0).astype(jnp.int32))

    piece = half // PIECES
    small = half // 4
    last = nl - 1
    units = (
        [(0, 0, half)]
        + [(1, p * piece, piece) for p in range(PIECES)]
        + [(l, 0, half) for l in range(2, last)]
        + [(last, p * piece, piece) for p in range(PIECES)]
    )

    def arrival(l, lo):
        return recv_e.at[l + lo // piece] if isinstance(l, int) and l == last else recv_e.at[l]

    def send_bulk(chosen):
        for l, lo, width in chosen:
            for to in [(me + 2 * g) % nm for g in range(1, ng)] + [(sib + 2 * g) % nm for g in range(ng)]:
                rdma(
                    ensemble.at[
                        l, :, pl.ds(pl.multiple_of((to % 2) * half + lo, 128), width)
                    ],
                    gathered.at[l, me, :, pl.ds(lo, width)],
                    send_e.at[0],
                    arrival(l, lo),
                    dev(member=to),
                ).start()

    def wait_bulk(l, lo, width):
        block = gathered.at[l, pl.ds(0, nm - 1), :, pl.ds(lo, width)]
        rdma(block, block, send_e.at[0], arrival(l, lo), dev(member=sib)).wait_recv()

    send_bulk(units[:LEAD])
    for i in range(1, nd):

        @pl.when(d >= i)
        def _():
            pl.semaphore_signal(
                answer.at[0], inc=1, device_id=dev(depth=d - i), device_id_type=MESH
            )

    @pl.when(has_side[0])
    def _():
        pl.semaphore_signal(answer.at[1], inc=1, device_id=dev(region=r - 1), device_id_type=MESH)

    for copy in smalls:
        copy.wait()
    local_own.wait()
    total = own[0].astype(F32) * weights[0]
    for l in range(1, nl):
        total = total + own[l].astype(F32) * weights[l]
    hi = total.astype(BF16)
    rest = total - hi.astype(F32)
    mid = rest.astype(BF16)
    low = (rest - mid.astype(F32)).astype(BF16)
    tile_ids = lax.broadcasted_iota(jnp.int32, (tt, kk), 0)
    onehot = jnp.where(tile_ids == tiles[...], 1.0, 0.0).astype(BF16)
    terms = jnp.dot(
        jnp.concatenate([hi, mid, low], axis=0), onehot, preferred_element_type=F32
    )
    picked = terms[0:mm] + terms[mm : 2 * mm] + terms[2 * mm : 3 * mm]
    part_mean = jnp.sum(picked, axis=0, keepdims=True) / mm
    top = part_mean.astype(BF16).astype(F32)
    second_row = (part_mean - top).astype(BF16).astype(F32)
    third_row = part_mean - top - second_row
    prow = lax.broadcasted_iota(jnp.int32, (16, kk), 0)
    split = jnp.where(prow == 0, top, jnp.where(prow == 1, second_row, third_row))
    part[0:mm] = (picked - part_mean).astype(BF16)
    part[mm : mm + 16] = jnp.where(prow < 3, split, 0.0).astype(BF16)

    def whole(block):
        values_of = block.astype(F32)
        return values_of[0:mm] + jnp.sum(values_of[mm : mm + 16], axis=0, keepdims=True)

    def part_copy(i):
        to = (d + i) % nd
        return rdma(part, part_in.at[d], plane_sent.at[0], recv_p.at[i - 1], dev(depth=to))

    def part_from(i):
        frm = (d + i) % nd
        return rdma(
            part, part_in.at[frm], plane_sent.at[0], recv_p.at[nd - i - 1], dev(depth=frm)
        )

    @pl.when(d < nd - 1)
    def _():
        pl.semaphore_wait(answer.at[0], nd - 1 - d)

    for i in range(1, nd):
        part_copy(i).start()

    pos[1] = jnp.broadcast_to(tiles[...].astype(F32), (8, kk))

    def pos_copy(side):
        return rdma(
            pos.at[1],
            pos.at[2 - 2 * side],
            side_sent.at[side],
            recv_pos.at[1 - side],
            dev(region=r + (2 * side - 1)),
        )

    def pos_from(side):
        return rdma(
            pos.at[1],
            pos.at[2 * side],
            side_sent.at[side],
            recv_pos.at[side],
            dev(region=r + (2 * side - 1)),
        )

    lane = (lax.broadcasted_iota(jnp.int32, (kk, half), 1) + c * half).astype(F32)

    def make_taper(w):
        position = pos[w].T[:, 0:1] + float((w - 1) * tt)
        close = jnp.maximum(0.0, 1.0 - jnp.abs(lane - position) * (1.0 / RADIUS))
        taper[w * kk : (w + 1) * kk] = close * close

    make_taper(1)

    @pl.when(has_side[1])
    def _():
        pl.semaphore_wait(answer.at[1], 1)

    for side in (0, 1):

        @pl.when(has_side[side])
        def _():
            pos_copy(side).start()

    predicted = whole(part[...])
    for i in range(1, nd):
        part_from(i).wait_recv()
        predicted = predicted + whole(part_in[(d + i) % nd])
    own_sum = jnp.sum(predicted, axis=0, keepdims=True)
    spread_in = predicted - own_sum / mm
    own_square = jnp.sum(spread_in * spread_in, axis=0, keepdims=True)
    qrow = lax.broadcasted_iota(jnp.int32, (2, kk), 0)
    squares[me] = jnp.where(qrow == 0, own_sum, own_square)
    obs[me, :, kk : 2 * kk] = spread_in.astype(BF16)

    def square_copy(j):
        return rdma(
            squares.at[me],
            squares.at[me],
            send_q.at[0],
            recv_q.at[0],
            dev(member=(me + j) % nm),
        )

    square_rest = squares.at[pl.ds(0, nm - 1)]
    square_all = rdma(square_rest, square_rest, send_q.at[0], recv_q.at[0], dev(member=sib))

    first_part = kk // (2 * nd)
    cuts = [0] + [first_part + (kk - first_part) * h // (nd - 1) for h in range(nd)]
    parts = [(cuts[h], cuts[h + 1] - cuts[h]) for h in range(nd)]
    whole_slot = (0, kk)

    def by_depth(step, ahead=0):
        for h in range(nd):

            @pl.when(d == (h - ahead) % nd)
            def _():
                step(h)

    def obs_at(slot, w, extent):
        return obs.at[slot, :, pl.ds(w * kk + extent[0], extent[1])]

    def obs_copy(g, h):
        block = obs_at(me, 1, parts[h])
        return rdma(
            block, block, plane_sent.at[0], recv_o.at[g - 1], dev(member=(me + 2 * g) % nm)
        )

    def obs_from(g, h):
        block = obs_at(cross(g), 1, parts[h])
        return rdma(block, block, plane_sent.at[0], recv_o.at[ng - g - 1], dev(member=sib))

    def obs_swap(g, i, h):
        block = obs_at(cross(g), 1, parts[h])
        return rdma(
            block, block, plane_sent.at[0], recv_y.at[g - 1, i - 1], dev(depth=(d + i) % nd)
        )

    def swap_from(g, i, h):
        block = obs_at(cross(g), 1, parts[h])
        return rdma(
            block, block, plane_sent.at[0], recv_y.at[g - 1, nd - i - 1], dev(depth=h)
        )

    def side_obs(side, slot, extent):
        return rdma(
            obs_at(slot, 1, extent),
            obs_at(slot, 2 if side == 0 else 0, extent),
            side_sent.at[side],
            recv_z.at[1 - side],
            dev(region=r + (2 * side - 1)),
        )

    slot_bytes = mm * kk * 2
    stat_bytes = 8 * kk * 4

    def group(size):
        block = taper.at[pl.ds(0, size // (4 * half))]
        return rdma(block, block, plane_sent.at[0], recv_pert.at[0], dev(member=sib))

    def group_from(size, number):
        block = taper.at[pl.ds(0, size // (4 * half))]
        return rdma(block, block, side_sent.at[number], recv_z.at[number], dev(member=sib))

    def sent_of(w):
        return plane_sent.at[0] if w == 1 else side_sent.at[w // 2]

    def obs_forward(w, slot, extent, number):
        block = obs_at(slot, w, extent)
        return rdma(block, block, sent_of(w), recv_f.at[number], dev(member=sib))

    def forward_all(w, wide, number):
        block = obs.at[pl.ds(0, wide[0]), :, pl.ds(0, wide[1])]
        return rdma(block, block, sent_of(w), recv_f.at[number], dev(member=sib))

    def cross(g):
        return 2 * ((q + g) % ng) + c

    for j in range(1, nm):
        square_copy(j).start()
    by_depth(lambda h: [obs_copy(g, h).start() for g in range(1, ng)])
    obs_forward(1, me, whole_slot, 0).start()
    send_bulk(units[LEAD:])
    for side in (0, 1):

        @pl.when(has_side[side])
        def _():
            side_obs(side, me, whole_slot).start()
            pos_from(side).wait_recv()
            make_taper(2 * side)

    square_all.wait_recv()
    moments = [squares[j] for j in range(nm)]
    obs_mean = sum(m[0:1] for m in moments) / members
    deviation = predicted - obs_mean
    square_sum = sum(
        m[1:2] + mm * (m[0:1] / mm - obs_mean) * (m[0:1] / mm - obs_mean) for m in moments
    )
    spread = square_sum / (members - 1)
    error = errors[...]
    innovation = values[...] - obs_mean
    first = jnp.sum(innovation * innovation, axis=1, keepdims=True)
    second = jnp.sum(spread + error, axis=1, keepdims=True)
    rp = tot_in.shape[1]
    trow = lax.broadcasted_iota(jnp.int32, (rp, 128), 0)
    tlane = lax.broadcasted_iota(jnp.int32, (rp, 128), 1)
    own_total = jnp.where(tlane == 0, first, second)
    krow = lax.broadcasted_iota(jnp.int32, (8, kk), 0)
    shifts_of = jnp.zeros((8, kk), F32)
    for g in range(nm):
        shifts_of = jnp.where(krow == g, moments[g][0:1] / mm - obs_mean, shifts_of)
    stats[1] = shifts_of

    def stat_copy(side):
        return rdma(
            stats.at[1],
            stats.at[2 - 2 * side],
            side_sent.at[side],
            recv_z.at[1 - side],
            dev(region=r + (2 * side - 1)),
        )

    def total_copy(way):
        return rdma(
            tot_out.at[way],
            tot_in.at[way],
            send_g.at[way],
            recv_g.at[way],
            dev(region=r + (1 - 2 * way)),
        )

    def total_from(way):
        return rdma(
            tot_out.at[way],
            tot_in.at[way],
            send_g.at[way],
            recv_g.at[way],
            dev(region=r - (1 - 2 * way)),
        )

    def relay(way):
        @pl.when(has_side[way])
        def _():
            total_from(way).wait_recv()

        behind = trow < r if way == 0 else trow > r
        tot_out[way] = jnp.where(
            behind, tot_in[way], jnp.where(trow == r, own_total, 0.0)
        )

        @pl.when(has_side[1 - way])
        def _():
            total_copy(way).start()

    low_end = r == 0
    high_end = r == nr - 1

    @pl.when(low_end)
    def _():
        relay(0)

    @pl.when(high_end)
    def _():
        relay(1)

    for side in (0, 1):

        @pl.when(has_side[side])
        def _():
            stat_copy(side).start()

    def hand_part(g, i, h):
        for side in (0, 1):

            @pl.when(has_side[side])
            def _():
                side_obs(side, cross(g), parts[h]).start()

        obs_forward(1, cross(g), parts[h], i).start()

    def take_part(h):
        for g in range(1, ng):
            obs_from(g, h).wait_recv()
            for i in range(1, nd):
                obs_swap(g, i, h).start()
            hand_part(g, 0, h)

    by_depth(take_part)

    def transpose_part(w, extent):
        lo, width = extent
        rows_of = pl.ds(w * kk + lo, width)
        shifts = stats[w, :, lo : lo + width].T
        for g in range(nm):
            block = obs[g, :, rows_of].astype(F32).T + shifts[:, g : g + 1]
            obs_t[rows_of, g * mm : (g + 1) * mm] = block.astype(BF16)

    everything = (0, half)

    middle = jnp.logical_and(has_side[0], has_side[1])
    beside = jnp.where(has_side[0], 0, 2)

    def by_place(step):
        @pl.when(middle)
        def _():
            step((0, 2))

        @pl.when(jnp.logical_not(middle))
        def _():
            step((beside,))

    def span(w):
        return pl.ds(w * kk if isinstance(w, int) else pl.multiple_of(w * kk, 128), kk)

    def gain_rows(l, windows, columns=everything):
        cols = slice(*columns)
        right = anom[l, :, :, cols].reshape(members, columns[1] - columns[0])
        for w in windows:
            cov = jnp.dot(obs_t[span(w)], right, preferred_element_type=F32)
            gain[l, span(w), cols] = (cov * taper[span(w), cols]).astype(BF16)

    def gain_part(l, h):
        at = pl.ds(kk + parts[h][0], parts[h][1])
        cov = jnp.dot(
            obs_t[at], anom[l].reshape(members, half), preferred_element_type=F32
        )
        gain[l, at] = (cov * taper[at]).astype(BF16)

    def wait_variable(l, columns=everything):
        wait_bulk(l, columns[0], columns[1] - columns[0])

    def center(l, columns=everything):
        cols = slice(*columns)
        raw = gathered[l, :, :, cols].astype(F32)
        mean = jnp.sum(jnp.sum(raw, axis=0), axis=0, keepdims=True) / members
        means[l, :, cols] = jnp.broadcast_to(mean, (8, columns[1] - columns[0]))
        anom[l, :, :, cols] = (raw - mean[None]).astype(BF16)

    def own_window(l, windows, columns=everything):
        center(l, columns)
        gain_rows(l, windows, columns)

    def sib_pert(slot):
        block = pert.at[slot, :, pl.ds(kk, kk)]
        return rdma(block, block, plane_sent.at[0], recv_pert.at[0], dev(member=sib))

    def side_pert(side):
        window = 2 * kk if side == 0 else 0
        return rdma(
            pert.at[c, :, pl.ds(kk, kk)],
            pert.at[c, :, pl.ds(window, kk)],
            side_sent.at[side],
            recv_pz.at[1 - side],
            dev(region=r + (2 * side - 1)),
        )

    def pert_forward(side, slot):
        block = pert.at[slot, :, pl.ds(2 * kk * side, kk)]
        return rdma(block, block, side_sent.at[side], recv_pert.at[0], dev(member=sib))

    def make_pert():
        everyone = jnp.where(trow < r, tot_in[0], jnp.where(trow > r, tot_in[1], own_total))
        grand = everyone[0:1]
        for i in range(1, nr):
            grand = grand + everyone[i : i + 1]
        inflation = grand[0:1, 0:1] / grand[0:1, 1:2]
        root = jnp.sqrt(inflation)
        infl_out[...] = inflation
        scale[...] = jnp.broadcast_to(root, (1, 128))
        factor = inflation / (inflation * spread + error)
        local_noise.wait()
        pert[c, :, kk : 2 * kk] = (
            (innovation + jnp.sqrt(error) * noise_v[...] - root * deviation)
            * (factor / (members - 1))
        ).astype(BF16)

        sib_pert(c).start()
        for side in (0, 1):

            @pl.when(has_side[side])
            def _():
                side_pert(side).start()

    mid_low = jnp.logical_and(r > 0, 2 * r < nr)
    mid_high = jnp.logical_and(r < nr - 1, 2 * r >= nr)

    @pl.when(mid_low)
    def _():
        relay(0)

    @pl.when(mid_high)
    def _():
        relay(1)

    local_half.wait()
    wait_variable(0)
    center(0)

    def own_part(h):
        forward_all(1, (1, kk + (ng - 1) * parts[h][1]), 0).wait_recv()
        transpose_part(1, parts[h])
        gain_part(0, h)

    by_depth(own_part)

    def swap_part(i, h):
        for g in range(1, ng):
            swap_from(g, i, h).wait_recv()
            hand_part(g, i, h)

    for i in range(1, nd):
        by_depth(functools.partial(swap_part, i), i)
    wait_variable(1)
    center(1)
    by_depth(lambda h: gain_part(1, h))

    @pl.when(mid_low)
    def _():
        relay(1)
        make_pert()

    @pl.when(mid_high)
    def _():
        relay(0)
        make_pert()

    def other_part(i, h):
        forward_all(1, (1, (ng - 1) * parts[h][1]), i).wait_recv()
        transpose_part(1, parts[h])
        gain_part(0, h)
        gain_part(1, h)

    for i in range(1, nd):
        by_depth(functools.partial(other_part, i), i)
    wait_variable(2)
    own_window(2, (1,))

    for side in (0, 1):

        @pl.when(has_side[side])
        def _():
            group_from(ng * slot_bytes + stat_bytes, side).wait_recv()
            for g in range(ng):
                obs_forward(2 * side, cross(g), whole_slot, nd + side).start()


    @pl.when(low_end)
    def _():
        relay(1)
        make_pert()

    @pl.when(high_end)
    def _():
        relay(0)
        make_pert()

    for side in (0, 1):

        @pl.when(has_side[side])
        def _():
            forward_all(2 * side, (ng, kk), nd + side).wait_recv()

            transpose_part(2 * side, whole_slot)

    def out_block(l, which, columns):
        lo, width = columns[0], columns[1] - columns[0]
        return out.at[l, :, pl.ds(pl.multiple_of(which * half + lo, 128), width)]

    def out_copies(l, columns):
        cols = slice(*columns)
        there = rdma(
            result.at[l, 1 - c, :, cols],
            out_block(l, c, columns),
            send_out.at[0],
            recv_out.at[0],
            dev(member=sib),
        )
        here = pltpu.make_async_copy(
            result.at[l, c, :, cols], out_block(l, c, columns), local_sem.at[0]
        )
        return there, here

    def finish_variable(l, sides, columns=everything):
        cols = slice(*columns)
        width = columns[1] - columns[0]
        if len(sides) == 2:
            increment = jnp.dot(
                pert[...].reshape(2 * mm, 3 * kk), gain[l, :, cols], preferred_element_type=F32
            )
        else:
            increment = jnp.zeros((2 * mm, width), F32)
            for w in (1,) + sides:
                increment = increment + jnp.dot(
                    pert[:, :, span(w)].reshape(2 * mm, kk),
                    gain[l, span(w), cols],
                    preferred_element_type=F32,
                )
        base = means[l, 0:1, cols][None] + scale[0:1, 0:1][None] * anom[
            l, pl.ds(2 * q, 2), :, cols
        ].astype(F32)
        result[l, :, :, cols] = (base + increment.reshape(2, mm, width)).astype(BF16)

    def send_result(l, columns=everything):
        for copy in out_copies(l, columns):
            copy.start()

    def early_gain(sides):
        def step(l, carry):
            gain_rows(l, sides)
            return carry

        lax.fori_loop(0, 3, step, 0)

    by_place(early_gain)
    for side in (0, 1):

        @pl.when(has_side[side])
        def _():
            side_pert(1 - side).wait_recv()
            pert_forward(side, c).start()

    ready = min(READY, last)

    def ahead(l, carry):
        wait_variable(l)
        by_place(lambda sides: own_window(l, (1,) + sides))
        return carry

    lax.fori_loop(3, ready, ahead, 0)
    @pl.when(middle)
    def _():
        group(3 * slot_bytes).wait_recv()

    @pl.when(jnp.logical_not(middle))
    def _():
        group(2 * slot_bytes).wait_recv()

    def late_variable(l, carry):
        by_place(lambda sides: finish_variable(l, sides))
        send_result(l)
        return carry

    lax.fori_loop(0, ready, late_variable, 0)

    def whole_variable(l, columns=everything):
        wait_variable(l, columns)

        def step(sides):
            own_window(l, (1,) + sides, columns)
            finish_variable(l, sides, columns)

        by_place(step)
        send_result(l, columns)

    def one_variable(l, carry):
        whole_variable(l)
        return carry

    lax.fori_loop(ready, last, one_variable, 0)
    for p in range(PIECES):
        whole_variable(last, (p * piece, (p + 1) * piece))

    sent = gathered.at[:, pl.ds(0, nm - 1)]
    rdma(sent, sent, send_e.at[0], recv_e.at[0], dev(member=sib)).wait_send()
    mine = out.at[:, :, pl.ds(pl.multiple_of(c * half, 128), half)]
    other = out.at[:, :, pl.ds(pl.multiple_of((1 - c) * half, 128), half)]
    pltpu.make_async_copy(mine, mine, local_sem.at[0]).wait()
    theirs = rdma(other, other, send_out.at[0], recv_out.at[0], dev(member=sib))
    theirs.wait_send()
    theirs.wait_recv()
    square_all.wait_send()

    def plane_done(h):
        part_bytes = mm * parts[h][1] * 2
        group(
            (nd - 1) * (mm + 16) * kk * 2
            + (ng + 1) * slot_bytes
            + (ng - 1) * nd * part_bytes
        ).wait_send()

    by_depth(plane_done)
    for way in (0, 1):

        @pl.when(has_side[1 - way])
        def _():
            total_copy(way).wait_send()

    for side in (0, 1):

        @pl.when(has_side[side])
        def _():
            group_from((2 * ng + 2) * slot_bytes + 2 * stat_bytes, side).wait_send()


def hand_on(block, out):
    pass


def solution(mesh):
    nr, nd, nm = (mesh.shape[a] for a in ("region", "depth", "member"))

    def shards(ensemble, obs_weights, obs_tiles, obs_values, obs_error, obs_noise):
        nl, mm, tt = ensemble.shape
        kk = obs_tiles.shape[0]
        ng = nm // 2
        half = tt // 2
        rp = -(-nr // 8) * 8
        dma = pltpu.SemaphoreType.DMA
        vmem = pl.BlockSpec(memory_space=pltpu.VMEM)
        anywhere = pl.BlockSpec(memory_space=pl.ANY)
        analysis, inflation = pl.pallas_call(
            functools.partial(kernel, (nr, nd, nm, nl, mm, tt, kk)),
            out_shape=(
                pltpu.VMEM((nl, mm, tt), BF16),
                pltpu.VMEM((1, 1), F32),
            ),
            in_specs=[anywhere] * 6,
            out_specs=(vmem, vmem),
            scratch_shapes=[
                pltpu.SMEM((nl,), F32),
                pltpu.VMEM((1, kk), jnp.int32),
                pltpu.VMEM((1, kk), F32),
                pltpu.VMEM((1, kk), F32),
                pltpu.VMEM((nl, mm, tt), BF16),
                pltpu.VMEM((nl, nm, mm, half), BF16),
                pltpu.VMEM((mm, kk), F32),
                pltpu.VMEM((mm + 16, kk), BF16),
                pltpu.VMEM((nd, mm + 16, kk), BF16),
                pltpu.VMEM((nm, 2, kk), F32),
                pltpu.VMEM((2, rp, 128), F32),
                pltpu.VMEM((2, rp, 128), F32),
                pltpu.VMEM((3, 8, kk), F32),
                pltpu.VMEM((3, 8, kk), F32),
                pltpu.VMEM((nm, mm, 3 * kk), BF16),
                pltpu.VMEM((2, mm, 3 * kk), BF16),
                pltpu.VMEM((3 * kk, nm * mm), BF16),
                pltpu.VMEM((3 * kk, half), F32),
                pltpu.VMEM((nl, nm, mm, half), BF16),
                pltpu.VMEM((nl, 8, half), F32),
                pltpu.VMEM((nl, 3 * kk, half), BF16),
                pltpu.VMEM((nl, 2, mm, half), BF16),
                pltpu.VMEM((1, 128), F32),
                pltpu.SemaphoreType.REGULAR((2,)),
                dma((1,)),
                dma((2,)),
                dma((1,)),
                dma((4,)),
                dma((3,)),
                dma((1,)),
                dma((nl - 1 + PIECES,)),
                dma((nd - 1,)),
                dma((1,)),
                dma((1,)),
                dma((ng - 1,)),
                dma((2,)),
                dma((2,)),
                dma((ng - 1, nd - 1)),
                dma((2,)),
                dma((2,)),
                dma((2,)),
                dma((nd + 2,)),
                dma((1,)),
                dma((1,)),
            ],
            compiler_params=pltpu.CompilerParams(
                collective_id=0, has_side_effects=True, vmem_limit_bytes=56 * 1024 * 1024
            ),
        )(
            obs_weights,
            ensemble,
            obs_tiles.reshape(1, kk),
            obs_values.reshape(1, kk),
            obs_error.reshape(1, kk),
            obs_noise,
        )
        analysis = pl.pallas_call(
            hand_on,
            out_shape=jax.ShapeDtypeStruct((nl, mm, tt), BF16),
            in_specs=[anywhere],
            out_specs=anywhere,
            input_output_aliases={0: 0},
        )(analysis)
        return analysis, inflation.reshape(())

    return jax.shard_map(
        shards,
        mesh=mesh,
        in_specs=(
            P("depth", "member", "region"),
            P("depth"),
            P("region"),
            P("region"),
            P("region"),
            P("member", "region"),
        ),
        out_specs=(P("depth", "member", "region"), P()),
        check_vma=False,
    )
```

```python
import functools

import jax
import jax.numpy as jnp
from jax import lax
from jax.experimental import pallas as pl
from jax.experimental.pallas import tpu as pltpu
from jax.sharding import PartitionSpec as P

RADIUS = 1024
LEAD = 2
READY = 4
PIECES = 2
F32 = jnp.float32
BF16 = jnp.bfloat16
MESH = pl.DeviceIdType.MESH


def kernel(
    sizes,
    weights_hbm,
    ensemble,
    tiles_hbm,
    values_hbm,
    errors_hbm,
    noise,
    out,
    infl_out,
    weights,
    tiles,
    values,
    errors,
    own,
    gathered,
    noise_v,
    part,
    part_in,
    squares,
    tot_in,
    tot_out,
    pos,
    stats,
    obs,
    pert,
    obs_t,
    taper,
    anom,
    means,
    gain,
    result,
    scale,
    answer,
    plane_sent,
    side_sent,
    recv_pert,
    small_sem,
    local_sem,
    send_e,
    recv_e,
    recv_p,
    send_q,
    recv_q,
    recv_o,
    send_g,
    recv_g,
    recv_y,
    recv_z,
    recv_pos,
    recv_pz,
    recv_f,
    send_out,
    recv_out,
):
    nr, nd, nm, nl, mm, tt, kk = sizes
    ng = nm // 2
    half = tt // 2
    members = nm * mm
    r = lax.axis_index("region")
    d = lax.axis_index("depth")
    me = lax.axis_index("member")
    q = me // 2
    c = me % 2
    sib = 2 * q + (1 - c)
    has_side = (r > 0, r < nr - 1)

    def dev(region=None, depth=None, member=None):
        return {
            "region": r if region is None else region,
            "depth": d if depth is None else depth,
            "member": me if member is None else member,
        }

    def rdma(src, dst, ssem, rsem, device):
        return pltpu.make_async_remote_copy(
            src_ref=src,
            dst_ref=dst,
            send_sem=ssem,
            recv_sem=rsem,
            device_id=device,
            device_id_type=MESH,
        )

    barrier = pltpu.get_barrier_semaphore()
    for j in range(1, nm):
        pl.semaphore_signal(
            barrier, inc=1, device_id=dev(member=(me + j) % nm), device_id_type=MESH
        )
    for i in range(1, nd):

        @pl.when(d + i < nd)
        def _():
            pl.semaphore_signal(barrier, inc=1, device_id=dev(depth=d + i), device_id_type=MESH)

    @pl.when(has_side[1])
    def _():
        pl.semaphore_signal(barrier, inc=1, device_id=dev(region=r + 1), device_id_type=MESH)

    local_own = pltpu.make_async_copy(ensemble, own, local_sem.at[0])
    local_own.start()
    smalls = [
        pltpu.make_async_copy(a, b, small_sem.at[i])
        for i, (a, b) in enumerate(
            ((weights_hbm, weights), (tiles_hbm, tiles), (values_hbm, values), (errors_hbm, errors))
        )
    ]
    for copy in smalls:
        copy.start()
    local_half = pltpu.make_async_copy(
        ensemble.at[:, :, pl.ds(pl.multiple_of(c * half, 128), half)],
        gathered.at[:, me],
        local_sem.at[1],
    )
    local_half.start()
    local_noise = pltpu.make_async_copy(noise, noise_v, local_sem.at[2])
    local_noise.start()

    pl.semaphore_wait(barrier, nm - 1 + d + (r > 0).astype(jnp.int32))

    piece = half // PIECES
    small = half // 4
    last = nl - 1
    units = (
        [(0, 0, half)]
        + [(1, p * piece, piece) for p in range(PIECES)]
        + [(l, 0, half) for l in range(2, last)]
        + [(last, p * piece, piece) for p in range(PIECES)]
    )

    def arrival(l, lo):
        return recv_e.at[l + lo // piece] if isinstance(l, int) and l == last else recv_e.at[l]

    def send_bulk(chosen):
        for l, lo, width in chosen:
            for to in [(me + 2 * g) % nm for g in range(1, ng)] + [(sib + 2 * g) % nm for g in range(ng)]:
                rdma(
                    ensemble.at[
                        l, :, pl.ds(pl.multiple_of((to % 2) * half + lo, 128), width)
                    ],
                    gathered.at[l, me, :, pl.ds(lo, width)],
                    send_e.at[0],
                    arrival(l, lo),
                    dev(member=to),
                ).start()

    def wait_bulk(l, lo, width):
        block = gathered.at[l, pl.ds(0, nm - 1), :, pl.ds(lo, width)]
        rdma(block, block, send_e.at[0], arrival(l, lo), dev(member=sib)).wait_recv()

    send_bulk(units[:LEAD])
    for i in range(1, nd):

        @pl.when(d >= i)
        def _():
            pl.semaphore_signal(
                answer.at[0], inc=1, device_id=dev(depth=d - i), device_id_type=MESH
            )

    @pl.when(has_side[0])
    def _():
        pl.semaphore_signal(answer.at[1], inc=1, device_id=dev(region=r - 1), device_id_type=MESH)

    for copy in smalls:
        copy.wait()
    local_own.wait()
    total = own[0].astype(F32) * weights[0]
    for l in range(1, nl):
        total = total + own[l].astype(F32) * weights[l]
    hi = total.astype(BF16)
    rest = total - hi.astype(F32)
    mid = rest.astype(BF16)
    low = (rest - mid.astype(F32)).astype(BF16)
    tile_ids = lax.broadcasted_iota(jnp.int32, (tt, kk), 0)
    onehot = jnp.where(tile_ids == tiles[...], 1.0, 0.0).astype(BF16)
    terms = jnp.dot(
        jnp.concatenate([hi, mid, low], axis=0), onehot, preferred_element_type=F32
    )
    picked = terms[0:mm] + terms[mm : 2 * mm] + terms[2 * mm : 3 * mm]
    part_mean = jnp.sum(picked, axis=0, keepdims=True) / mm
    top = part_mean.astype(BF16).astype(F32)
    second_row = (part_mean - top).astype(BF16).astype(F32)
    third_row = part_mean - top - second_row
    prow = lax.broadcasted_iota(jnp.int32, (16, kk), 0)
    split = jnp.where(prow == 0, top, jnp.where(prow == 1, second_row, third_row))
    part[0:mm] = (picked - part_mean).astype(BF16)
    part[mm : mm + 16] = jnp.where(prow < 3, split, 0.0).astype(BF16)

    def whole(block):
        values_of = block.astype(F32)
        return values_of[0:mm] + jnp.sum(values_of[mm : mm + 16], axis=0, keepdims=True)

    def part_copy(i):
        to = (d + i) % nd
        return rdma(part, part_in.at[d], plane_sent.at[0], recv_p.at[i - 1], dev(depth=to))

    def part_from(i):
        frm = (d + i) % nd
        return rdma(
            part, part_in.at[frm], plane_sent.at[0], recv_p.at[nd - i - 1], dev(depth=frm)
        )

    @pl.when(d < nd - 1)
    def _():
        pl.semaphore_wait(answer.at[0], nd - 1 - d)

    for i in range(1, nd):
        part_copy(i).start()

    pos[1] = jnp.broadcast_to(tiles[...].astype(F32), (8, kk))

    def pos_copy(side):
        return rdma(
            pos.at[1],
            pos.at[2 - 2 * side],
            side_sent.at[side],
            recv_pos.at[1 - side],
            dev(region=r + (2 * side - 1)),
        )

    def pos_from(side):
        return rdma(
            pos.at[1],
            pos.at[2 * side],
            side_sent.at[side],
            recv_pos.at[side],
            dev(region=r + (2 * side - 1)),
        )

    lane = (lax.broadcasted_iota(jnp.int32, (kk, half), 1) + c * half).astype(F32)

    def make_taper(w):
        position = pos[w].T[:, 0:1] + float((w - 1) * tt)
        close = jnp.maximum(0.0, 1.0 - jnp.abs(lane - position) * (1.0 / RADIUS))
        taper[w * kk : (w + 1) * kk] = close * close

    make_taper(1)

    @pl.when(has_side[1])
    def _():
        pl.semaphore_wait(answer.at[1], 1)

    for side in (0, 1):

        @pl.when(has_side[side])
        def _():
            pos_copy(side).start()

    predicted = whole(part[...])
    for i in range(1, nd):
        part_from(i).wait_recv()
        predicted = predicted + whole(part_in[(d + i) % nd])
    own_sum = jnp.sum(predicted, axis=0, keepdims=True)
    spread_in = predicted - own_sum / mm
    own_square = jnp.sum(spread_in * spread_in, axis=0, keepdims=True)
    qrow = lax.broadcasted_iota(jnp.int32, (2, kk), 0)
    squares[me] = jnp.where(qrow == 0, own_sum, own_square)
    obs[me, :, kk : 2 * kk] = spread_in.astype(BF16)

    def square_copy(j):
        return rdma(
            squares.at[me],
            squares.at[me],
            send_q.at[0],
            recv_q.at[0],
            dev(member=(me + j) % nm),
        )

    square_rest = squares.at[pl.ds(0, nm - 1)]
    square_all = rdma(square_rest, square_rest, send_q.at[0], recv_q.at[0], dev(member=sib))

    def cuts(first):
        at = [0] + [first + (kk - first) * h // (nd - 1) for h in range(nd)]
        return [(at[h], at[h + 1] - at[h]) for h in range(nd)]

    shares = (cuts(kk // nd), cuts(kk // (2 * nd)))
    whole_slot = (0, kk)
    first_region = jnp.logical_and(r == 0, ng == 2)
    sends_late = jnp.logical_and(first_region, q == 1)
    takes_late = jnp.logical_and(first_region, q == 0)

    def by_depth(step, ahead=0, late=takes_late):
        for h in range(nd):
            for parts, chosen in zip(shares, (jnp.logical_not(late), late)):

                @pl.when(jnp.logical_and(d == (h - ahead) % nd, chosen))
                def _():
                    step(parts[h])

    def obs_at(slot, w, extent):
        return obs.at[slot, :, pl.ds(w * kk + extent[0], extent[1])]

    def obs_copy(g, extent):
        block = obs_at(me, 1, extent)
        return rdma(
            block, block, plane_sent.at[0], recv_o.at[g - 1], dev(member=(me + 2 * g) % nm)
        )

    def obs_from(g, extent):
        block = obs_at(cross(g), 1, extent)
        return rdma(block, block, plane_sent.at[0], recv_o.at[ng - g - 1], dev(member=sib))

    def obs_swap(g, i, extent):
        block = obs_at(cross(g), 1, extent)
        return rdma(
            block, block, plane_sent.at[0], recv_y.at[g - 1, i - 1], dev(depth=(d + i) % nd)
        )

    def swap_from(g, i, extent):
        block = obs_at(cross(g), 1, extent)
        return rdma(
            block, block, plane_sent.at[0], recv_y.at[g - 1, nd - i - 1], dev(depth=(d + i) % nd)
        )

    def side_obs(side, slot, extent):
        return rdma(
            obs_at(slot, 1, extent),
            obs_at(slot, 2 if side == 0 else 0, extent),
            side_sent.at[side],
            recv_z.at[1 - side],
            dev(region=r + (2 * side - 1)),
        )

    slot_bytes = mm * kk * 2
    stat_bytes = 8 * kk * 4

    def group(size):
        block = taper.at[pl.ds(0, size // (4 * piece)), pl.ds(0, piece)]
        return rdma(block, block, plane_sent.at[0], recv_pert.at[0], dev(member=sib))

    def group_from(size, number):
        block = taper.at[pl.ds(0, size // (4 * piece)), pl.ds(0, piece)]
        return rdma(block, block, side_sent.at[number], recv_z.at[number], dev(member=sib))

    def sent_of(w):
        return plane_sent.at[0] if w == 1 else side_sent.at[w // 2]

    def obs_forward(w, slot, extent, number):
        block = obs_at(slot, w, extent)
        return rdma(block, block, sent_of(w), recv_f.at[number], dev(member=sib))

    def forward_all(w, wide, number):
        block = obs.at[pl.ds(0, wide[0]), :, pl.ds(0, wide[1])]
        return rdma(block, block, sent_of(w), recv_f.at[number], dev(member=sib))

    def cross(g):
        return 2 * ((q + g) % ng) + c

    for j in range(1, nm):
        square_copy(j).start()
    by_depth(
        lambda extent: [obs_copy(g, extent).start() for g in range(1, ng)], late=sends_late
    )
    obs_forward(1, me, whole_slot, 0).start()
    send_bulk(units[LEAD:])
    for side in (0, 1):

        @pl.when(has_side[side])
        def _():
            side_obs(side, me, whole_slot).start()
            pos_from(side).wait_recv()
            make_taper(2 * side)

    square_all.wait_recv()
    moments = [squares[j] for j in range(nm)]
    obs_mean = sum(m[0:1] for m in moments) / members
    deviation = predicted - obs_mean
    square_sum = sum(
        m[1:2] + mm * (m[0:1] / mm - obs_mean) * (m[0:1] / mm - obs_mean) for m in moments
    )
    spread = square_sum / (members - 1)
    error = errors[...]
    innovation = values[...] - obs_mean
    first = jnp.sum(innovation * innovation, axis=1, keepdims=True)
    second = jnp.sum(spread + error, axis=1, keepdims=True)
    rp = tot_in.shape[1]
    trow = lax.broadcasted_iota(jnp.int32, (rp, 128), 0)
    tlane = lax.broadcasted_iota(jnp.int32, (rp, 128), 1)
    own_total = jnp.where(tlane == 0, first, second)
    krow = lax.broadcasted_iota(jnp.int32, (8, kk), 0)
    shifts_of = jnp.zeros((8, kk), F32)
    for g in range(nm):
        shifts_of = jnp.where(krow == g, moments[g][0:1] / mm - obs_mean, shifts_of)
    stats[1] = shifts_of

    def stat_copy(side):
        return rdma(
            stats.at[1],
            stats.at[2 - 2 * side],
            side_sent.at[side],
            recv_z.at[1 - side],
            dev(region=r + (2 * side - 1)),
        )

    def total_copy(way):
        return rdma(
            tot_out.at[way],
            tot_in.at[way],
            send_g.at[way],
            recv_g.at[way],
            dev(region=r + (1 - 2 * way)),
        )

    def total_from(way):
        return rdma(
            tot_out.at[way],
            tot_in.at[way],
            send_g.at[way],
            recv_g.at[way],
            dev(region=r - (1 - 2 * way)),
        )

    def relay(way):
        @pl.when(has_side[way])
        def _():
            total_from(way).wait_recv()

        behind = trow < r if way == 0 else trow > r
        tot_out[way] = jnp.where(
            behind, tot_in[way], jnp.where(trow == r, own_total, 0.0)
        )

        @pl.when(has_side[1 - way])
        def _():
            total_copy(way).start()

    low_end = r == 0
    high_end = r == nr - 1

    @pl.when(low_end)
    def _():
        relay(0)

    @pl.when(high_end)
    def _():
        relay(1)

    for side in (0, 1):

        @pl.when(has_side[side])
        def _():
            stat_copy(side).start()

    def hand_part(g, i, extent):
        for side in (0, 1):

            @pl.when(has_side[side])
            def _():
                side_obs(side, cross(g), extent).start()

        obs_forward(1, cross(g), extent, i).start()

    def take_part(extent):
        for g in range(1, ng):
            obs_from(g, extent).wait_recv()
            for i in range(1, nd):
                obs_swap(g, i, extent).start()
            hand_part(g, 0, extent)

    by_depth(take_part)

    def transpose_part(w, extent):
        lo, width = extent
        rows_of = pl.ds(w * kk + lo, width)
        shifts = stats[w, :, lo : lo + width].T
        for g in range(nm):
            block = obs[g, :, rows_of].astype(F32).T + shifts[:, g : g + 1]
            obs_t[rows_of, g * mm : (g + 1) * mm] = block.astype(BF16)

    everything = (0, half)

    middle = jnp.logical_and(has_side[0], has_side[1])
    beside = jnp.where(has_side[0], 0, 2)

    def by_place(step):
        @pl.when(middle)
        def _():
            step((0, 2))

        @pl.when(jnp.logical_not(middle))
        def _():
            step((beside,))

    def span(w):
        return pl.ds(w * kk if isinstance(w, int) else pl.multiple_of(w * kk, 128), kk)

    def gain_rows(l, windows, columns=everything):
        cols = slice(*columns)
        right = anom[l, :, :, cols].reshape(members, columns[1] - columns[0])
        for w in windows:
            cov = jnp.dot(obs_t[span(w)], right, preferred_element_type=F32)
            gain[l, span(w), cols] = (cov * taper[span(w), cols]).astype(BF16)

    def gain_part(l, extent):
        at = pl.ds(kk + extent[0], extent[1])
        cov = jnp.dot(
            obs_t[at], anom[l].reshape(members, half), preferred_element_type=F32
        )
        gain[l, at] = (cov * taper[at]).astype(BF16)

    def wait_variable(l, columns=everything):
        wait_bulk(l, columns[0], columns[1] - columns[0])

    def center(l, columns=everything):
        cols = slice(*columns)
        raw = gathered[l, :, :, cols].astype(F32)
        mean = jnp.sum(jnp.sum(raw, axis=0), axis=0, keepdims=True) / members
        means[l, :, cols] = jnp.broadcast_to(mean, (8, columns[1] - columns[0]))
        anom[l, :, :, cols] = (raw - mean[None]).astype(BF16)

    def own_window(l, windows, columns=everything):
        center(l, columns)
        gain_rows(l, windows, columns)

    def sib_pert(slot):
        block = pert.at[slot, :, pl.ds(kk, kk)]
        return rdma(block, block, plane_sent.at[0], recv_pert.at[0], dev(member=sib))

    def side_pert(side):
        window = 2 * kk if side == 0 else 0
        return rdma(
            pert.at[c, :, pl.ds(kk, kk)],
            pert.at[c, :, pl.ds(window, kk)],
            side_sent.at[side],
            recv_pz.at[1 - side],
            dev(region=r + (2 * side - 1)),
        )

    def pert_forward(side, slot):
        block = pert.at[slot, :, pl.ds(2 * kk * side, kk)]
        return rdma(block, block, side_sent.at[side], recv_pert.at[0], dev(member=sib))

    def make_pert():
        everyone = jnp.where(trow < r, tot_in[0], jnp.where(trow > r, tot_in[1], own_total))
        grand = everyone[0:1]
        for i in range(1, nr):
            grand = grand + everyone[i : i + 1]
        inflation = grand[0:1, 0:1] / grand[0:1, 1:2]
        root = jnp.sqrt(inflation)
        infl_out[...] = inflation
        scale[...] = jnp.broadcast_to(root, (1, 128))
        factor = inflation / (inflation * spread + error)
        local_noise.wait()
        pert[c, :, kk : 2 * kk] = (
            (innovation + jnp.sqrt(error) * noise_v[...] - root * deviation)
            * (factor / (members - 1))
        ).astype(BF16)

        sib_pert(c).start()
        for side in (0, 1):

            @pl.when(has_side[side])
            def _():
                side_pert(side).start()

    mid_low = jnp.logical_and(r > 0, 2 * r < nr)
    mid_high = jnp.logical_and(r < nr - 1, 2 * r >= nr)

    @pl.when(mid_low)
    def _():
        relay(0)

    @pl.when(mid_high)
    def _():
        relay(1)

    local_half.wait()
    wait_variable(0)
    center(0)

    def own_part(extent):
        forward_all(1, (1, kk + (ng - 1) * extent[1]), 0).wait_recv()
        transpose_part(1, extent)
        gain_part(0, extent)

    by_depth(own_part)

    def swap_part(i, extent):
        for g in range(1, ng):
            swap_from(g, i, extent).wait_recv()
            hand_part(g, i, extent)

    for i in range(1, nd):
        by_depth(functools.partial(swap_part, i), i)
    wait_variable(1)
    center(1)
    by_depth(lambda extent: gain_part(1, extent))

    @pl.when(mid_low)
    def _():
        relay(1)
        make_pert()

    @pl.when(mid_high)
    def _():
        relay(0)
        make_pert()

    def other_part(i, extent):
        forward_all(1, (1, (ng - 1) * extent[1]), i).wait_recv()
        transpose_part(1, extent)
        gain_part(0, extent)
        gain_part(1, extent)

    for i in range(1, nd):
        by_depth(functools.partial(other_part, i), i)
    wait_variable(2)
    own_window(2, (1,))

    for side in (0, 1):

        @pl.when(has_side[side])
        def _():
            group_from(ng * slot_bytes + stat_bytes, side).wait_recv()
            for g in range(ng):
                obs_forward(2 * side, cross(g), whole_slot, nd + side).start()


    @pl.when(low_end)
    def _():
        relay(1)
        make_pert()

    @pl.when(high_end)
    def _():
        relay(0)
        make_pert()

    for side in (0, 1):

        @pl.when(has_side[side])
        def _():
            forward_all(2 * side, (ng, kk), nd + side).wait_recv()

            transpose_part(2 * side, whole_slot)

    def out_block(l, which, columns):
        lo, width = columns[0], columns[1] - columns[0]
        return out.at[l, :, pl.ds(pl.multiple_of(which * half + lo, 128), width)]

    def out_copies(l, columns):
        cols = slice(*columns)
        there = rdma(
            result.at[l, 1 - c, :, cols],
            out_block(l, c, columns),
            send_out.at[0],
            recv_out.at[0],
            dev(member=sib),
        )
        here = pltpu.make_async_copy(
            result.at[l, c, :, cols], out_block(l, c, columns), local_sem.at[0]
        )
        return there, here

    def finish_variable(l, sides, columns=everything):
        cols = slice(*columns)
        width = columns[1] - columns[0]
        if len(sides) == 2:
            increment = jnp.dot(
                pert[...].reshape(2 * mm, 3 * kk), gain[l, :, cols], preferred_element_type=F32
            )
        else:
            increment = jnp.zeros((2 * mm, width), F32)
            for w in (1,) + sides:
                increment = increment + jnp.dot(
                    pert[:, :, span(w)].reshape(2 * mm, kk),
                    gain[l, span(w), cols],
                    preferred_element_type=F32,
                )
        base = means[l, 0:1, cols][None] + scale[0:1, 0:1][None] * anom[
            l, pl.ds(2 * q, 2), :, cols
        ].astype(F32)
        result[l, :, :, cols] = (base + increment.reshape(2, mm, width)).astype(BF16)

    def send_result(l, columns=everything):
        for copy in out_copies(l, columns):
            copy.start()

    def early_gain(sides):
        def step(l, carry):
            gain_rows(l, sides)
            return carry

        lax.fori_loop(0, 3, step, 0)

    by_place(early_gain)
    for side in (0, 1):

        @pl.when(has_side[side])
        def _():
            side_pert(1 - side).wait_recv()
            pert_forward(side, c).start()

    ready = min(READY, last)

    def ahead(l, carry):
        wait_variable(l)
        by_place(lambda sides: own_window(l, (1,) + sides))
        return carry

    lax.fori_loop(3, ready, ahead, 0)
    @pl.when(middle)
    def _():
        group(3 * slot_bytes).wait_recv()

    @pl.when(jnp.logical_not(middle))
    def _():
        group(2 * slot_bytes).wait_recv()

    def late_variable(l, carry):
        by_place(lambda sides: finish_variable(l, sides))
        send_result(l)
        return carry

    lax.fori_loop(0, ready, late_variable, 0)

    def whole_variable(l, columns=everything):
        wait_variable(l, columns)

        def step(sides):
            own_window(l, (1,) + sides, columns)
            finish_variable(l, sides, columns)

        by_place(step)
        send_result(l, columns)

    def one_variable(l, carry):
        whole_variable(l)
        return carry

    lax.fori_loop(ready, last, one_variable, 0)
    for p in range(PIECES):
        whole_variable(last, (p * piece, (p + 1) * piece))

    sent = gathered.at[:, pl.ds(0, nm - 1)]
    rdma(sent, sent, send_e.at[0], recv_e.at[0], dev(member=sib)).wait_send()
    mine = out.at[:, :, pl.ds(pl.multiple_of(c * half, 128), half)]
    other = out.at[:, :, pl.ds(pl.multiple_of((1 - c) * half, 128), half)]
    pltpu.make_async_copy(mine, mine, local_sem.at[0]).wait()
    theirs = rdma(other, other, send_out.at[0], recv_out.at[0], dev(member=sib))
    theirs.wait_send()
    theirs.wait_recv()
    square_all.wait_send()

    def plane_done(sent, taken):
        columns = sent[1] + (nd - 1) * taken[1]
        group(
            (nd - 1) * (mm + 16) * kk * 2
            + (ng + 1) * slot_bytes
            + (ng - 1) * mm * columns * 2
        ).wait_send()

    by_depth(
        lambda sent: by_depth(lambda taken: plane_done(sent, taken)), late=sends_late
    )
    for way in (0, 1):

        @pl.when(has_side[1 - way])
        def _():
            total_copy(way).wait_send()

    for side in (0, 1):

        @pl.when(has_side[side])
        def _():
            group_from((2 * ng + 2) * slot_bytes + 2 * stat_bytes, side).wait_send()


def hand_on(block, out):
    pass


def solution(mesh):
    nr, nd, nm = (mesh.shape[a] for a in ("region", "depth", "member"))

    def shards(ensemble, obs_weights, obs_tiles, obs_values, obs_error, obs_noise):
        nl, mm, tt = ensemble.shape
        kk = obs_tiles.shape[0]
        ng = nm // 2
        half = tt // 2
        rp = -(-nr // 8) * 8
        dma = pltpu.SemaphoreType.DMA
        vmem = pl.BlockSpec(memory_space=pltpu.VMEM)
        anywhere = pl.BlockSpec(memory_space=pl.ANY)
        analysis, inflation = pl.pallas_call(
            functools.partial(kernel, (nr, nd, nm, nl, mm, tt, kk)),
            out_shape=(
                pltpu.VMEM((nl, mm, tt), BF16),
                pltpu.VMEM((1, 1), F32),
            ),
            in_specs=[anywhere] * 6,
            out_specs=(vmem, vmem),
            scratch_shapes=[
                pltpu.SMEM((nl,), F32),
                pltpu.VMEM((1, kk), jnp.int32),
                pltpu.VMEM((1, kk), F32),
                pltpu.VMEM((1, kk), F32),
                pltpu.VMEM((nl, mm, tt), BF16),
                pltpu.VMEM((nl, nm, mm, half), BF16),
                pltpu.VMEM((mm, kk), F32),
                pltpu.VMEM((mm + 16, kk), BF16),
                pltpu.VMEM((nd, mm + 16, kk), BF16),
                pltpu.VMEM((nm, 2, kk), F32),
                pltpu.VMEM((2, rp, 128), F32),
                pltpu.VMEM((2, rp, 128), F32),
                pltpu.VMEM((3, 8, kk), F32),
                pltpu.VMEM((3, 8, kk), F32),
                pltpu.VMEM((nm, mm, 3 * kk), BF16),
                pltpu.VMEM((2, mm, 3 * kk), BF16),
                pltpu.VMEM((3 * kk, nm * mm), BF16),
                pltpu.VMEM((3 * kk, half), F32),
                pltpu.VMEM((nl, nm, mm, half), BF16),
                pltpu.VMEM((nl, 8, half), F32),
                pltpu.VMEM((nl, 3 * kk, half), BF16),
                pltpu.VMEM((nl, 2, mm, half), BF16),
                pltpu.VMEM((1, 128), F32),
                pltpu.SemaphoreType.REGULAR((2,)),
                dma((1,)),
                dma((2,)),
                dma((1,)),
                dma((4,)),
                dma((3,)),
                dma((1,)),
                dma((nl - 1 + PIECES,)),
                dma((nd - 1,)),
                dma((1,)),
                dma((1,)),
                dma((ng - 1,)),
                dma((2,)),
                dma((2,)),
                dma((ng - 1, nd - 1)),
                dma((2,)),
                dma((2,)),
                dma((2,)),
                dma((nd + 2,)),
                dma((1,)),
                dma((1,)),
            ],
            compiler_params=pltpu.CompilerParams(
                collective_id=0, has_side_effects=True, vmem_limit_bytes=56 * 1024 * 1024
            ),
        )(
            obs_weights,
            ensemble,
            obs_tiles.reshape(1, kk),
            obs_values.reshape(1, kk),
            obs_error.reshape(1, kk),
            obs_noise,
        )
        analysis = pl.pallas_call(
            hand_on,
            out_shape=jax.ShapeDtypeStruct((nl, mm, tt), BF16),
            in_specs=[anywhere],
            out_specs=anywhere,
            input_output_aliases={0: 0},
        )(analysis)
        return analysis, inflation.reshape(())

    return jax.shard_map(
        shards,
        mesh=mesh,
        in_specs=(
            P("depth", "member", "region"),
            P("depth"),
            P("region"),
            P("region"),
            P("region"),
            P("member", "region"),
        ),
        out_specs=(P("depth", "member", "region"), P()),
        check_vma=False,
    )
```

```python
import functools

import jax
import jax.numpy as jnp
from jax import lax
from jax.experimental import pallas as pl
from jax.experimental.pallas import tpu as pltpu
from jax.sharding import PartitionSpec as P

RADIUS = 1024
LEAD = 2
READY = 4
PIECES = 2
F32 = jnp.float32
BF16 = jnp.bfloat16
MESH = pl.DeviceIdType.MESH


def kernel(
    sizes,
    weights_hbm,
    ensemble,
    tiles_hbm,
    values_hbm,
    errors_hbm,
    noise,
    out,
    infl_out,
    weights,
    tiles,
    values,
    errors,
    own,
    gathered,
    noise_v,
    part,
    part_in,
    squares,
    tot_in,
    tot_out,
    pos,
    stats,
    obs,
    pert,
    obs_t,
    taper,
    anom,
    means,
    gain,
    result,
    scale,
    answer,
    plane_sent,
    side_sent,
    recv_pert,
    small_sem,
    local_sem,
    send_e,
    recv_e,
    recv_p,
    send_q,
    recv_q,
    recv_o,
    send_g,
    recv_g,
    recv_y,
    recv_z,
    recv_pos,
    recv_pz,
    recv_f,
    send_out,
    recv_out,
):
    nr, nd, nm, nl, mm, tt, kk = sizes
    ng = nm // 2
    half = tt // 2
    members = nm * mm
    r = lax.axis_index("region")
    d = lax.axis_index("depth")
    me = lax.axis_index("member")
    q = me // 2
    c = me % 2
    sib = 2 * q + (1 - c)
    has_side = (r > 0, r < nr - 1)

    def dev(region=None, depth=None, member=None):
        return {
            "region": r if region is None else region,
            "depth": d if depth is None else depth,
            "member": me if member is None else member,
        }

    def rdma(src, dst, ssem, rsem, device):
        return pltpu.make_async_remote_copy(
            src_ref=src,
            dst_ref=dst,
            send_sem=ssem,
            recv_sem=rsem,
            device_id=device,
            device_id_type=MESH,
        )

    barrier = pltpu.get_barrier_semaphore()
    for j in range(1, nm):
        pl.semaphore_signal(
            barrier, inc=1, device_id=dev(member=(me + j) % nm), device_id_type=MESH
        )
    for i in range(1, nd):

        @pl.when(d + i < nd)
        def _():
            pl.semaphore_signal(barrier, inc=1, device_id=dev(depth=d + i), device_id_type=MESH)

    @pl.when(has_side[1])
    def _():
        pl.semaphore_signal(barrier, inc=1, device_id=dev(region=r + 1), device_id_type=MESH)

    local_own = pltpu.make_async_copy(ensemble, own, local_sem.at[0])
    local_own.start()
    smalls = [
        pltpu.make_async_copy(a, b, small_sem.at[i])
        for i, (a, b) in enumerate(
            ((weights_hbm, weights), (tiles_hbm, tiles), (values_hbm, values), (errors_hbm, errors))
        )
    ]
    for copy in smalls:
        copy.start()
    local_half = pltpu.make_async_copy(
        ensemble.at[:, :, pl.ds(pl.multiple_of(c * half, 128), half)],
        gathered.at[:, me],
        local_sem.at[1],
    )
    local_half.start()
    local_noise = pltpu.make_async_copy(noise, noise_v, local_sem.at[2])
    local_noise.start()

    pl.semaphore_wait(barrier, nm - 1 + d + (r > 0).astype(jnp.int32))

    piece = half // PIECES
    small = half // 4
    last = nl - 1
    units = (
        [(0, 0, half)]
        + [(1, p * piece, piece) for p in range(PIECES)]
        + [(l, 0, half) for l in range(2, last)]
        + [(last, p * piece, piece) for p in range(PIECES)]
    )

    def arrival(l, lo):
        return recv_e.at[l + lo // piece] if isinstance(l, int) and l == last else recv_e.at[l]

    def send_bulk(chosen):
        for l, lo, width in chosen:
            for to in [(me + 2 * g) % nm for g in range(1, ng)] + [(sib + 2 * g) % nm for g in range(ng)]:
                rdma(
                    ensemble.at[
                        l, :, pl.ds(pl.multiple_of((to % 2) * half + lo, 128), width)
                    ],
                    gathered.at[l, me, :, pl.ds(lo, width)],
                    send_e.at[0],
                    arrival(l, lo),
                    dev(member=to),
                ).start()

    def wait_bulk(l, lo, width):
        block = gathered.at[l, pl.ds(0, nm - 1), :, pl.ds(lo, width)]
        rdma(block, block, send_e.at[0], arrival(l, lo), dev(member=sib)).wait_recv()

    send_bulk(units[:LEAD])
    for i in range(1, nd):

        @pl.when(d >= i)
        def _():
            pl.semaphore_signal(
                answer.at[0], inc=1, device_id=dev(depth=d - i), device_id_type=MESH
            )

    @pl.when(has_side[0])
    def _():
        pl.semaphore_signal(answer.at[1], inc=1, device_id=dev(region=r - 1), device_id_type=MESH)

    for copy in smalls:
        copy.wait()
    local_own.wait()
    total = own[0].astype(F32) * weights[0]
    for l in range(1, nl):
        total = total + own[l].astype(F32) * weights[l]
    hi = total.astype(BF16)
    rest = total - hi.astype(F32)
    mid = rest.astype(BF16)
    low = (rest - mid.astype(F32)).astype(BF16)
    tile_ids = lax.broadcasted_iota(jnp.int32, (tt, kk), 0)
    onehot = jnp.where(tile_ids == tiles[...], 1.0, 0.0).astype(BF16)
    terms = jnp.dot(
        jnp.concatenate([hi, mid, low], axis=0), onehot, preferred_element_type=F32
    )
    picked = terms[0:mm] + terms[mm : 2 * mm] + terms[2 * mm : 3 * mm]
    part_mean = jnp.sum(picked, axis=0, keepdims=True) / mm
    top = part_mean.astype(BF16).astype(F32)
    second_row = (part_mean - top).astype(BF16).astype(F32)
    third_row = part_mean - top - second_row
    prow = lax.broadcasted_iota(jnp.int32, (16, kk), 0)
    split = jnp.where(prow == 0, top, jnp.where(prow == 1, second_row, third_row))
    part[0:mm] = (picked - part_mean).astype(BF16)
    part[mm : mm + 16] = jnp.where(prow < 3, split, 0.0).astype(BF16)

    def whole(block):
        values_of = block.astype(F32)
        return values_of[0:mm] + jnp.sum(values_of[mm : mm + 16], axis=0, keepdims=True)

    def part_copy(i):
        to = (d + i) % nd
        return rdma(part, part_in.at[d], plane_sent.at[0], recv_p.at[i - 1], dev(depth=to))

    def part_from(i):
        frm = (d + i) % nd
        return rdma(
            part, part_in.at[frm], plane_sent.at[0], recv_p.at[nd - i - 1], dev(depth=frm)
        )

    @pl.when(d < nd - 1)
    def _():
        pl.semaphore_wait(answer.at[0], nd - 1 - d)

    for i in range(1, nd):
        part_copy(i).start()

    pos[1] = jnp.broadcast_to(tiles[...].astype(F32), (8, kk))

    def pos_copy(side):
        return rdma(
            pos.at[1],
            pos.at[2 - 2 * side],
            side_sent.at[side],
            recv_pos.at[1 - side],
            dev(region=r + (2 * side - 1)),
        )

    def pos_from(side):
        return rdma(
            pos.at[1],
            pos.at[2 * side],
            side_sent.at[side],
            recv_pos.at[side],
            dev(region=r + (2 * side - 1)),
        )

    lane = (lax.broadcasted_iota(jnp.int32, (kk, half), 1) + c * half).astype(F32)

    def make_taper(w):
        position = pos[w].T[:, 0:1] + float((w - 1) * tt)
        close = jnp.maximum(0.0, 1.0 - jnp.abs(lane - position) * (1.0 / RADIUS))
        taper[w * kk : (w + 1) * kk] = close * close

    make_taper(1)

    @pl.when(has_side[1])
    def _():
        pl.semaphore_wait(answer.at[1], 1)

    for side in (0, 1):

        @pl.when(has_side[side])
        def _():
            pos_copy(side).start()

    predicted = whole(part[...])
    for i in range(1, nd):
        part_from(i).wait_recv()
        predicted = predicted + whole(part_in[(d + i) % nd])
    own_sum = jnp.sum(predicted, axis=0, keepdims=True)
    spread_in = predicted - own_sum / mm
    own_square = jnp.sum(spread_in * spread_in, axis=0, keepdims=True)
    qrow = lax.broadcasted_iota(jnp.int32, (2, kk), 0)
    squares[me] = jnp.where(qrow == 0, own_sum, own_square)
    obs[me, :, kk : 2 * kk] = spread_in.astype(BF16)

    def square_copy(slot, to, number):
        block = squares.at[slot]
        return rdma(block, block, send_q.at[0], recv_q.at[number], dev(member=to))

    def square_wait(count, number):
        block = squares.at[pl.ds(0, count)]
        return rdma(block, block, send_q.at[0], recv_q.at[number], dev(member=sib))

    def cuts(first):
        at = [0] + [first + (kk - first) * h // (nd - 1) for h in range(nd)]
        return [(at[h], at[h + 1] - at[h]) for h in range(nd)]

    shares = (cuts(kk // nd), cuts(kk // (2 * nd)))
    whole_slot = (0, kk)
    first_region = jnp.logical_and(r == 0, ng == 2)
    sends_late = jnp.logical_and(first_region, q == 1)
    takes_late = jnp.logical_and(first_region, q == 0)

    def by_depth(step, ahead=0, late=takes_late):
        for h in range(nd):
            for parts, chosen in zip(shares, (jnp.logical_not(late), late)):

                @pl.when(jnp.logical_and(d == (h - ahead) % nd, chosen))
                def _():
                    step(parts[h])

    def obs_at(slot, w, extent):
        return obs.at[slot, :, pl.ds(w * kk + extent[0], extent[1])]

    def obs_copy(g, extent):
        block = obs_at(me, 1, extent)
        return rdma(
            block, block, plane_sent.at[0], recv_o.at[g - 1], dev(member=(me + 2 * g) % nm)
        )

    def obs_from(g, extent):
        block = obs_at(cross(g), 1, extent)
        return rdma(block, block, plane_sent.at[0], recv_o.at[ng - g - 1], dev(member=sib))

    def obs_swap(g, i, extent):
        block = obs_at(cross(g), 1, extent)
        return rdma(
            block, block, plane_sent.at[0], recv_y.at[g - 1, i - 1], dev(depth=(d + i) % nd)
        )

    def swap_from(g, i, extent):
        block = obs_at(cross(g), 1, extent)
        return rdma(
            block, block, plane_sent.at[0], recv_y.at[g - 1, nd - i - 1], dev(depth=(d + i) % nd)
        )

    def side_obs(side, slot, extent):
        return rdma(
            obs_at(slot, 1, extent),
            obs_at(slot, 2 if side == 0 else 0, extent),
            side_sent.at[side],
            recv_z.at[1 - side],
            dev(region=r + (2 * side - 1)),
        )

    slot_bytes = mm * kk * 2
    stat_bytes = 8 * kk * 4

    def group(size):
        block = taper.at[pl.ds(0, size // (4 * piece)), pl.ds(0, piece)]
        return rdma(block, block, plane_sent.at[0], recv_pert.at[0], dev(member=sib))

    def group_from(size, number):
        block = taper.at[pl.ds(0, size // (4 * piece)), pl.ds(0, piece)]
        return rdma(block, block, side_sent.at[number], recv_z.at[number], dev(member=sib))

    def sent_of(w):
        return plane_sent.at[0] if w == 1 else side_sent.at[w // 2]

    def obs_forward(w, slot, extent, number):
        block = obs_at(slot, w, extent)
        return rdma(block, block, sent_of(w), recv_f.at[number], dev(member=sib))

    def forward_all(w, wide, number):
        block = obs.at[pl.ds(0, wide[0]), :, pl.ds(0, wide[1])]
        return rdma(block, block, sent_of(w), recv_f.at[number], dev(member=sib))

    def cross(g):
        return 2 * ((q + g) % ng) + c

    for g in range(1, ng):
        square_copy(me, (me + 2 * g) % nm, 1).start()
    square_copy(me, sib, 0).start()
    by_depth(
        lambda extent: [obs_copy(g, extent).start() for g in range(1, ng)], late=sends_late
    )
    obs_forward(1, me, whole_slot, 0).start()
    send_bulk(units[LEAD:])
    for side in (0, 1):

        @pl.when(has_side[side])
        def _():
            side_obs(side, me, whole_slot).start()
            pos_from(side).wait_recv()
            make_taper(2 * side)

    square_wait(ng - 1, 1).wait_recv()
    for g in range(1, ng):
        square_copy(cross(g), sib, 0).start()
    square_wait(ng, 0).wait_recv()
    moments = [squares[j] for j in range(nm)]
    obs_mean = sum(m[0:1] for m in moments) / members
    deviation = predicted - obs_mean
    square_sum = sum(
        m[1:2] + mm * (m[0:1] / mm - obs_mean) * (m[0:1] / mm - obs_mean) for m in moments
    )
    spread = square_sum / (members - 1)
    error = errors[...]
    innovation = values[...] - obs_mean
    first = jnp.sum(innovation * innovation, axis=1, keepdims=True)
    second = jnp.sum(spread + error, axis=1, keepdims=True)
    rp = tot_in.shape[1]
    trow = lax.broadcasted_iota(jnp.int32, (rp, 128), 0)
    tlane = lax.broadcasted_iota(jnp.int32, (rp, 128), 1)
    own_total = jnp.where(tlane == 0, first, second)
    krow = lax.broadcasted_iota(jnp.int32, (8, kk), 0)
    shifts_of = jnp.zeros((8, kk), F32)
    for g in range(nm):
        shifts_of = jnp.where(krow == g, moments[g][0:1] / mm - obs_mean, shifts_of)
    stats[1] = shifts_of

    def stat_copy(side):
        return rdma(
            stats.at[1],
            stats.at[2 - 2 * side],
            side_sent.at[side],
            recv_z.at[1 - side],
            dev(region=r + (2 * side - 1)),
        )

    def total_copy(way):
        return rdma(
            tot_out.at[way],
            tot_in.at[way],
            send_g.at[way],
            recv_g.at[way],
            dev(region=r + (1 - 2 * way)),
        )

    def total_from(way):
        return rdma(
            tot_out.at[way],
            tot_in.at[way],
            send_g.at[way],
            recv_g.at[way],
            dev(region=r - (1 - 2 * way)),
        )

    def relay(way):
        @pl.when(has_side[way])
        def _():
            total_from(way).wait_recv()

        behind = trow < r if way == 0 else trow > r
        tot_out[way] = jnp.where(
            behind, tot_in[way], jnp.where(trow == r, own_total, 0.0)
        )

        @pl.when(has_side[1 - way])
        def _():
            total_copy(way).start()

    low_end = r == 0
    high_end = r == nr - 1

    @pl.when(low_end)
    def _():
        relay(0)

    @pl.when(high_end)
    def _():
        relay(1)

    for side in (0, 1):

        @pl.when(has_side[side])
        def _():
            stat_copy(side).start()

    def hand_part(g, i, extent):
        for side in (0, 1):

            @pl.when(has_side[side])
            def _():
                side_obs(side, cross(g), extent).start()

        obs_forward(1, cross(g), extent, i).start()

    def take_part(extent):
        for g in range(1, ng):
            obs_from(g, extent).wait_recv()
            for i in range(1, nd):
                obs_swap(g, i, extent).start()
            hand_part(g, 0, extent)

    by_depth(take_part)

    def transpose_part(w, extent):
        lo, width = extent
        rows_of = pl.ds(w * kk + lo, width)
        shifts = stats[w, :, lo : lo + width].T
        for g in range(nm):
            block = obs[g, :, rows_of].astype(F32).T + shifts[:, g : g + 1]
            obs_t[rows_of, g * mm : (g + 1) * mm] = block.astype(BF16)

    everything = (0, half)

    middle = jnp.logical_and(has_side[0], has_side[1])
    beside = jnp.where(has_side[0], 0, 2)

    def by_place(step):
        @pl.when(middle)
        def _():
            step((0, 2))

        @pl.when(jnp.logical_not(middle))
        def _():
            step((beside,))

    def span(w):
        return pl.ds(w * kk if isinstance(w, int) else pl.multiple_of(w * kk, 128), kk)

    def gain_rows(l, windows, columns=everything):
        cols = slice(*columns)
        right = anom[l, :, :, cols].reshape(members, columns[1] - columns[0])
        for w in windows:
            cov = jnp.dot(obs_t[span(w)], right, preferred_element_type=F32)
            gain[l, span(w), cols] = (cov * taper[span(w), cols]).astype(BF16)

    def gain_part(l, extent):
        at = pl.ds(kk + extent[0], extent[1])
        cov = jnp.dot(
            obs_t[at], anom[l].reshape(members, half), preferred_element_type=F32
        )
        gain[l, at] = (cov * taper[at]).astype(BF16)

    def wait_variable(l, columns=everything):
        wait_bulk(l, columns[0], columns[1] - columns[0])

    def center(l, columns=everything):
        cols = slice(*columns)
        raw = gathered[l, :, :, cols].astype(F32)
        mean = jnp.sum(jnp.sum(raw, axis=0), axis=0, keepdims=True) / members
        means[l, :, cols] = jnp.broadcast_to(mean, (8, columns[1] - columns[0]))
        anom[l, :, :, cols] = (raw - mean[None]).astype(BF16)

    def own_window(l, windows, columns=everything):
        center(l, columns)
        gain_rows(l, windows, columns)

    def sib_pert(slot):
        block = pert.at[slot, :, pl.ds(kk, kk)]
        return rdma(block, block, plane_sent.at[0], recv_pert.at[0], dev(member=sib))

    def side_pert(side):
        window = 2 * kk if side == 0 else 0
        return rdma(
            pert.at[c, :, pl.ds(kk, kk)],
            pert.at[c, :, pl.ds(window, kk)],
            side_sent.at[side],
            recv_pz.at[1 - side],
            dev(region=r + (2 * side - 1)),
        )

    def pert_forward(side, slot):
        block = pert.at[slot, :, pl.ds(2 * kk * side, kk)]
        return rdma(block, block, side_sent.at[side], recv_pert.at[0], dev(member=sib))

    def make_pert():
        everyone = jnp.where(trow < r, tot_in[0], jnp.where(trow > r, tot_in[1], own_total))
        grand = everyone[0:1]
        for i in range(1, nr):
            grand = grand + everyone[i : i + 1]
        inflation = grand[0:1, 0:1] / grand[0:1, 1:2]
        root = jnp.sqrt(inflation)
        infl_out[...] = inflation
        scale[...] = jnp.broadcast_to(root, (1, 128))
        factor = inflation / (inflation * spread + error)
        local_noise.wait()
        pert[c, :, kk : 2 * kk] = (
            (innovation + jnp.sqrt(error) * noise_v[...] - root * deviation)
            * (factor / (members - 1))
        ).astype(BF16)

        sib_pert(c).start()
        for side in (0, 1):

            @pl.when(has_side[side])
            def _():
                side_pert(side).start()

    mid_low = jnp.logical_and(r > 0, 2 * r < nr)
    mid_high = jnp.logical_and(r < nr - 1, 2 * r >= nr)

    @pl.when(mid_low)
    def _():
        relay(0)

    @pl.when(mid_high)
    def _():
        relay(1)

    local_half.wait()
    wait_variable(0)
    center(0)

    def own_part(extent):
        forward_all(1, (1, kk + (ng - 1) * extent[1]), 0).wait_recv()
        transpose_part(1, extent)
        gain_part(0, extent)

    by_depth(own_part)

    def swap_part(i, extent):
        for g in range(1, ng):
            swap_from(g, i, extent).wait_recv()
            hand_part(g, i, extent)

    for i in range(1, nd):
        by_depth(functools.partial(swap_part, i), i)
    wait_variable(1)
    center(1)
    by_depth(lambda extent: gain_part(1, extent))

    @pl.when(mid_low)
    def _():
        relay(1)
        make_pert()

    @pl.when(mid_high)
    def _():
        relay(0)
        make_pert()

    def other_part(i, extent):
        forward_all(1, (1, (ng - 1) * extent[1]), i).wait_recv()
        transpose_part(1, extent)
        gain_part(0, extent)
        gain_part(1, extent)

    for i in range(1, nd):
        by_depth(functools.partial(other_part, i), i)
    wait_variable(2)
    own_window(2, (1,))

    for side in (0, 1):

        @pl.when(has_side[side])
        def _():
            group_from(ng * slot_bytes + stat_bytes, side).wait_recv()
            for g in range(ng):
                obs_forward(2 * side, cross(g), whole_slot, nd + side).start()


    @pl.when(low_end)
    def _():
        relay(1)
        make_pert()

    @pl.when(high_end)
    def _():
        relay(0)
        make_pert()

    for side in (0, 1):

        @pl.when(has_side[side])
        def _():
            forward_all(2 * side, (ng, kk), nd + side).wait_recv()

            transpose_part(2 * side, whole_slot)

    def out_block(l, which, columns):
        lo, width = columns[0], columns[1] - columns[0]
        return out.at[l, :, pl.ds(pl.multiple_of(which * half + lo, 128), width)]

    def out_copies(l, columns):
        cols = slice(*columns)
        there = rdma(
            result.at[l, 1 - c, :, cols],
            out_block(l, c, columns),
            send_out.at[0],
            recv_out.at[0],
            dev(member=sib),
        )
        here = pltpu.make_async_copy(
            result.at[l, c, :, cols], out_block(l, c, columns), local_sem.at[0]
        )
        return there, here

    def finish_variable(l, sides, columns=everything):
        cols = slice(*columns)
        width = columns[1] - columns[0]
        if len(sides) == 2:
            increment = jnp.dot(
                pert[...].reshape(2 * mm, 3 * kk), gain[l, :, cols], preferred_element_type=F32
            )
        else:
            increment = jnp.zeros((2 * mm, width), F32)
            for w in (1,) + sides:
                increment = increment + jnp.dot(
                    pert[:, :, span(w)].reshape(2 * mm, kk),
                    gain[l, span(w), cols],
                    preferred_element_type=F32,
                )
        base = means[l, 0:1, cols][None] + scale[0:1, 0:1][None] * anom[
            l, pl.ds(2 * q, 2), :, cols
        ].astype(F32)
        result[l, :, :, cols] = (base + increment.reshape(2, mm, width)).astype(BF16)

    def send_result(l, columns=everything):
        for copy in out_copies(l, columns):
            copy.start()

    def early_gain(sides):
        def step(l, carry):
            gain_rows(l, sides)
            return carry

        lax.fori_loop(0, 3, step, 0)

    by_place(early_gain)
    for side in (0, 1):

        @pl.when(has_side[side])
        def _():
            side_pert(1 - side).wait_recv()
            pert_forward(side, c).start()

    ready = min(READY, last)

    def ahead(l, carry):
        wait_variable(l)
        by_place(lambda sides: own_window(l, (1,) + sides))
        return carry

    lax.fori_loop(3, ready, ahead, 0)
    @pl.when(middle)
    def _():
        group(3 * slot_bytes).wait_recv()

    @pl.when(jnp.logical_not(middle))
    def _():
        group(2 * slot_bytes).wait_recv()

    def late_variable(l, carry):
        by_place(lambda sides: finish_variable(l, sides))
        send_result(l)
        return carry

    lax.fori_loop(0, ready, late_variable, 0)

    def whole_variable(l, columns=everything):
        wait_variable(l, columns)

        def step(sides):
            own_window(l, (1,) + sides, columns)
            finish_variable(l, sides, columns)

        by_place(step)
        send_result(l, columns)

    def one_variable(l, carry):
        whole_variable(l)
        return carry

    lax.fori_loop(ready, last, one_variable, 0)
    for p in range(PIECES):
        whole_variable(last, (p * piece, (p + 1) * piece))

    sent = gathered.at[:, pl.ds(0, nm - 1)]
    rdma(sent, sent, send_e.at[0], recv_e.at[0], dev(member=sib)).wait_send()
    mine = out.at[:, :, pl.ds(pl.multiple_of(c * half, 128), half)]
    other = out.at[:, :, pl.ds(pl.multiple_of((1 - c) * half, 128), half)]
    pltpu.make_async_copy(mine, mine, local_sem.at[0]).wait()
    theirs = rdma(other, other, send_out.at[0], recv_out.at[0], dev(member=sib))
    theirs.wait_send()
    theirs.wait_recv()
    square_wait(nm - 1, 0).wait_send()

    def plane_done(sent, taken):
        columns = sent[1] + (nd - 1) * taken[1]
        group(
            (nd - 1) * (mm + 16) * kk * 2
            + (ng + 1) * slot_bytes
            + (ng - 1) * mm * columns * 2
        ).wait_send()

    by_depth(
        lambda sent: by_depth(lambda taken: plane_done(sent, taken)), late=sends_late
    )
    for way in (0, 1):

        @pl.when(has_side[1 - way])
        def _():
            total_copy(way).wait_send()

    for side in (0, 1):

        @pl.when(has_side[side])
        def _():
            group_from((2 * ng + 2) * slot_bytes + 2 * stat_bytes, side).wait_send()


def hand_on(block, out):
    pass


def solution(mesh):
    nr, nd, nm = (mesh.shape[a] for a in ("region", "depth", "member"))

    def shards(ensemble, obs_weights, obs_tiles, obs_values, obs_error, obs_noise):
        nl, mm, tt = ensemble.shape
        kk = obs_tiles.shape[0]
        ng = nm // 2
        half = tt // 2
        rp = -(-nr // 8) * 8
        dma = pltpu.SemaphoreType.DMA
        vmem = pl.BlockSpec(memory_space=pltpu.VMEM)
        anywhere = pl.BlockSpec(memory_space=pl.ANY)
        analysis, inflation = pl.pallas_call(
            functools.partial(kernel, (nr, nd, nm, nl, mm, tt, kk)),
            out_shape=(
                pltpu.VMEM((nl, mm, tt), BF16),
                pltpu.VMEM((1, 1), F32),
            ),
            in_specs=[anywhere] * 6,
            out_specs=(vmem, vmem),
            scratch_shapes=[
                pltpu.SMEM((nl,), F32),
                pltpu.VMEM((1, kk), jnp.int32),
                pltpu.VMEM((1, kk), F32),
                pltpu.VMEM((1, kk), F32),
                pltpu.VMEM((nl, mm, tt), BF16),
                pltpu.VMEM((nl, nm, mm, half), BF16),
                pltpu.VMEM((mm, kk), F32),
                pltpu.VMEM((mm + 16, kk), BF16),
                pltpu.VMEM((nd, mm + 16, kk), BF16),
                pltpu.VMEM((nm, 2, kk), F32),
                pltpu.VMEM((2, rp, 128), F32),
                pltpu.VMEM((2, rp, 128), F32),
                pltpu.VMEM((3, 8, kk), F32),
                pltpu.VMEM((3, 8, kk), F32),
                pltpu.VMEM((nm, mm, 3 * kk), BF16),
                pltpu.VMEM((2, mm, 3 * kk), BF16),
                pltpu.VMEM((3 * kk, nm * mm), BF16),
                pltpu.VMEM((3 * kk, half), F32),
                pltpu.VMEM((nl, nm, mm, half), BF16),
                pltpu.VMEM((nl, 8, half), F32),
                pltpu.VMEM((nl, 3 * kk, half), BF16),
                pltpu.VMEM((nl, 2, mm, half), BF16),
                pltpu.VMEM((1, 128), F32),
                pltpu.SemaphoreType.REGULAR((2,)),
                dma((1,)),
                dma((2,)),
                dma((1,)),
                dma((4,)),
                dma((3,)),
                dma((1,)),
                dma((nl - 1 + PIECES,)),
                dma((nd - 1,)),
                dma((1,)),
                dma((2,)),
                dma((ng - 1,)),
                dma((2,)),
                dma((2,)),
                dma((ng - 1, nd - 1)),
                dma((2,)),
                dma((2,)),
                dma((2,)),
                dma((nd + 2,)),
                dma((1,)),
                dma((1,)),
            ],
            compiler_params=pltpu.CompilerParams(
                collective_id=0, has_side_effects=True, vmem_limit_bytes=56 * 1024 * 1024
            ),
        )(
            obs_weights,
            ensemble,
            obs_tiles.reshape(1, kk),
            obs_values.reshape(1, kk),
            obs_error.reshape(1, kk),
            obs_noise,
        )
        analysis = pl.pallas_call(
            hand_on,
            out_shape=jax.ShapeDtypeStruct((nl, mm, tt), BF16),
            in_specs=[anywhere],
            out_specs=anywhere,
            input_output_aliases={0: 0},
        )(analysis)
        return analysis, inflation.reshape(())

    return jax.shard_map(
        shards,
        mesh=mesh,
        in_specs=(
            P("depth", "member", "region"),
            P("depth"),
            P("region"),
            P("region"),
            P("region"),
            P("member", "region"),
        ),
        out_specs=(P("depth", "member", "region"), P()),
        check_vma=False,
    )
```
